32 devices in a mesh: fsdp: 32 (over z, y, x, core).
Axes of the slice: x: 2, y: 2, z: 4, core: 2. Of those that a mesh axis runs over, the one named last changes fastest.
Arguments:
- tok_ids: int32 [32, 256], P('fsdp')
- grad_out: bfloat16 [32, 256, 2048], P('fsdp')
- emb_table: bfloat16 [151936, 2048], P('fsdp')
- norm_gain: bfloat16 [2048], P('fsdp')
- w_query: bfloat16 [2048, 2048], P('fsdp')
- b_query: bfloat16 [2048], P('fsdp')
- w_key: bfloat16 [2048, 256], P('fsdp')
- b_key: bfloat16 [256], P('fsdp')
- w_value: bfloat16 [2048, 256], P('fsdp')
- b_value: bfloat16 [256], P('fsdp')
- w_out: bfloat16 [2048, 2048], P('fsdp')
Outputs:
- output 1: bfloat16 [32, 256, 2048], P('fsdp')
- output 2: bfloat16 [151936, 2048], P('fsdp')
- output 3: float32 [2048], P('fsdp')
- output 4: float32 [2048, 2048], P('fsdp')
- output 5: float32 [2048], P('fsdp')
- output 6: float32 [2048, 256], P('fsdp')
- output 7: float32 [256], P('fsdp')
- output 8: float32 [2048, 256], P('fsdp')
- output 9: float32 [256], P('fsdp')
- output 10: float32 [2048, 2048], P('fsdp')
All inputs are finite; a program needn't handle non-finite values.
Results may differ from the reference program's by a relative error of at most 0.0179842.
Values are sent between devices in bfloat16 or wider.
A program may use at most 1 GiB of HBM per device.

```python
import jax
import jax.numpy as jnp
from jax import lax

VOCAB = 151936
D_MODEL = 2048
HEADS = 16
KV_HEADS = 2
HEAD_DIM = 128
BATCH = 32
SEQ = 256
HOT_IDS = 4096
ROPE_THETA = 1.0e6
NORM_EPS = 1e-6
MASK_VALUE = -1e30


def draw_ids(key_ids):
    key_pick, key_hot, key_wide = jax.random.split(key_ids, 3)
    pick_hot = jax.random.randint(key_pick, (BATCH, SEQ), 0, 2)
    low_ids = jax.random.randint(key_hot, (BATCH, SEQ), 0, HOT_IDS)
    hot_ids = (low_ids * low_ids) // HOT_IDS
    wide_ids = jax.random.randint(key_wide, (BATCH, SEQ), 0, VOCAB)
    tok_ids = jnp.where(pick_hot == 0, hot_ids, wide_ids).astype(jnp.int32)
    return tok_ids.at[0, SEQ - 1].set(VOCAB - 1)


def setup_inputs(seed: int = 0) -> dict:
    key_list = jax.random.split(jax.random.key(seed), 12)
    q_width = HEADS * HEAD_DIM
    kv_width = KV_HEADS * HEAD_DIM
    in_scale = D_MODEL ** -0.5
    out_scale = q_width ** -0.5

    def normal(key_n, shape):
        return jax.random.normal(key_n, shape, jnp.float32)

    return {
        "tok_ids": draw_ids(key_list[0]),
        "grad_out": normal(key_list[1], (BATCH, SEQ, D_MODEL)).astype(jnp.bfloat16),
        "emb_table": normal(key_list[2], (VOCAB, D_MODEL)).astype(jnp.bfloat16),
        "norm_gain": (1.0 + 0.3 * normal(key_list[3], (D_MODEL,))).astype(jnp.bfloat16),
        "w_query": (in_scale * normal(key_list[4], (D_MODEL, q_width))).astype(jnp.bfloat16),
        "b_query": (0.5 * normal(key_list[5], (q_width,))).astype(jnp.bfloat16),
        "w_key": (in_scale * normal(key_list[6], (D_MODEL, kv_width))).astype(jnp.bfloat16),
        "b_key": (0.5 * normal(key_list[7], (kv_width,))).astype(jnp.bfloat16),
        "w_value": (in_scale * normal(key_list[8], (D_MODEL, kv_width))).astype(jnp.bfloat16),
        "b_value": (0.5 * normal(key_list[9], (kv_width,))).astype(jnp.bfloat16),
        "w_out": (out_scale * normal(key_list[10], (q_width, D_MODEL))).astype(jnp.bfloat16),
    }


def rope_tables():
    half_dim = HEAD_DIM // 2
    inv_freq = jnp.power(ROPE_THETA, -(jnp.arange(half_dim, dtype=jnp.float32) * 2.0 / HEAD_DIM))
    angles = jnp.arange(SEQ, dtype=jnp.float32)[:, None] * inv_freq[None, :]
    angles = jnp.concatenate([angles, angles], axis=-1)
    return jnp.cos(angles)[:, None, :], jnp.sin(angles)[:, None, :]


def rotate(vector, cos_t, sin_t):
    half_dim = HEAD_DIM // 2
    turned = jnp.concatenate([-vector[..., half_dim:], vector[..., :half_dim]], axis=-1)
    return vector * cos_t + turned * sin_t


def block_seq(x_seq, params):
    gain_vec, w_query, b_query, w_key, b_key, w_value, b_value, w_out = params
    cos_t, sin_t = rope_tables()
    q_group = HEADS // KV_HEADS
    inv_rms = lax.rsqrt(jnp.mean(x_seq * x_seq, axis=-1, keepdims=True) + NORM_EPS)
    hidden = (x_seq * inv_rms * gain_vec).astype(jnp.bfloat16).astype(jnp.float32)
    q_lin = jnp.dot(hidden, w_query, preferred_element_type=jnp.float32) + b_query
    k_lin = jnp.dot(hidden, w_key, preferred_element_type=jnp.float32) + b_key
    v_lin = jnp.dot(hidden, w_value, preferred_element_type=jnp.float32) + b_value
    q_rot = rotate(q_lin.reshape(SEQ, HEADS, HEAD_DIM), cos_t, sin_t)
    q_rot = q_rot.astype(jnp.bfloat16).astype(jnp.float32).reshape(SEQ, KV_HEADS, q_group, HEAD_DIM)
    k_rot = rotate(k_lin.reshape(SEQ, KV_HEADS, HEAD_DIM), cos_t, sin_t)
    k_rot = k_rot.astype(jnp.bfloat16).astype(jnp.float32)
    v_val = v_lin.reshape(SEQ, KV_HEADS, HEAD_DIM).astype(jnp.bfloat16).astype(jnp.float32)
    scores = jnp.einsum("qkgd,skd->kgqs", q_rot, k_rot) * (HEAD_DIM ** -0.5)
    causal = jnp.arange(SEQ)[:, None] >= jnp.arange(SEQ)[None, :]
    scores = jnp.where(causal, scores, MASK_VALUE)
    prob_b = jax.nn.softmax(scores, axis=-1).astype(jnp.bfloat16).astype(jnp.float32)
    attn_out = jnp.einsum("kgqs,skd->qkgd", prob_b, v_val).reshape(SEQ, HEADS * HEAD_DIM)
    attn_out = attn_out.astype(jnp.bfloat16).astype(jnp.float32)
    proj_out = jnp.dot(attn_out, w_out, preferred_element_type=jnp.float32)
    return (x_seq + proj_out).astype(jnp.bfloat16)


def reference(tok_ids, grad_out, emb_table, norm_gain, w_query, b_query, w_key, b_key, w_value, b_value, w_out):
    x_all = jnp.take(emb_table, tok_ids, axis=0).astype(jnp.float32)
    params = tuple(weight.astype(jnp.float32) for weight in (norm_gain, w_query, b_query, w_key, b_key, w_value, b_value, w_out))
    seq_step = jax.checkpoint(block_seq)

    def forward(x_in, prm_list):
        return lax.map(lambda x_seq: seq_step(x_seq, prm_list), x_in)

    block_out, pullback = jax.vjp(forward, x_all, params)
    d_x, d_params = pullback(grad_out)
    grad_table = jax.ops.segment_sum(d_x.reshape(-1, D_MODEL), tok_ids.reshape(-1), num_segments=VOCAB)
    grad_table = grad_table.astype(jnp.bfloat16)
    return (block_out, grad_table, d_params[0], d_params[1], d_params[2], d_params[3], d_params[4], d_params[5], d_params[6], d_params[7])
```

```python
import functools

import jax
import jax.numpy as jnp
from jax import lax
from jax.experimental import pallas as pl
from jax.experimental.pallas import tpu as pltpu
from jax.sharding import PartitionSpec as P

HEAD_DIM = 128
ROPE_THETA = 1.0e6
NORM_EPS = 1e-6
MASK_VALUE = -1e30
N_DEV = 32
HOT_CAP = 176
COLD_CAP = 16
QKV = 2560
WCOLS = 4608
MESH = pl.DeviceIdType.MESH


def rope_tables(seq_len):
    half_dim = HEAD_DIM // 2
    inv_freq = jnp.power(ROPE_THETA, -(jnp.arange(half_dim, dtype=jnp.float32) * 2.0 / HEAD_DIM))
    angles = jnp.arange(seq_len, dtype=jnp.float32)[:, None] * inv_freq[None, :]
    angles = jnp.concatenate([angles, angles], axis=-1)
    return jnp.cos(angles)[:, None, :], jnp.sin(angles)[:, None, :]


def rotate(vector, cos_t, sin_t):
    half_dim = HEAD_DIM // 2
    turned = jnp.concatenate([-vector[..., half_dim:], vector[..., :half_dim]], axis=-1)
    return vector * cos_t + turned * sin_t


def rotate_back(grad_in, cos_t, sin_t):
    half_dim = HEAD_DIM // 2
    scaled = grad_in * sin_t
    turned = jnp.concatenate([scaled[..., half_dim:], -scaled[..., :half_dim]], axis=-1)
    return grad_in * cos_t + turned


RELAY_A = tuple(8 * z + 2 for z in (3, 2, 1)) + tuple(8 * z + 6 for z in (1, 0))
RELAY_B = tuple(8 * z + 4 for z in (3, 2, 1)) + tuple(8 * z + 6 for z in (3, 2))
N_RELAY = 5


def far_blocks():
    out = []
    for k in range(N_RELAY):
        for core in range(2):
            out.append((RELAY_A[k] + core, 2 + core, k))
            out.append((RELAY_B[k] + core, 4 + core, k))
    return out


def near_blocks():
    return [8 * z + c for z in (3, 2, 1) for c in range(2)] + [2, 3, 4, 5, 1]


def enter_all(me):
    barrier = pltpu.get_barrier_semaphore()

    def tell(off, carry):
        pl.semaphore_signal(barrier, inc=1, device_id=(lax.rem(me + off, N_DEV),), device_id_type=MESH)
        return carry

    lax.fori_loop(1, N_DEV, tell, 0)
    pl.semaphore_wait(barrier, N_DEV - 1)


def small_gather_kernel(src, dst, send_sem, recv_sem, own_sem):
    me = lax.axis_index("fsdp")
    enter_all(me)

    def copy(off):
        return pltpu.make_async_remote_copy(
            src_ref=src, dst_ref=dst.at[me], send_sem=send_sem.at[off], recv_sem=recv_sem.at[off],
            device_id=(lax.rem(me + off, N_DEV),), device_id_type=MESH)

    def start(off, carry):
        copy(off).start()
        return carry

    def finish(off, carry):
        copy(off).wait()
        return carry

    lax.fori_loop(1, N_DEV, start, 0)
    own = pltpu.make_async_copy(src, dst.at[me], own_sem)
    own.start()
    lax.fori_loop(1, N_DEV, finish, 0)
    own.wait()


def small_gather(block):
    return pl.pallas_call(
        small_gather_kernel,
        out_shape=jax.ShapeDtypeStruct((N_DEV,) + block.shape, block.dtype),
        in_specs=[pl.BlockSpec(memory_space=pltpu.VMEM)],
        out_specs=pl.BlockSpec(memory_space=pltpu.VMEM),
        scratch_shapes=[pltpu.SemaphoreType.DMA((N_DEV,)), pltpu.SemaphoreType.DMA((N_DEV,)), pltpu.SemaphoreType.DMA],
        compiler_params=pltpu.CompilerParams(collective_id=1, has_side_effects=True),
        name="small_gather",
    )(block)


def cold_copy(me, off, src, dst, rows, send_sem, recv_sem):
    other = lax.rem(me + off, N_DEV)
    return pltpu.make_async_remote_copy(
        src_ref=src.at[pl.ds(pl.multiple_of(other * rows, rows), rows)],
        dst_ref=dst.at[pl.ds(pl.multiple_of(me * rows, rows), rows)],
        send_sem=send_sem.at[off], recv_sem=recv_sem.at[off],
        device_id=(other,), device_id_type=MESH)


def relay_ids(me, k):
    core = lax.rem(me, 2)
    is_a = me < 4
    return jnp.where(is_a, RELAY_A[k], RELAY_B[k]) + core


def lookup_kernel(hot_send, cold_send, hot_recv, cold_recv, relay, hs_sem, hr_sem, rr_sem, fs_sem, cs_sem, cr_sem, own_sem):
    me = lax.axis_index("fsdp")
    enter_all(me)

    def hot_block(dev):
        return hot_send.at[pl.ds(dev * HOT_CAP, HOT_CAP)]

    def out_copies():
        copies = []
        near = near_blocks()
        far = far_blocks()
        order = []
        while near or far:
            if far:
                order.extend(far[:4])
                far = far[4:]
            if near:
                order.extend(near[:2])
                near = near[2:]
        for item in order:
            if isinstance(item, tuple):
                dev, via, k = item
                copies.append(pltpu.make_async_remote_copy(
                    src_ref=hot_block(dev), dst_ref=relay.at[k], send_sem=hs_sem.at[dev], recv_sem=rr_sem.at[k],
                    device_id=(via,), device_id_type=MESH))
            else:
                copies.append(pltpu.make_async_remote_copy(
                    src_ref=hot_block(item), dst_ref=hot_recv, send_sem=hs_sem.at[item], recv_sem=hr_sem,
                    device_id=(item,), device_id_type=MESH))
        return copies

    @pl.when(me == 0)
    def _():
        for copy in out_copies():
            copy.start()

    def start(off, carry):
        cold_copy(me, off, cold_send, cold_recv, COLD_CAP, cs_sem, cr_sem).start()
        return carry

    lax.fori_loop(1, N_DEV, start, 0)
    own_rows = pl.ds(pl.multiple_of(me * COLD_CAP, COLD_CAP), COLD_CAP)
    own_cold = pltpu.make_async_copy(cold_send.at[own_rows], cold_recv.at[own_rows], own_sem.at[0])
    own_cold.start()
    own_hot = pltpu.make_async_copy(hot_block(0), hot_recv, own_sem.at[1])

    @pl.when(me == 0)
    def _():
        own_hot.start()

    @pl.when((me >= 2) & (me < 6))
    def _():
        def onward(k):
            return pltpu.make_async_remote_copy(
                src_ref=relay.at[k], dst_ref=hot_recv, send_sem=fs_sem.at[k], recv_sem=hr_sem,
                device_id=(relay_ids(me, k),), device_id_type=MESH)

        for k in range(N_RELAY):
            pltpu.make_async_copy(relay.at[k], relay.at[k], rr_sem.at[k]).wait()
            onward(k).start()
        for k in range(N_RELAY):
            onward(k).wait_send()

    def finish(off, carry):
        cold_copy(me, off, cold_send, cold_recv, COLD_CAP, cs_sem, cr_sem).wait()
        return carry

    lax.fori_loop(1, N_DEV, finish, 0)
    own_cold.wait()

    @pl.when(me == 0)
    def _():
        own_hot.wait()
        for copy in out_copies():
            copy.wait_send()

    @pl.when(me != 0)
    def _():
        pltpu.make_async_copy(hot_recv, hot_recv, hr_sem).wait()


def lookup_exchange(hot_send, cold_send):
    width = hot_send.shape[1]
    dma = pltpu.SemaphoreType.DMA
    return pl.pallas_call(
        lookup_kernel,
        out_shape=(jax.ShapeDtypeStruct((HOT_CAP, width), jnp.bfloat16),
                   jax.ShapeDtypeStruct((N_DEV * COLD_CAP, width), jnp.bfloat16)),
        in_specs=[pl.BlockSpec(memory_space=pl.ANY)] * 2,
        out_specs=(pl.BlockSpec(memory_space=pl.ANY),) * 2,
        scratch_shapes=[pltpu.VMEM((N_RELAY, HOT_CAP, width), jnp.bfloat16),
                        dma((N_DEV,)), dma, dma((N_RELAY,)), dma((N_RELAY,)), dma((N_DEV,)), dma((N_DEV,)), dma((2,))],
        compiler_params=pltpu.CompilerParams(collective_id=2, has_side_effects=True),
        cost_estimate=pl.CostEstimate(flops=60_000_000_000, bytes_accessed=30_000_000, transcendentals=0),
        name="lookup_exchange",
    )(hot_send, cold_send)


def return_kernel(hot_send, cold_send, vec_send, hot_recv, cold_recv, vec_recv, relay,
                  hs_sem, hr_sem, rr_sem, fs_sem, cs_sem, cr_sem, vs_sem, vr_sem, own_sem):
    me = lax.axis_index("fsdp")
    enter_all(me)

    def hot_block(dev):
        return hot_recv.at[pl.ds(pl.multiple_of(dev * HOT_CAP, HOT_CAP), HOT_CAP)]

    def direct():
        return pltpu.make_async_remote_copy(
            src_ref=hot_send, dst_ref=hot_block(me), send_sem=hs_sem, recv_sem=hr_sem.at[me],
            device_id=(0,), device_id_type=MESH)

    def to_relay(via, k):
        return pltpu.make_async_remote_copy(
            src_ref=hot_send, dst_ref=relay.at[k], send_sem=hs_sem, recv_sem=rr_sem.at[k],
            device_id=(via,), device_id_type=MESH)

    far = far_blocks()
    is_near = functools.reduce(lambda a, b: a | b, [me == dev for dev in near_blocks()])

    @pl.when(is_near)
    def _():
        direct().start()

    for dev, via, k in far:
        @pl.when(me == dev)
        def _(via=via, k=k):
            to_relay(via, k).start()

    def vec_copy(off):
        other = lax.rem(me + off, N_DEV)
        return pltpu.make_async_remote_copy(
            src_ref=vec_send.at[other], dst_ref=vec_recv.at[me], send_sem=vs_sem.at[off], recv_sem=vr_sem.at[off],
            device_id=(other,), device_id_type=MESH)

    def start(off, carry):
        cold_copy(me, off, cold_send, cold_recv, COLD_CAP, cs_sem, cr_sem).start()
        vec_copy(off).start()
        return carry

    lax.fori_loop(1, N_DEV, start, 0)
    own_rows = pl.ds(pl.multiple_of(me * COLD_CAP, COLD_CAP), COLD_CAP)
    own_cold = pltpu.make_async_copy(cold_send.at[own_rows], cold_recv.at[own_rows], own_sem.at[0])
    own_cold.start()
    own_vec = pltpu.make_async_copy(vec_send.at[me], vec_recv.at[me], own_sem.at[2])
    own_vec.start()
    own_hot = pltpu.make_async_copy(hot_send, hot_block(0), own_sem.at[1])

    @pl.when(me == 0)
    def _():
        own_hot.start()

    @pl.when((me >= 2) & (me < 6))
    def _():
        def onward(k):
            src = relay_ids(me, k)
            return pltpu.make_async_remote_copy(
                src_ref=relay.at[k], dst_ref=hot_block(src), send_sem=fs_sem.at[k], recv_sem=hr_sem.at[src],
                device_id=(0,), device_id_type=MESH)

        for k in reversed(range(N_RELAY)):
            pltpu.make_async_copy(relay.at[k], relay.at[k], rr_sem.at[k]).wait()
            onward(k).start()
        for k in range(N_RELAY):
            onward(k).wait_send()

    @pl.when(is_near)
    def _():
        direct().wait_send()

    for dev, via, k in far:
        @pl.when(me == dev)
        def _(via=via, k=k):
            to_relay(via, k).wait_send()

    def finish(off, carry):
        cold_copy(me, off, cold_send, cold_recv, COLD_CAP, cs_sem, cr_sem).wait()
        vec_copy(off).wait()
        return carry

    lax.fori_loop(1, N_DEV, finish, 0)
    own_cold.wait()
    own_vec.wait()

    @pl.when(me == 0)
    def _():
        own_hot.wait()

        def arrived(dev, carry):
            pltpu.make_async_copy(hot_block(dev), hot_block(dev), hr_sem.at[dev]).wait()
            return carry

        lax.fori_loop(1, N_DEV, arrived, 0)


def return_exchange(hot_send, cold_send, vec_send):
    width = hot_send.shape[1]
    dma = pltpu.SemaphoreType.DMA
    return pl.pallas_call(
        return_kernel,
        out_shape=(jax.ShapeDtypeStruct((N_DEV * HOT_CAP, width), jnp.bfloat16),
                   jax.ShapeDtypeStruct((N_DEV * COLD_CAP, width), jnp.bfloat16),
                   jax.ShapeDtypeStruct(vec_send.shape, jnp.float32)),
        in_specs=[pl.BlockSpec(memory_space=pl.ANY)] * 3,
        out_specs=(pl.BlockSpec(memory_space=pl.ANY),) * 3,
        scratch_shapes=[pltpu.VMEM((N_RELAY, HOT_CAP, width), jnp.bfloat16),
                        dma, dma((N_DEV,)), dma((N_RELAY,)), dma((N_RELAY,)), dma((N_DEV,)), dma((N_DEV,)),
                        dma((N_DEV,)), dma((N_DEV,)), dma((3,))],
        compiler_params=pltpu.CompilerParams(collective_id=3, has_side_effects=True),
        cost_estimate=pl.CostEstimate(flops=60_000_000_000, bytes_accessed=30_000_000, transcendentals=0),
        name="return_exchange",
    )(hot_send, cold_send, vec_send)


GRAD_TILE = 512


def weight_grad_kernel(hidden_ref, attn_ref, g_ref, out_ref):
    step = pl.program_id(0)
    dims = (((0,), (0,)), ((), ()))

    @pl.when(step < QKV // GRAD_TILE)
    def _():
        out_ref[...] = lax.dot_general(hidden_ref[...], g_ref[...], dims, preferred_element_type=jnp.float32)

    @pl.when(step >= QKV // GRAD_TILE)
    def _():
        out_ref[...] = lax.dot_general(attn_ref[...], g_ref[...], dims, preferred_element_type=jnp.float32)


def weight_grads(hidden, attn_b, grads):
    tokens, width = hidden.shape
    return pl.pallas_call(
        weight_grad_kernel,
        grid=(WCOLS // GRAD_TILE,),
        out_shape=jax.ShapeDtypeStruct((width, WCOLS), jnp.float32),
        in_specs=[pl.BlockSpec((tokens, width), lambda j: (0, 0)),
                  pl.BlockSpec((tokens, width), lambda j: (0, 0)),
                  pl.BlockSpec((tokens, GRAD_TILE), lambda j: (0, j))],
        out_specs=pl.BlockSpec((width, GRAD_TILE), lambda j: (0, j)),
        compiler_params=pltpu.CompilerParams(vmem_limit_bytes=40 * 1024 * 1024),
        cost_estimate=pl.CostEstimate(flops=2 * tokens * width * WCOLS, bytes_accessed=width * WCOLS * 4, transcendentals=0),
        name="weight_grads",
    )(hidden, attn_b, grads)


def block_fwd_bwd(x_rows, grad_out, gain_vec, w_all, b_qkv):
    seq_len, model_width = x_rows.shape
    w_qkv = w_all[:, :QKV]
    w_out = w_all[:, QKV:]
    n_heads, kv_heads = 16, 2
    q_group = n_heads // kv_heads
    q_width = n_heads * HEAD_DIM
    kv_width = kv_heads * HEAD_DIM
    score_scale = HEAD_DIM ** -0.5
    cos_t, sin_t = rope_tables(seq_len)
    x_full = x_rows.astype(jnp.float32)
    inv_rms = lax.rsqrt(jnp.mean(x_full * x_full, axis=-1, keepdims=True) + NORM_EPS)
    x_norm = x_full * inv_rms
    gain_f = gain_vec.astype(jnp.float32)
    hidden = (x_norm * gain_f).astype(jnp.bfloat16)
    lin = jnp.dot(hidden, w_qkv, preferred_element_type=jnp.float32) + b_qkv.astype(jnp.float32)
    q_lin = lin[:, :q_width]
    k_lin = lin[:, q_width:q_width + kv_width]
    v_lin = lin[:, q_width + kv_width:]
    q_rot = rotate(q_lin.reshape(seq_len, n_heads, HEAD_DIM), cos_t, sin_t).astype(jnp.bfloat16)
    q_rot = q_rot.reshape(seq_len, kv_heads, q_group, HEAD_DIM)
    k_rot = rotate(k_lin.reshape(seq_len, kv_heads, HEAD_DIM), cos_t, sin_t).astype(jnp.bfloat16)
    v_val = v_lin.astype(jnp.bfloat16).reshape(seq_len, kv_heads, HEAD_DIM)
    scores = jnp.einsum("qkgd,skd->kgqs", q_rot, k_rot, preferred_element_type=jnp.float32) * score_scale
    causal = jnp.arange(seq_len)[:, None] >= jnp.arange(seq_len)[None, :]
    scores = jnp.where(causal, scores, MASK_VALUE)
    prob_f = jax.nn.softmax(scores, axis=-1)
    prob_b = prob_f.astype(jnp.bfloat16)
    attn_out = jnp.einsum("kgqs,skd->qkgd", prob_b, v_val, preferred_element_type=jnp.float32)
    attn_b = attn_out.astype(jnp.bfloat16).reshape(seq_len, q_width)
    proj_out = jnp.dot(attn_b, w_out, preferred_element_type=jnp.float32)
    block_out = (x_full + proj_out).astype(jnp.bfloat16)

    d_attn = jnp.einsum("lo,io->li", grad_out, w_out, preferred_element_type=jnp.float32)
    d_attn = d_attn.astype(jnp.bfloat16).reshape(seq_len, kv_heads, q_group, HEAD_DIM)
    d_probs = jnp.einsum("qkgd,skd->kgqs", d_attn, v_val, preferred_element_type=jnp.float32)
    d_val = jnp.einsum("kgqs,qkgd->skd", prob_b, d_attn, preferred_element_type=jnp.float32)
    d_scores = prob_f * (d_probs - jnp.sum(d_probs * prob_f, axis=-1, keepdims=True))
    d_scores = (d_scores * score_scale).astype(jnp.bfloat16)
    d_qrot = jnp.einsum("kgqs,skd->qkgd", d_scores, k_rot, preferred_element_type=jnp.float32)
    d_krot = jnp.einsum("kgqs,qkgd->skd", d_scores, q_rot, preferred_element_type=jnp.float32)
    d_query = rotate_back(d_qrot.reshape(seq_len, n_heads, HEAD_DIM), cos_t, sin_t).reshape(seq_len, q_width)
    d_key = rotate_back(d_krot, cos_t, sin_t).reshape(seq_len, kv_width)
    d_value = d_val.reshape(seq_len, kv_width)
    d_lin = jnp.concatenate([d_query, d_key, d_value], axis=1)
    grad_b = jnp.sum(d_lin, axis=0)
    d_lin_b = d_lin.astype(jnp.bfloat16)
    grad_w = weight_grads(hidden, attn_b, jnp.concatenate([d_lin_b, grad_out], axis=1))
    d_hidden = jnp.einsum("lo,io->li", d_lin_b, w_qkv, preferred_element_type=jnp.float32)
    grad_gain = jnp.sum(d_hidden * x_norm, axis=0)
    d_norm = d_hidden * gain_f
    d_x = grad_out.astype(jnp.float32) + inv_rms * (d_norm - x_norm * jnp.mean(d_norm * x_norm, axis=-1, keepdims=True))
    return block_out, d_x, grad_w, grad_gain, grad_b


def solution(mesh):
    row_spec = P("fsdp", None)
    vec_spec = P("fsdp")
    act_spec = P("fsdp", None, None)
    weight_specs = (vec_spec, row_spec, vec_spec, row_spec, vec_spec, row_spec, vec_spec, row_spec)
    in_specs = (row_spec, act_spec, row_spec) + weight_specs
    out_specs = (act_spec, row_spec) + weight_specs

    def device_step(tok_ids, grad_out, table_part, gain_part, wq_part, bq_part, wk_part, bk_part, wv_part, bv_part, wo_part):
        rows_dev, model_width = table_part.shape
        seq_len = tok_ids.shape[1]
        me = lax.axis_index("fsdp")
        first_row = me * rows_dev
        w_all = lax.all_gather(jnp.concatenate([wq_part, wk_part, wv_part, wo_part], axis=1), "fsdp", axis=0, tiled=True)

        vec_part = jnp.concatenate([gain_part, bq_part, bk_part, bv_part]).astype(jnp.float32)
        block = jnp.concatenate([tok_ids.reshape(-1).astype(jnp.float32), jnp.pad(vec_part, (0, 1024 - 256 - 144))])
        gathered = small_gather(block.reshape(8, 128)).reshape(N_DEV, 1024)
        all_ids = gathered[:, :seq_len].astype(jnp.int32)
        vecs = gathered[:, seq_len:seq_len + 144].astype(jnp.bfloat16)
        gain_full = vecs[:, :64].reshape(-1)
        b_qkv = jnp.concatenate([vecs[:, 64:128].reshape(-1), vecs[:, 128:136].reshape(-1), vecs[:, 136:144].reshape(-1)])

        owner = all_ids // rows_dev
        before = (jnp.arange(seq_len)[:, None] < jnp.arange(seq_len)[None, :]).astype(jnp.bfloat16)
        counts = jnp.sum((owner[:, :, None] == jnp.arange(N_DEV)).astype(jnp.int32), axis=1)
        overflow = (jnp.max(counts[:, 0]) > HOT_CAP) | (jnp.max(counts[:, 1:]) > COLD_CAP)

        def slot_rows(mask, values, cap):
            rank = jnp.dot(mask.astype(jnp.bfloat16), before, preferred_element_type=jnp.float32).astype(jnp.int32)
            hit = mask[:, None, :] & (rank[:, None, :] == jnp.arange(cap)[None, :, None])
            return jnp.sum(jnp.where(hit, values[:, None, :] + 1, 0), axis=2).reshape(-1) - 1

        hot_rows = slot_rows(owner == 0, all_ids, HOT_CAP)
        cold_rows = slot_rows((owner == me) & (owner > 0), all_ids - first_row, COLD_CAP)
        hot_send = jnp.take(table_part, jnp.maximum(hot_rows, 0), axis=0)
        cold_send = jnp.take(table_part, jnp.maximum(cold_rows, 0), axis=0)
        hot_recv, cold_recv = lookup_exchange(hot_send, cold_send)

        my_ids = tok_ids.reshape(-1)
        my_owner = my_ids // rows_dev
        same = (my_owner[:, None] == my_owner[None, :]) & (jnp.arange(seq_len)[None, :] < jnp.arange(seq_len)[:, None])
        my_rank = jnp.sum(same.astype(jnp.int32), axis=1)
        hot_slot = jnp.where(my_owner == 0, my_rank, -1)
        cold_slot = jnp.where(my_owner > 0, my_owner * COLD_CAP + my_rank, -1)
        hot_pick = (hot_slot[:, None] == jnp.arange(HOT_CAP)[None, :]).astype(jnp.bfloat16)
        cold_pick = (cold_slot[:, None] == jnp.arange(N_DEV * COLD_CAP)[None, :]).astype(jnp.bfloat16)

        def rows_fast():
            picked = jnp.dot(hot_pick, hot_recv, preferred_element_type=jnp.float32)
            picked = picked + jnp.dot(cold_pick, cold_recv, preferred_element_type=jnp.float32)
            return picked.astype(jnp.bfloat16)

        def rows_dense():
            local_idx = all_ids - first_row
            is_owned = (local_idx >= 0) & (local_idx < rows_dev)
            looked = jnp.take(table_part, jnp.where(is_owned, local_idx, 0), axis=0)
            looked = jnp.where(is_owned[..., None], looked, jnp.zeros((), jnp.bfloat16))
            return lax.psum_scatter(looked, "fsdp", scatter_dimension=0)

        x_rows = lax.cond(overflow, rows_dense, rows_fast)
        g_rows = grad_out.reshape(seq_len, model_width)
        block_out, d_x, grad_w, grad_gain, grad_b = block_fwd_bwd(x_rows, g_rows, gain_full, w_all, b_qkv)
        w_red = lax.psum_scatter(grad_w, "fsdp", scatter_dimension=0, tiled=True)

        dx_b = d_x.astype(jnp.bfloat16)
        tdims = (((0,), (0,)), ((), ()))
        hot_back = lax.dot_general(hot_pick, dx_b, tdims, preferred_element_type=jnp.float32).astype(jnp.bfloat16)
        cold_back = lax.dot_general(cold_pick, dx_b, tdims, preferred_element_type=jnp.float32).astype(jnp.bfloat16)
        vec_grad = jnp.concatenate(
            [grad_gain.reshape(N_DEV, 64), grad_b[:2048].reshape(N_DEV, 64), grad_b[2048:2304].reshape(N_DEV, 8),
             grad_b[2304:].reshape(N_DEV, 8), jnp.zeros((N_DEV, 1024 - 144), jnp.float32)], axis=1)
        hot_sum, cold_sum, vec_sum = return_exchange(hot_back, cold_back, vec_grad.reshape(N_DEV, 8, 128))

        def table_fast():
            hot_idx = jnp.where((me == 0) & (hot_rows >= 0), hot_rows, rows_dev)
            cold_idx = jnp.where(cold_rows >= 0, cold_rows, rows_dev)
            total = jnp.zeros((rows_dev, model_width), jnp.float32)
            total = total.at[hot_idx].add(hot_sum.astype(jnp.float32), mode="drop")
            total = total.at[cold_idx].add(cold_sum.astype(jnp.float32), mode="drop")
            return total.astype(jnp.bfloat16)

        def table_dense():
            local_idx = all_ids - first_row
            is_owned = (local_idx >= 0) & (local_idx < rows_dev)
            all_dx = lax.all_gather(d_x, "fsdp")
            seg_idx = jnp.where(is_owned, local_idx, rows_dev)
            total = jax.ops.segment_sum(all_dx.reshape(-1, model_width), seg_idx.reshape(-1), num_segments=rows_dev)
            return total.astype(jnp.bfloat16)

        grad_table = lax.cond(overflow, table_dense, table_fast)
        v_red = jnp.sum(vec_sum.reshape(N_DEV, 1024), axis=0)
        return (block_out[None], grad_table, v_red[:64], w_red[:, :2048], v_red[64:128], w_red[:, 2048:2304],
                v_red[128:136], w_red[:, 2304:2560], v_red[136:144], w_red[:, 2560:])

    return jax.shard_map(device_step, mesh=mesh, in_specs=in_specs, out_specs=out_specs, check_vma=False)
```

```python
import functools

import jax
import jax.numpy as jnp
from jax import lax
from jax.experimental import pallas as pl
from jax.experimental.pallas import tpu as pltpu
from jax.sharding import PartitionSpec as P

HEAD_DIM = 128
ROPE_THETA = 1.0e6
NORM_EPS = 1e-6
MASK_VALUE = -1e30
N_DEV = 32
HOT_CAP = 176
COLD_CAP = 16
QKV = 2560
WCOLS = 4608
MESH = pl.DeviceIdType.MESH


RELAYS = {2: (26, 18, 10, 6), 4: (28, 20, 12, 14), 8: (30, 22)}
N_RELAY = 4
RELAY_STEPS = (6, 9, 12, 15)


def far_blocks():
    out = []
    for k in range(N_RELAY):
        for via, ends in RELAYS.items():
            if k < len(ends):
                out.extend((ends[k] + core, via + core, k) for core in range(2))
    return out


def near_blocks():
    return [24, 25, 16, 17, 8, 9, 2, 3, 4, 5, 1]


def enter_all(me):
    barrier = pltpu.get_barrier_semaphore()

    def tell(off, carry):
        pl.semaphore_signal(barrier, inc=1, device_id=(lax.rem(me + off, N_DEV),), device_id_type=MESH)
        return carry

    lax.fori_loop(1, N_DEV, tell, 0)
    pl.semaphore_wait(barrier, N_DEV - 1)


def small_gather_kernel(src, dst, send_sem, recv_sem, own_sem):
    me = lax.axis_index("fsdp")
    enter_all(me)

    def copy(off):
        return pltpu.make_async_remote_copy(
            src_ref=src, dst_ref=dst.at[me], send_sem=send_sem.at[off], recv_sem=recv_sem.at[off],
            device_id=(lax.rem(me + off, N_DEV),), device_id_type=MESH)

    def start(off, carry):
        copy(off).start()
        return carry

    def finish(off, carry):
        copy(off).wait()
        return carry

    lax.fori_loop(1, N_DEV, start, 0)
    own = pltpu.make_async_copy(src, dst.at[me], own_sem)
    own.start()
    lax.fori_loop(1, N_DEV, finish, 0)
    own.wait()


def small_gather(block):
    return pl.pallas_call(
        small_gather_kernel,
        out_shape=jax.ShapeDtypeStruct((N_DEV,) + block.shape, block.dtype),
        in_specs=[pl.BlockSpec(memory_space=pltpu.VMEM)],
        out_specs=pl.BlockSpec(memory_space=pltpu.VMEM),
        scratch_shapes=[pltpu.SemaphoreType.DMA((N_DEV,)), pltpu.SemaphoreType.DMA((N_DEV,)), pltpu.SemaphoreType.DMA],
        compiler_params=pltpu.CompilerParams(collective_id=1, has_side_effects=True),
        name="small_gather",
    )(block)


def rows_at(ref, start, rows):
    return ref.at[pl.ds(pl.multiple_of(start, 16), rows)]


def on_relays(me, body):
    for via, ends in RELAYS.items():
        for core in range(2):
            @pl.when(me == via + core)
            def _(ends=ends, core=core):
                body([end + core for end in ends])


def lookup_kernel(send, hot_recv, cold_recv, relay, hs_sem, hr_sem, rr_sem, fs_sem, cs_sem, cr_sem, own_sem):
    me = lax.axis_index("fsdp")
    enter_all(me)

    def block(dev):
        return rows_at(send, dev * HOT_CAP, HOT_CAP)

    def near_copy(dev):
        return pltpu.make_async_remote_copy(
            src_ref=block(dev), dst_ref=hot_recv, send_sem=hs_sem.at[dev], recv_sem=hr_sem,
            device_id=(dev,), device_id_type=MESH)

    def far_copy(dev, via, k):
        return pltpu.make_async_remote_copy(
            src_ref=block(dev), dst_ref=relay.at[k], send_sem=hs_sem.at[dev], recv_sem=rr_sem.at[k],
            device_id=(via,), device_id_type=MESH)

    def cold_copy(off):
        other = lax.rem(me + off, N_DEV)
        return pltpu.make_async_remote_copy(
            src_ref=rows_at(send, other * HOT_CAP, COLD_CAP), dst_ref=rows_at(cold_recv, (me - 1) * COLD_CAP, COLD_CAP),
            send_sem=cs_sem.at[off], recv_sem=cr_sem.at[off], device_id=(other,), device_id_type=MESH)

    def cold_from(off):
        src = lax.rem(me - off + N_DEV, N_DEV)
        return src, pltpu.make_async_copy(
            rows_at(send, 0, COLD_CAP), rows_at(cold_recv, jnp.maximum(src - 1, 0) * COLD_CAP, COLD_CAP), cr_sem.at[off])

    own_hot = pltpu.make_async_copy(block(0), hot_recv, own_sem.at[0])
    own_cold = pltpu.make_async_copy(
        rows_at(send, me * HOT_CAP, COLD_CAP), rows_at(cold_recv, jnp.maximum(me - 1, 0) * COLD_CAP, COLD_CAP), own_sem.at[1])

    @pl.when(me == 0)
    def _():
        far, near = far_blocks(), near_blocks()
        for dev, via, k in far[:6]:
            far_copy(dev, via, k).start()
        for dev in near[:4]:
            near_copy(dev).start()
        for dev, via, k in far[6:]:
            far_copy(dev, via, k).start()
        for dev in near[4:]:
            near_copy(dev).start()
        own_hot.start()

    @pl.when(me != 0)
    def _():
        def start(off, carry):
            cold_copy(off).start()
            return carry

        lax.fori_loop(1, N_DEV, start, 0)
        own_cold.start()

    def pass_on(ends):
        def onward(k):
            return pltpu.make_async_remote_copy(
                src_ref=relay.at[k], dst_ref=hot_recv, send_sem=fs_sem.at[k], recv_sem=hr_sem,
                device_id=(ends[k],), device_id_type=MESH)

        for k in range(len(ends)):
            pltpu.make_async_copy(relay.at[k], relay.at[k], rr_sem.at[k]).wait()
            onward(k).start()
        for k in range(len(ends)):
            onward(k).wait_send()

    on_relays(me, pass_on)

    def arrived(off, carry):
        src, copy = cold_from(off)

        @pl.when(src != 0)
        def _():
            copy.wait()

        return carry

    lax.fori_loop(1, N_DEV, arrived, 0)

    @pl.when(me == 0)
    def _():
        own_hot.wait()
        for dev, via, k in far_blocks():
            far_copy(dev, via, k).wait_send()
        for dev in near_blocks():
            near_copy(dev).wait_send()

    @pl.when(me != 0)
    def _():
        pltpu.make_async_copy(hot_recv, hot_recv, hr_sem).wait()

        def sent(off, carry):
            cold_copy(off).wait_send()
            return carry

        lax.fori_loop(1, N_DEV, sent, 0)
        own_cold.wait()


def lookup_exchange(send):
    width = send.shape[1]
    dma = pltpu.SemaphoreType.DMA
    return pl.pallas_call(
        lookup_kernel,
        out_shape=(jax.ShapeDtypeStruct((HOT_CAP, width), jnp.bfloat16),
                   jax.ShapeDtypeStruct(((N_DEV - 1) * COLD_CAP, width), jnp.bfloat16)),
        in_specs=[pl.BlockSpec(memory_space=pl.ANY)],
        out_specs=(pl.BlockSpec(memory_space=pl.ANY),) * 2,
        scratch_shapes=[pltpu.VMEM((N_RELAY, HOT_CAP, width), jnp.bfloat16),
                        dma((N_DEV,)), dma, dma((N_RELAY,)), dma((N_RELAY,)), dma((N_DEV,)), dma((N_DEV,)), dma((2,))],
        compiler_params=pltpu.CompilerParams(collective_id=2, has_side_effects=True),
        cost_estimate=pl.CostEstimate(flops=60_000_000_000, bytes_accessed=30_000_000, transcendentals=0),
        name="lookup_exchange",
    )(send)


def return_kernel(hot_send, cold_send, vec_send, own, oth, recv, vec_recv, out, relay,
                  held, got0, send1, keep1, got1, send2, keep2, got2, send3, keep3, got3,
                  held_sem, s0_sem, r0_sem, s1_sem, r1_sem, s2_sem, r2_sem, s3_sem, r3_sem, hs_sem, hr_sem, rr_sem, fs_sem, cs_sem, cr_sem, vs_sem, vr_sem, own_sem):
    me = lax.axis_index("fsdp")
    enter_all(me)

    def block(dev):
        return rows_at(recv, dev * HOT_CAP, HOT_CAP)

    def near_copy(dev):
        return pltpu.make_async_remote_copy(
            src_ref=hot_send, dst_ref=block(dev), send_sem=hs_sem, recv_sem=hr_sem.at[dev],
            device_id=(0,), device_id_type=MESH)

    def far_copy(via, k):
        return pltpu.make_async_remote_copy(
            src_ref=hot_send, dst_ref=relay.at[k], send_sem=hs_sem, recv_sem=rr_sem.at[k],
            device_id=(via,), device_id_type=MESH)

    def vec_copy(off):
        other = lax.rem(me + off, N_DEV)
        return pltpu.make_async_remote_copy(
            src_ref=vec_send.at[other], dst_ref=vec_recv.at[me], send_sem=vs_sem.at[off], recv_sem=vr_sem.at[off],
            device_id=(other,), device_id_type=MESH)

    def cold_copy(off):
        other = lax.rem(me + off, N_DEV)
        return other, pltpu.make_async_remote_copy(
            src_ref=rows_at(cold_send, jnp.maximum(other - 1, 0) * COLD_CAP, COLD_CAP),
            dst_ref=rows_at(recv, me * HOT_CAP, COLD_CAP),
            send_sem=cs_sem.at[off], recv_sem=cr_sem.at[off], device_id=(other,), device_id_type=MESH)

    def cold_from(off):
        src = lax.rem(me - off + N_DEV, N_DEV)
        return pltpu.make_async_copy(
            rows_at(cold_send, 0, COLD_CAP), rows_at(recv, src * HOT_CAP, COLD_CAP), cr_sem.at[off])

    own_hot = pltpu.make_async_copy(hot_send, block(0), own_sem.at[0])
    own_cold = pltpu.make_async_copy(
        rows_at(cold_send, jnp.maximum(me - 1, 0) * COLD_CAP, COLD_CAP), rows_at(recv, me * HOT_CAP, COLD_CAP), own_sem.at[1])
    own_vec = pltpu.make_async_copy(vec_send.at[me], vec_recv.at[me], own_sem.at[2])

    for dev in near_blocks():
        @pl.when(me == dev)
        def _(dev=dev):
            near_copy(dev).start()

    for dev, via, k in far_blocks():
        @pl.when(me == dev)
        def _(via=via, k=k):
            far_copy(via, k).start()

    def start(off, carry):
        other, copy = cold_copy(off)

        @pl.when(other != 0)
        def _():
            copy.start()

        vec_copy(off).start()
        return carry

    lax.fori_loop(1, N_DEV, start, 0)
    own_vec.start()

    @pl.when(me == 0)
    def _():
        own_hot.start()

    @pl.when(me != 0)
    def _():
        own_cold.start()

    groups, half, width = own.shape
    core, x, y, z = lax.rem(me, 2), lax.rem(me // 2, 2), lax.rem(me // 4, 2), me // 8
    first = jnp.where(core == 0, x, y)
    second = jnp.where(core == 0, y, x)
    span = jnp.where(core == 0, 2, 4)
    near1 = me + span * (1 - 2 * first)
    near2 = me + (6 - span) * (1 - 2 * second)
    f32, bf16 = jnp.float32, jnp.bfloat16

    def part(size, index):
        return pl.ds(pl.multiple_of(index * size, size), size)

    def to(src, dst, send_sem, recv_sem, dev):
        return pltpu.make_async_remote_copy(src_ref=src, dst_ref=dst, send_sem=send_sem, recv_sem=recv_sem,
                                            device_id=(dev,), device_id_type=MESH)

    def copy0(g):
        return to(oth.at[g], got0.at[g], s0_sem, r0_sem.at[g], me + 1 - 2 * core)

    def load(g):
        return pltpu.make_async_copy(own.at[g], held.at[lax.rem(g, 2)], held_sem.at[lax.rem(g, 2)])

    def copy1(g):
        return to(send1.at[g], got1.at[g], s1_sem, r1_sem.at[g], near1)

    def copy2(g):
        return to(send2.at[g], got2.at[g], s2_sem, r2_sem.at[g], near2)

    def copy3(g, dz):
        peer = lax.rem(z + dz, 4)
        return to(send3.at[g, dz - 1], got3.at[g, dz - 1], s3_sem, r3_sem.at[g, dz - 1], me + 8 * (peer - z))

    load(0).start()
    load(1).start()

    def start0(g, carry):
        copy0(g).start()
        return carry

    lax.fori_loop(0, groups, start0, 0)

    def stage(lag, step, body):
        g = step - lag

        @pl.when((g >= 0) & (g < groups))
        def _():
            body(g, lax.rem(g + 3, 3))

    def across_core(g, slot):
        copy0(g).wait_recv()
        load(g).wait()
        here = held.at[lax.rem(g, 2)]
        for sent in range(2):
            rows = part(half // 2, 1 - first if sent else first)
            total = here[rows, :] + got0[g, rows, :].astype(f32)
            if sent:
                send1[g] = total.astype(bf16)
            else:
                keep1[slot] = total
        copy1(g).start()

        @pl.when(g + 2 < groups)
        def _():
            load(g + 2).start()

    def across_first(g, slot):
        copy1(g).wait_recv()
        for sent in range(2):
            rows = part(half // 4, 1 - second if sent else second)
            total = keep1[slot, rows, :] + got1[g, rows, :].astype(f32)
            if sent:
                send2[g] = total.astype(bf16)
            else:
                keep2[slot] = total
        copy2(g).start()

    def across_second(g, slot):
        copy2(g).wait_recv()
        for dz in range(1, 4):
            rows = part(half // 16, lax.rem(z + dz, 4))
            send3[g, dz - 1] = (keep2[slot, rows, :] + got2[g, rows, :].astype(f32)).astype(bf16)
        rows = part(half // 16, z)
        keep3[slot] = keep2[slot, rows, :] + got2[g, rows, :].astype(f32)
        for dz in range(1, 4):
            copy3(g, dz).start()

    def across_z(g, slot):
        total = keep3[slot]
        for dz in range(1, 4):
            copy3(g, dz).wait_recv()
            total = total + got3[g, dz - 1].astype(f32)
        out[:, pl.ds(pl.multiple_of(g * width, width), width)] = total

    def onward(ends, k):
        return to(relay.at[k], block(ends[k]), fs_sem.at[k], hr_sem.at[ends[k]], 0)

    def run(step, carry):
        stage(0, step, across_core)
        stage(2, step, across_first)
        stage(4, step, across_second)
        stage(6, step, across_z)

        def pass_on(ends):
            for k in reversed(range(len(ends))):
                @pl.when(step == RELAY_STEPS[N_RELAY - 1 - k])
                def _(k=k):
                    pltpu.make_async_copy(relay.at[k], relay.at[k], rr_sem.at[k]).wait()
                    onward(ends, k).start()

        on_relays(me, pass_on)
        return carry

    lax.fori_loop(0, groups + 6, run, 0)

    def passed(ends):
        for k in range(len(ends)):
            onward(ends, k).wait_send()

    on_relays(me, passed)

    for buf, sem in ((got0, s0_sem), (send1, s1_sem), (send2, s2_sem), (send3, s3_sem)):
        pltpu.make_async_copy(buf, buf, sem).wait()

    def finish(off, carry):
        other, copy = cold_copy(off)

        @pl.when(other != 0)
        def _():
            copy.wait_send()

        vec_copy(off).wait()
        return carry

    lax.fori_loop(1, N_DEV, finish, 0)
    own_vec.wait()

    @pl.when(me != 0)
    def _():
        def arrived(off, carry):
            cold_from(off).wait()
            return carry

        lax.fori_loop(1, N_DEV, arrived, 0)
        own_cold.wait()
        far_copy(2, 0).wait_send()

    @pl.when(me == 0)
    def _():
        own_hot.wait()

        def arrived(dev, carry):
            pltpu.make_async_copy(block(dev), block(dev), hr_sem.at[dev]).wait()
            return carry

        lax.fori_loop(1, N_DEV, arrived, 0)


def return_exchange(hot_send, cold_send, vec_send, own, oth):
    width = hot_send.shape[1]
    groups, half, cols = own.shape
    dma = pltpu.SemaphoreType.DMA
    f32, bf16 = jnp.float32, jnp.bfloat16
    anywhere = pl.BlockSpec(memory_space=pl.ANY)
    return pl.pallas_call(
        return_kernel,
        out_shape=(jax.ShapeDtypeStruct((N_DEV * HOT_CAP, width), bf16),
                   jax.ShapeDtypeStruct(vec_send.shape, f32),
                   jax.ShapeDtypeStruct((half // 16, groups * cols), f32)),
        in_specs=[anywhere] * 5,
        out_specs=(anywhere, anywhere, pl.BlockSpec(memory_space=pltpu.VMEM)),
        scratch_shapes=[pltpu.VMEM((N_RELAY, HOT_CAP, width), bf16),
                        pltpu.VMEM((2, half, cols), f32), pltpu.VMEM((groups, half, cols), bf16),
                        pltpu.VMEM((groups, half // 2, cols), bf16), pltpu.VMEM((3, half // 2, cols), f32),
                        pltpu.VMEM((groups, half // 2, cols), bf16),
                        pltpu.VMEM((groups, half // 4, cols), bf16), pltpu.VMEM((3, half // 4, cols), f32),
                        pltpu.VMEM((groups, half // 4, cols), bf16),
                        pltpu.VMEM((groups, 3, half // 16, cols), bf16), pltpu.VMEM((3, half // 16, cols), f32),
                        pltpu.VMEM((groups, 3, half // 16, cols), bf16),
                        dma((2,)), dma, dma((groups,)), dma, dma((groups,)), dma, dma((groups,)), dma, dma((groups, 3)),
                        dma, dma((N_DEV,)), dma((N_RELAY,)), dma((N_RELAY,)), dma((N_DEV,)), dma((N_DEV,)),
                        dma((N_DEV,)), dma((N_DEV,)), dma((3,))],
        compiler_params=pltpu.CompilerParams(collective_id=3, has_side_effects=True, vmem_limit_bytes=56 * 1024 * 1024),
        cost_estimate=pl.CostEstimate(flops=60_000_000_000, bytes_accessed=60_000_000, transcendentals=0),
        name="return_exchange",
    )(hot_send, cold_send, vec_send, own, oth)


GROUP = 256
CHUNK = 64


def weight_grad_kernel(hidden_ref, attn_ref, g_ref, own_ref, oth_ref):
    step = pl.program_id(0)
    core = lax.rem(lax.axis_index("fsdp"), 2)
    dims = (((0,), (0,)), ((), ()))

    def place(lhs_ref):
        res = lax.dot_general(lhs_ref[...], g_ref[...], dims, preferred_element_type=jnp.float32)
        for mine in range(2):
            @pl.when(core == mine)
            def _(mine=mine):
                for dev in range(N_DEV):
                    z, y, x, c = dev // 8, dev // 4 % 2, dev // 2 % 2, dev % 2
                    spot = ((x * 2 + y) if c == 0 else (y * 2 + x)) * 4 + z
                    chunk = res[dev * CHUNK:(dev + 1) * CHUNK]
                    if c == mine:
                        own_ref[0, spot * CHUNK:(spot + 1) * CHUNK, :] = chunk
                    else:
                        oth_ref[0, spot * CHUNK:(spot + 1) * CHUNK, :] = chunk.astype(jnp.bfloat16)

    @pl.when(step < QKV // GROUP)
    def _():
        place(hidden_ref)

    @pl.when(step >= QKV // GROUP)
    def _():
        place(attn_ref)


def weight_grads(hidden, attn_b, grads):
    tokens, width = hidden.shape
    groups, half = WCOLS // GROUP, width // 2
    return pl.pallas_call(
        weight_grad_kernel,
        grid=(groups,),
        out_shape=(jax.ShapeDtypeStruct((groups, half, GROUP), jnp.float32),
                   jax.ShapeDtypeStruct((groups, half, GROUP), jnp.bfloat16)),
        in_specs=[pl.BlockSpec((tokens, width), lambda j: (0, 0)),
                  pl.BlockSpec((tokens, width), lambda j: (0, 0)),
                  pl.BlockSpec((tokens, GROUP), lambda j: (0, j))],
        out_specs=(pl.BlockSpec((1, half, GROUP), lambda j: (j, 0, 0)),) * 2,
        compiler_params=pltpu.CompilerParams(vmem_limit_bytes=40 * 1024 * 1024),
        cost_estimate=pl.CostEstimate(flops=2 * tokens * width * WCOLS, bytes_accessed=width * WCOLS * 3, transcendentals=0),
        name="weight_grads",
    )(hidden, attn_b, grads)


Q_GROUP = 8
KV_HEADS = 2


def turn(vector):
    return pltpu.roll(vector, HEAD_DIM // 2, 1)


def attention_kernel(q_ref, k_ref, v_ref, d_attn_ref, cos_ref, sin_ref,
                     attn_ref, dq_ref, dk_ref, dv_ref, gq_ref, gk_ref, gv_ref, k_rot, v_val, dk_sum, dv_sum):
    member = lax.rem(pl.program_id(0), Q_GROUP)
    scale = HEAD_DIM ** -0.5
    cos_t, sin_t = cos_ref[...], sin_ref[...]
    rows_t = (((1,), (1,)), ((), ()))
    cols_t = (((0,), (0,)), ((), ()))
    f32 = jnp.float32

    @pl.when(member == 0)
    def _():
        k_lin = k_ref[...]
        k_rot[...] = (k_lin * cos_t + turn(k_lin) * sin_t).astype(jnp.bfloat16)
        v_val[...] = v_ref[...].astype(jnp.bfloat16)
        dk_sum[...] = jnp.zeros_like(dk_sum)
        dv_sum[...] = jnp.zeros_like(dv_sum)

    q_lin = q_ref[...]
    q_rot = (q_lin * cos_t + turn(q_lin) * sin_t).astype(jnp.bfloat16)
    scores = lax.dot_general(q_rot, k_rot[...], rows_t, preferred_element_type=f32) * scale
    seq = scores.shape[0]
    causal = lax.broadcasted_iota(jnp.int32, (seq, seq), 0) >= lax.broadcasted_iota(jnp.int32, (seq, seq), 1)
    scores = jnp.where(causal, scores, MASK_VALUE)
    weight = jnp.exp(scores - jnp.max(scores, axis=1, keepdims=True))
    prob_f = weight / jnp.sum(weight, axis=1, keepdims=True)
    prob_b = prob_f.astype(jnp.bfloat16)
    attn_ref[...] = jnp.dot(prob_b, v_val[...], preferred_element_type=f32).astype(jnp.bfloat16)

    d_attn = d_attn_ref[...]
    d_probs = lax.dot_general(d_attn, v_val[...], rows_t, preferred_element_type=f32)
    dv_sum[...] += lax.dot_general(prob_b, d_attn, cols_t, preferred_element_type=f32)
    d_scores = prob_f * (d_probs - jnp.sum(d_probs * prob_f, axis=1, keepdims=True))
    d_scores = (d_scores * scale).astype(jnp.bfloat16)
    d_qrot = jnp.dot(d_scores, k_rot[...], preferred_element_type=f32)
    dk_sum[...] += lax.dot_general(d_scores, q_rot, cols_t, preferred_element_type=f32)
    d_query = d_qrot * cos_t - turn(d_qrot) * sin_t
    dq_ref[...] = d_query.astype(jnp.bfloat16)
    gq_ref[...] = jnp.sum(d_query, axis=0, keepdims=True)

    @pl.when(member == Q_GROUP - 1)
    def _():
        d_krot = dk_sum[...]
        d_key = d_krot * cos_t - turn(d_krot) * sin_t
        d_value = dv_sum[...]
        dk_ref[...] = d_key.astype(jnp.bfloat16)
        dv_ref[...] = d_value.astype(jnp.bfloat16)
        gk_ref[...] = jnp.sum(d_key, axis=0, keepdims=True)
        gv_ref[...] = jnp.sum(d_value, axis=0, keepdims=True)


def attention(lin, d_attn, cos_t, sin_t):
    seq = lin.shape[0]
    heads = KV_HEADS * Q_GROUP

    def cols(index):
        return pl.BlockSpec((seq, HEAD_DIM), lambda h: (0, index(h)))

    def line(index):
        return pl.BlockSpec((1, HEAD_DIM), lambda h: (0, index(h)))

    def shape(rows, width, dtype):
        return jax.ShapeDtypeStruct((rows, width), dtype)

    q_width, kv_width = heads * HEAD_DIM, KV_HEADS * HEAD_DIM
    own = lambda h: h
    group = lambda h: h // Q_GROUP
    first = lambda h: 0
    return pl.pallas_call(
        attention_kernel,
        grid=(heads,),
        in_specs=[cols(own), cols(lambda h: heads + h // Q_GROUP), cols(lambda h: heads + KV_HEADS + h // Q_GROUP),
                  cols(own), cols(first), cols(first)],
        out_specs=(cols(own), cols(own), cols(group), cols(group), line(own), line(group), line(group)),
        out_shape=(shape(seq, q_width, jnp.bfloat16), shape(seq, q_width, jnp.bfloat16),
                   shape(seq, kv_width, jnp.bfloat16), shape(seq, kv_width, jnp.bfloat16),
                   shape(1, q_width, jnp.float32), shape(1, kv_width, jnp.float32), shape(1, kv_width, jnp.float32)),
        scratch_shapes=[pltpu.VMEM((seq, HEAD_DIM), jnp.bfloat16), pltpu.VMEM((seq, HEAD_DIM), jnp.bfloat16),
                        pltpu.VMEM((seq, HEAD_DIM), jnp.float32), pltpu.VMEM((seq, HEAD_DIM), jnp.float32)],
        cost_estimate=pl.CostEstimate(flops=14 * seq * seq * q_width, bytes_accessed=10_000_000, transcendentals=heads * seq * seq),
        name="attention",
    )(lin, lin, lin, d_attn, cos_t, sin_t)


def block_fwd_bwd(x_rows, grad_out, gain_vec, w_all, b_qkv):
    seq_len = x_rows.shape[0]
    w_qkv = w_all[:, :QKV]
    w_out = w_all[:, QKV:]
    half_dim = HEAD_DIM // 2
    inv_freq = jnp.power(ROPE_THETA, -(jnp.arange(half_dim, dtype=jnp.float32) * 2.0 / HEAD_DIM))
    angles = jnp.arange(seq_len, dtype=jnp.float32)[:, None] * inv_freq[None, :]
    cos_h, sin_h = jnp.cos(angles), jnp.sin(angles)
    cos_t = jnp.concatenate([cos_h, cos_h], axis=1)
    sin_t = jnp.concatenate([-sin_h, sin_h], axis=1)
    x_full = x_rows.astype(jnp.float32)
    inv_rms = lax.rsqrt(jnp.mean(x_full * x_full, axis=-1, keepdims=True) + NORM_EPS)
    x_norm = x_full * inv_rms
    gain_f = gain_vec.astype(jnp.float32)
    hidden = (x_norm * gain_f).astype(jnp.bfloat16)
    lin = jnp.dot(hidden, w_qkv, preferred_element_type=jnp.float32) + b_qkv.astype(jnp.float32)
    d_attn = jnp.einsum("lo,io->li", grad_out, w_out, preferred_element_type=jnp.float32).astype(jnp.bfloat16)
    attn_b, dq_b, dk_b, dv_b, grad_bq, grad_bk, grad_bv = attention(lin, d_attn, cos_t, sin_t)
    proj_out = jnp.dot(attn_b, w_out, preferred_element_type=jnp.float32)
    block_out = (x_full + proj_out).astype(jnp.bfloat16)
    d_lin_b = jnp.concatenate([dq_b, dk_b, dv_b], axis=1)
    grad_w = weight_grads(hidden, attn_b, jnp.concatenate([d_lin_b, grad_out], axis=1))
    d_hidden = jnp.einsum("lo,io->li", d_lin_b, w_qkv, preferred_element_type=jnp.float32)
    grad_gain = jnp.sum(d_hidden * x_norm, axis=0)
    d_norm = d_hidden * gain_f
    d_x = grad_out.astype(jnp.float32) + inv_rms * (d_norm - x_norm * jnp.mean(d_norm * x_norm, axis=-1, keepdims=True))
    grad_b = jnp.concatenate([grad_bq[0], grad_bk[0], grad_bv[0]])
    return block_out, d_x, grad_w, grad_gain, grad_b


def solution(mesh):
    row_spec = P("fsdp", None)
    vec_spec = P("fsdp")
    act_spec = P("fsdp", None, None)
    weight_specs = (vec_spec, row_spec, vec_spec, row_spec, vec_spec, row_spec, vec_spec, row_spec)
    in_specs = (row_spec, act_spec, row_spec) + weight_specs
    out_specs = (act_spec, row_spec) + weight_specs

    def device_step(tok_ids, grad_out, table_part, gain_part, wq_part, bq_part, wk_part, bk_part, wv_part, bv_part, wo_part):
        rows_dev, model_width = table_part.shape
        seq_len = tok_ids.shape[1]
        me = lax.axis_index("fsdp")
        first_row = me * rows_dev
        w_all = lax.all_gather(jnp.concatenate([wq_part, wk_part, wv_part, wo_part], axis=1), "fsdp", axis=0, tiled=True)

        vec_part = jnp.concatenate([gain_part, bq_part, bk_part, bv_part]).astype(jnp.float32)
        block = jnp.concatenate([tok_ids.reshape(-1).astype(jnp.float32), jnp.pad(vec_part, (0, 1024 - 256 - 144))])
        gathered = small_gather(block.reshape(8, 128)).reshape(N_DEV, 1024)
        all_ids = gathered[:, :seq_len].astype(jnp.int32)
        vecs = gathered[:, seq_len:seq_len + 144].astype(jnp.bfloat16)
        gain_full = vecs[:, :64].reshape(-1)
        b_qkv = jnp.concatenate([vecs[:, 64:128].reshape(-1), vecs[:, 128:136].reshape(-1), vecs[:, 136:144].reshape(-1)])

        owner = all_ids // rows_dev
        before = (jnp.arange(seq_len)[:, None] < jnp.arange(seq_len)[None, :]).astype(jnp.bfloat16)
        counts = jnp.sum((owner[:, :, None] == jnp.arange(N_DEV)).astype(jnp.int32), axis=1)
        overflow = (jnp.max(counts[:, 0]) > HOT_CAP) | (jnp.max(counts[:, 1:]) > COLD_CAP)

        def slot_rows(mask, values, cap):
            rank = jnp.dot(mask.astype(jnp.bfloat16), before, preferred_element_type=jnp.float32).astype(jnp.int32)
            hit = mask[:, None, :] & (rank[:, None, :] == jnp.arange(cap)[None, :, None])
            return jnp.sum(jnp.where(hit, values[:, None, :] + 1, 0), axis=2).reshape(-1) - 1

        rows = slot_rows(owner == me, all_ids - first_row, HOT_CAP)
        hot_recv, cold_recv = lookup_exchange(jnp.take(table_part, jnp.maximum(rows, 0), axis=0, mode="clip"))

        my_ids = tok_ids.reshape(-1)
        my_owner = my_ids // rows_dev
        same = (my_owner[:, None] == my_owner[None, :]) & (jnp.arange(seq_len)[None, :] < jnp.arange(seq_len)[:, None])
        my_rank = jnp.sum(same.astype(jnp.int32), axis=1)
        hot_slot = jnp.where(my_owner == 0, my_rank, -1)
        cold_slot = jnp.where(my_owner > 0, (my_owner - 1) * COLD_CAP + my_rank, -1)
        hot_pick = (hot_slot[:, None] == jnp.arange(HOT_CAP)[None, :]).astype(jnp.bfloat16)
        cold_pick = (cold_slot[:, None] == jnp.arange((N_DEV - 1) * COLD_CAP)[None, :]).astype(jnp.bfloat16)

        def rows_fast():
            picked = jnp.dot(hot_pick, hot_recv, preferred_element_type=jnp.float32)
            picked = picked + jnp.dot(cold_pick, cold_recv, preferred_element_type=jnp.float32)
            return picked.astype(jnp.bfloat16)

        ring = [(i, (i + 1) % N_DEV) for i in range(N_DEV)]

        def owned_rows(step):
            local_idx = jnp.take(all_ids, lax.rem(me - step + N_DEV, N_DEV), axis=0) - first_row
            return local_idx, (local_idx >= 0) & (local_idx < rows_dev)

        def rows_ring():
            def body(step, acc):
                local_idx, is_owned = owned_rows(step)
                looked = jnp.take(table_part, jnp.where(is_owned, local_idx, 0), axis=0, mode="clip")
                acc = jnp.where(is_owned[:, None], looked, acc)
                return lax.ppermute(acc, "fsdp", ring)

            return lax.fori_loop(0, N_DEV, body, jnp.zeros((seq_len, model_width), jnp.bfloat16))

        x_rows = lax.cond(overflow, rows_ring, rows_fast)
        g_rows = grad_out.reshape(seq_len, model_width)
        block_out, d_x, grad_w, grad_gain, grad_b = block_fwd_bwd(x_rows, g_rows, gain_full, w_all, b_qkv)
        dx_b = d_x.astype(jnp.bfloat16)
        tdims = (((0,), (0,)), ((), ()))
        hot_back = lax.dot_general(hot_pick, dx_b, tdims, preferred_element_type=jnp.float32).astype(jnp.bfloat16)
        cold_back = lax.dot_general(cold_pick, dx_b, tdims, preferred_element_type=jnp.float32).astype(jnp.bfloat16)
        vec_grad = jnp.concatenate(
            [grad_gain.reshape(N_DEV, 64), grad_b[:2048].reshape(N_DEV, 64), grad_b[2048:2304].reshape(N_DEV, 8),
             grad_b[2304:].reshape(N_DEV, 8), jnp.zeros((N_DEV, 1024 - 144), jnp.float32)], axis=1)
        dx_recv, vec_sum, w_red = return_exchange(hot_back, cold_back, vec_grad.reshape(N_DEV, 8, 128), *grad_w)

        def table_fast():
            idx = jnp.where(rows >= 0, rows, rows_dev)
            total = jnp.zeros((rows_dev, model_width), jnp.float32)
            return total.at[idx].add(dx_recv.astype(jnp.float32), mode="drop").astype(jnp.bfloat16)

        def table_ring():
            def body(step, carry):
                total, moving = carry
                local_idx, is_owned = owned_rows(step)
                seg_idx = jnp.where(is_owned, local_idx, rows_dev)
                total = total.at[seg_idx].add(moving.astype(jnp.float32), mode="drop")
                return total, lax.ppermute(moving, "fsdp", ring)

            start = (jnp.zeros((rows_dev, model_width), jnp.float32), dx_b)
            return lax.fori_loop(0, N_DEV, body, start)[0].astype(jnp.bfloat16)

        grad_table = lax.cond(overflow, table_ring, table_fast)
        v_red = jnp.sum(vec_sum.reshape(N_DEV, 1024), axis=0)
        return (block_out[None], grad_table, v_red[:64], w_red[:, :2048], v_red[64:128], w_red[:, 2048:2304],
                v_red[128:136], w_red[:, 2304:2560], v_red[136:144], w_red[:, 2560:])

    return jax.shard_map(device_step, mesh=mesh, in_specs=in_specs, out_specs=out_specs, check_vma=False)
```

```python
import functools

import jax
import jax.numpy as jnp
from jax import lax
from jax.experimental import pallas as pl
from jax.experimental.pallas import tpu as pltpu
from jax.sharding import PartitionSpec as P

HEAD_DIM = 128
ROPE_THETA = 1.0e6
NORM_EPS = 1e-6
MASK_VALUE = -1e30
N_DEV = 32
HOT_CAP = 160
COLD_CAP = 16
QKV = 2560
WCOLS = 4608
MESH = pl.DeviceIdType.MESH


RELAYS = {2: (26, 18, 10, 6), 4: (28, 20, 12, 14), 8: (30, 22)}
N_RELAY = 4
RELAY_STEPS = (6, 9, 12, 15)


def far_blocks():
    out = []
    for k in range(N_RELAY):
        for via, ends in RELAYS.items():
            if k < len(ends):
                out.extend((ends[k] + core, via + core, k) for core in range(2))
    return out


def near_blocks():
    return [24, 25, 16, 17, 8, 9, 2, 3, 4, 5, 1]


def enter_all(me):
    barrier = pltpu.get_barrier_semaphore()

    def tell(off, carry):
        pl.semaphore_signal(barrier, inc=1, device_id=(lax.rem(me + off, N_DEV),), device_id_type=MESH)
        return carry

    lax.fori_loop(1, N_DEV, tell, 0)
    pl.semaphore_wait(barrier, N_DEV - 1)


def small_gather_kernel(src, dst, send_sem, recv_sem, own_sem):
    me = lax.axis_index("fsdp")
    enter_all(me)

    def copy(off):
        return pltpu.make_async_remote_copy(
            src_ref=src, dst_ref=dst.at[me], send_sem=send_sem.at[off], recv_sem=recv_sem.at[off],
            device_id=(lax.rem(me + off, N_DEV),), device_id_type=MESH)

    def start(off, carry):
        copy(off).start()
        return carry

    def finish(off, carry):
        copy(off).wait()
        return carry

    lax.fori_loop(1, N_DEV, start, 0)
    own = pltpu.make_async_copy(src, dst.at[me], own_sem)
    own.start()
    lax.fori_loop(1, N_DEV, finish, 0)
    own.wait()


def small_gather(block):
    return pl.pallas_call(
        small_gather_kernel,
        out_shape=jax.ShapeDtypeStruct((N_DEV,) + block.shape, block.dtype),
        in_specs=[pl.BlockSpec(memory_space=pltpu.VMEM)],
        out_specs=pl.BlockSpec(memory_space=pltpu.VMEM),
        scratch_shapes=[pltpu.SemaphoreType.DMA((N_DEV,)), pltpu.SemaphoreType.DMA((N_DEV,)), pltpu.SemaphoreType.DMA],
        compiler_params=pltpu.CompilerParams(collective_id=1, has_side_effects=True),
        name="small_gather",
    )(block)


def rows_at(ref, start, rows):
    return ref.at[pl.ds(pl.multiple_of(start, 16), rows)]


def on_relays(me, body):
    for via, ends in RELAYS.items():
        for core in range(2):
            @pl.when(me == via + core)
            def _(ends=ends, core=core):
                body([end + core for end in ends])


def lookup_kernel(send, hot_recv, cold_recv, relay, hs_sem, hr_sem, rr_sem, fs_sem, cs_sem, cr_sem, own_sem):
    me = lax.axis_index("fsdp")
    enter_all(me)

    def block(dev):
        return rows_at(send, dev * HOT_CAP, HOT_CAP)

    def near_copy(dev):
        return pltpu.make_async_remote_copy(
            src_ref=block(dev), dst_ref=hot_recv, send_sem=hs_sem.at[dev], recv_sem=hr_sem,
            device_id=(dev,), device_id_type=MESH)

    def far_copy(dev, via, k):
        return pltpu.make_async_remote_copy(
            src_ref=block(dev), dst_ref=relay.at[k], send_sem=hs_sem.at[dev], recv_sem=rr_sem.at[k],
            device_id=(via,), device_id_type=MESH)

    def cold_copy(off):
        other = lax.rem(me + off, N_DEV)
        return pltpu.make_async_remote_copy(
            src_ref=rows_at(send, other * HOT_CAP, COLD_CAP), dst_ref=rows_at(cold_recv, (me - 1) * COLD_CAP, COLD_CAP),
            send_sem=cs_sem.at[off], recv_sem=cr_sem.at[off], device_id=(other,), device_id_type=MESH)

    def cold_from(off):
        src = lax.rem(me - off + N_DEV, N_DEV)
        return src, pltpu.make_async_copy(
            rows_at(send, 0, COLD_CAP), rows_at(cold_recv, jnp.maximum(src - 1, 0) * COLD_CAP, COLD_CAP), cr_sem.at[off])

    own_hot = pltpu.make_async_copy(block(0), hot_recv, own_sem.at[0])
    own_cold = pltpu.make_async_copy(
        rows_at(send, me * HOT_CAP, COLD_CAP), rows_at(cold_recv, jnp.maximum(me - 1, 0) * COLD_CAP, COLD_CAP), own_sem.at[1])

    @pl.when(me == 0)
    def _():
        far, near = far_blocks(), near_blocks()
        for dev, via, k in far[:6]:
            far_copy(dev, via, k).start()
        for dev in near[:4]:
            near_copy(dev).start()
        for dev, via, k in far[6:]:
            far_copy(dev, via, k).start()
        for dev in near[4:]:
            near_copy(dev).start()
        own_hot.start()

    @pl.when(me != 0)
    def _():
        def start(off, carry):
            cold_copy(off).start()
            return carry

        lax.fori_loop(1, N_DEV, start, 0)
        own_cold.start()

    def pass_on(ends):
        def onward(k):
            return pltpu.make_async_remote_copy(
                src_ref=relay.at[k], dst_ref=hot_recv, send_sem=fs_sem.at[k], recv_sem=hr_sem,
                device_id=(ends[k],), device_id_type=MESH)

        for k in range(len(ends)):
            pltpu.make_async_copy(relay.at[k], relay.at[k], rr_sem.at[k]).wait()
            onward(k).start()
        for k in range(len(ends)):
            onward(k).wait_send()

    on_relays(me, pass_on)

    def arrived(off, carry):
        src, copy = cold_from(off)

        @pl.when(src != 0)
        def _():
            copy.wait()

        return carry

    lax.fori_loop(1, N_DEV, arrived, 0)

    @pl.when(me == 0)
    def _():
        own_hot.wait()
        for dev, via, k in far_blocks():
            far_copy(dev, via, k).wait_send()
        for dev in near_blocks():
            near_copy(dev).wait_send()

    @pl.when(me != 0)
    def _():
        pltpu.make_async_copy(hot_recv, hot_recv, hr_sem).wait()

        def sent(off, carry):
            cold_copy(off).wait_send()
            return carry

        lax.fori_loop(1, N_DEV, sent, 0)
        own_cold.wait()


def lookup_exchange(send):
    width = send.shape[1]
    dma = pltpu.SemaphoreType.DMA
    return pl.pallas_call(
        lookup_kernel,
        out_shape=(jax.ShapeDtypeStruct((HOT_CAP, width), jnp.bfloat16),
                   jax.ShapeDtypeStruct(((N_DEV - 1) * COLD_CAP, width), jnp.bfloat16)),
        in_specs=[pl.BlockSpec(memory_space=pl.ANY)],
        out_specs=(pl.BlockSpec(memory_space=pl.ANY),) * 2,
        scratch_shapes=[pltpu.VMEM((N_RELAY, HOT_CAP, width), jnp.bfloat16),
                        dma((N_DEV,)), dma, dma((N_RELAY,)), dma((N_RELAY,)), dma((N_DEV,)), dma((N_DEV,)), dma((2,))],
        compiler_params=pltpu.CompilerParams(collective_id=2, has_side_effects=True),
        cost_estimate=pl.CostEstimate(flops=60_000_000_000, bytes_accessed=30_000_000, transcendentals=0),
        name="lookup_exchange",
    )(send)


def return_kernel(hot_send, cold_send, vec_send, own, oth, recv, vec_recv, out, relay,
                  held, got0, send1, keep1, got1, send2, keep2, got2, send3, keep3, got3,
                  held_sem, s0_sem, r0_sem, s1_sem, r1_sem, s2_sem, r2_sem, s3_sem, r3_sem, hs_sem, hr_sem, rr_sem, fs_sem, cs_sem, cr_sem, vs_sem, vr_sem, own_sem):
    me = lax.axis_index("fsdp")
    enter_all(me)

    def block(dev):
        return rows_at(recv, dev * HOT_CAP, HOT_CAP)

    def near_copy(dev):
        return pltpu.make_async_remote_copy(
            src_ref=hot_send, dst_ref=block(dev), send_sem=hs_sem, recv_sem=hr_sem.at[dev],
            device_id=(0,), device_id_type=MESH)

    def far_copy(via, k):
        return pltpu.make_async_remote_copy(
            src_ref=hot_send, dst_ref=relay.at[k], send_sem=hs_sem, recv_sem=rr_sem.at[k],
            device_id=(via,), device_id_type=MESH)

    def vec_copy(off):
        other = lax.rem(me + off, N_DEV)
        return pltpu.make_async_remote_copy(
            src_ref=vec_send.at[other], dst_ref=vec_recv.at[me], send_sem=vs_sem.at[off], recv_sem=vr_sem.at[off],
            device_id=(other,), device_id_type=MESH)

    def cold_copy(off):
        other = lax.rem(me + off, N_DEV)
        return other, pltpu.make_async_remote_copy(
            src_ref=rows_at(cold_send, jnp.maximum(other - 1, 0) * COLD_CAP, COLD_CAP),
            dst_ref=rows_at(recv, me * HOT_CAP, COLD_CAP),
            send_sem=cs_sem.at[off], recv_sem=cr_sem.at[off], device_id=(other,), device_id_type=MESH)

    def cold_from(off):
        src = lax.rem(me - off + N_DEV, N_DEV)
        return pltpu.make_async_copy(
            rows_at(cold_send, 0, COLD_CAP), rows_at(recv, src * HOT_CAP, COLD_CAP), cr_sem.at[off])

    own_hot = pltpu.make_async_copy(hot_send, block(0), own_sem.at[0])
    own_cold = pltpu.make_async_copy(
        rows_at(cold_send, jnp.maximum(me - 1, 0) * COLD_CAP, COLD_CAP), rows_at(recv, me * HOT_CAP, COLD_CAP), own_sem.at[1])
    own_vec = pltpu.make_async_copy(vec_send.at[me], vec_recv.at[me], own_sem.at[2])

    for dev in near_blocks():
        @pl.when(me == dev)
        def _(dev=dev):
            near_copy(dev).start()

    for dev, via, k in far_blocks():
        @pl.when(me == dev)
        def _(via=via, k=k):
            far_copy(via, k).start()

    def start(off, carry):
        other, copy = cold_copy(off)

        @pl.when(other != 0)
        def _():
            copy.start()

        vec_copy(off).start()
        return carry

    lax.fori_loop(1, N_DEV, start, 0)
    own_vec.start()

    @pl.when(me == 0)
    def _():
        own_hot.start()

    @pl.when(me != 0)
    def _():
        own_cold.start()

    groups, half, width = own.shape
    core, x, y, z = lax.rem(me, 2), lax.rem(me // 2, 2), lax.rem(me // 4, 2), me // 8
    first = jnp.where(core == 0, x, y)
    second = jnp.where(core == 0, y, x)
    span = jnp.where(core == 0, 2, 4)
    near1 = me + span * (1 - 2 * first)
    near2 = me + (6 - span) * (1 - 2 * second)
    f32, bf16 = jnp.float32, jnp.bfloat16

    def part(size, index):
        return pl.ds(pl.multiple_of(index * size, size), size)

    def to(src, dst, send_sem, recv_sem, dev):
        return pltpu.make_async_remote_copy(src_ref=src, dst_ref=dst, send_sem=send_sem, recv_sem=recv_sem,
                                            device_id=(dev,), device_id_type=MESH)

    def copy0(g):
        return to(oth.at[g], got0.at[g], s0_sem, r0_sem.at[g], me + 1 - 2 * core)

    def load(g):
        return pltpu.make_async_copy(own.at[g], held.at[lax.rem(g, 2)], held_sem.at[lax.rem(g, 2)])

    def copy1(g):
        return to(send1.at[g], got1.at[g], s1_sem, r1_sem.at[g], near1)

    def copy2(g):
        return to(send2.at[g], got2.at[g], s2_sem, r2_sem.at[g], near2)

    def copy3(g, dz):
        peer = lax.rem(z + dz, 4)
        return to(send3.at[g, dz - 1], got3.at[g, dz - 1], s3_sem, r3_sem.at[g, dz - 1], me + 8 * (peer - z))

    load(0).start()
    load(1).start()

    def start0(g, carry):
        copy0(g).start()
        return carry

    lax.fori_loop(0, groups, start0, 0)

    def stage(lag, step, body):
        g = step - lag

        @pl.when((g >= 0) & (g < groups))
        def _():
            body(g, lax.rem(g + 3, 3))

    def across_core(g, slot):
        copy0(g).wait_recv()
        load(g).wait()
        here = held.at[lax.rem(g, 2)]
        for sent in range(2):
            rows = part(half // 2, 1 - first if sent else first)
            total = here[rows, :] + got0[g, rows, :].astype(f32)
            if sent:
                send1[g] = total.astype(bf16)
            else:
                keep1[slot] = total
        copy1(g).start()

        @pl.when(g + 2 < groups)
        def _():
            load(g + 2).start()

    def across_first(g, slot):
        copy1(g).wait_recv()
        for sent in range(2):
            rows = part(half // 4, 1 - second if sent else second)
            total = keep1[slot, rows, :] + got1[g, rows, :].astype(f32)
            if sent:
                send2[g] = total.astype(bf16)
            else:
                keep2[slot] = total
        copy2(g).start()

    def across_second(g, slot):
        copy2(g).wait_recv()
        for dz in range(1, 4):
            rows = part(half // 16, lax.rem(z + dz, 4))
            send3[g, dz - 1] = (keep2[slot, rows, :] + got2[g, rows, :].astype(f32)).astype(bf16)
        rows = part(half // 16, z)
        keep3[slot] = keep2[slot, rows, :] + got2[g, rows, :].astype(f32)
        for dz in range(1, 4):
            copy3(g, dz).start()

    def across_z(g, slot):
        total = keep3[slot]
        for dz in range(1, 4):
            copy3(g, dz).wait_recv()
            total = total + got3[g, dz - 1].astype(f32)
        out[:, pl.ds(pl.multiple_of(g * width, width), width)] = total

    def onward(ends, k):
        return to(relay.at[k], block(ends[k]), fs_sem.at[k], hr_sem.at[ends[k]], 0)

    def run(step, carry):
        stage(0, step, across_core)
        stage(2, step, across_first)
        stage(4, step, across_second)
        stage(6, step, across_z)

        def pass_on(ends):
            for k in reversed(range(len(ends))):
                @pl.when(step == RELAY_STEPS[N_RELAY - 1 - k])
                def _(k=k):
                    pltpu.make_async_copy(relay.at[k], relay.at[k], rr_sem.at[k]).wait()
                    onward(ends, k).start()

        on_relays(me, pass_on)
        return carry

    lax.fori_loop(0, groups + 6, run, 0)

    def passed(ends):
        for k in range(len(ends)):
            onward(ends, k).wait_send()

    on_relays(me, passed)

    for buf, sem in ((got0, s0_sem), (send1, s1_sem), (send2, s2_sem), (send3, s3_sem)):
        pltpu.make_async_copy(buf, buf, sem).wait()

    def finish(off, carry):
        other, copy = cold_copy(off)

        @pl.when(other != 0)
        def _():
            copy.wait_send()

        vec_copy(off).wait()
        return carry

    lax.fori_loop(1, N_DEV, finish, 0)
    own_vec.wait()

    @pl.when(me != 0)
    def _():
        def arrived(off, carry):
            cold_from(off).wait()
            return carry

        lax.fori_loop(1, N_DEV, arrived, 0)
        own_cold.wait()
        far_copy(2, 0).wait_send()

    @pl.when(me == 0)
    def _():
        own_hot.wait()

        def arrived(dev, carry):
            pltpu.make_async_copy(block(dev), block(dev), hr_sem.at[dev]).wait()
            return carry

        lax.fori_loop(1, N_DEV, arrived, 0)


def return_exchange(hot_send, cold_send, vec_send, own, oth):
    width = hot_send.shape[1]
    groups, half, cols = own.shape
    dma = pltpu.SemaphoreType.DMA
    f32, bf16 = jnp.float32, jnp.bfloat16
    anywhere = pl.BlockSpec(memory_space=pl.ANY)
    return pl.pallas_call(
        return_kernel,
        out_shape=(jax.ShapeDtypeStruct((N_DEV * HOT_CAP, width), bf16),
                   jax.ShapeDtypeStruct(vec_send.shape, f32),
                   jax.ShapeDtypeStruct((half // 16, groups * cols), f32)),
        in_specs=[anywhere] * 5,
        out_specs=(anywhere, anywhere, pl.BlockSpec(memory_space=pltpu.VMEM)),
        scratch_shapes=[pltpu.VMEM((N_RELAY, HOT_CAP, width), bf16),
                        pltpu.VMEM((2, half, cols), f32), pltpu.VMEM((groups, half, cols), bf16),
                        pltpu.VMEM((groups, half // 2, cols), bf16), pltpu.VMEM((3, half // 2, cols), f32),
                        pltpu.VMEM((groups, half // 2, cols), bf16),
                        pltpu.VMEM((groups, half // 4, cols), bf16), pltpu.VMEM((3, half // 4, cols), f32),
                        pltpu.VMEM((groups, half // 4, cols), bf16),
                        pltpu.VMEM((groups, 3, half // 16, cols), bf16), pltpu.VMEM((3, half // 16, cols), f32),
                        pltpu.VMEM((groups, 3, half // 16, cols), bf16),
                        dma((2,)), dma, dma((groups,)), dma, dma((groups,)), dma, dma((groups,)), dma, dma((groups, 3)),
                        dma, dma((N_DEV,)), dma((N_RELAY,)), dma((N_RELAY,)), dma((N_DEV,)), dma((N_DEV,)),
                        dma((N_DEV,)), dma((N_DEV,)), dma((3,))],
        compiler_params=pltpu.CompilerParams(collective_id=3, has_side_effects=True, vmem_limit_bytes=56 * 1024 * 1024),
        cost_estimate=pl.CostEstimate(flops=60_000_000_000, bytes_accessed=60_000_000, transcendentals=0),
        name="return_exchange",
    )(hot_send, cold_send, vec_send, own, oth)


GROUP = 256
CHUNK = 64


def weight_grad_kernel(hidden_ref, attn_ref, g_ref, own_ref, oth_ref):
    step = pl.program_id(0)
    core = lax.rem(lax.axis_index("fsdp"), 2)
    dims = (((0,), (0,)), ((), ()))

    def place(lhs_ref):
        res = lax.dot_general(lhs_ref[...], g_ref[...], dims, preferred_element_type=jnp.float32)
        for mine in range(2):
            @pl.when(core == mine)
            def _(mine=mine):
                for dev in range(N_DEV):
                    z, y, x, c = dev // 8, dev // 4 % 2, dev // 2 % 2, dev % 2
                    spot = ((x * 2 + y) if c == 0 else (y * 2 + x)) * 4 + z
                    chunk = res[dev * CHUNK:(dev + 1) * CHUNK]
                    if c == mine:
                        own_ref[0, spot * CHUNK:(spot + 1) * CHUNK, :] = chunk
                    else:
                        oth_ref[0, spot * CHUNK:(spot + 1) * CHUNK, :] = chunk.astype(jnp.bfloat16)

    @pl.when(step < QKV // GROUP)
    def _():
        place(hidden_ref)

    @pl.when(step >= QKV // GROUP)
    def _():
        place(attn_ref)


def weight_grads(hidden, attn_b, grads):
    tokens, width = hidden.shape
    groups, half = WCOLS // GROUP, width // 2
    return pl.pallas_call(
        weight_grad_kernel,
        grid=(groups,),
        out_shape=(jax.ShapeDtypeStruct((groups, half, GROUP), jnp.float32),
                   jax.ShapeDtypeStruct((groups, half, GROUP), jnp.bfloat16)),
        in_specs=[pl.BlockSpec((tokens, width), lambda j: (0, 0)),
                  pl.BlockSpec((tokens, width), lambda j: (0, 0)),
                  pl.BlockSpec((tokens, GROUP), lambda j: (0, j))],
        out_specs=(pl.BlockSpec((1, half, GROUP), lambda j: (j, 0, 0)),) * 2,
        compiler_params=pltpu.CompilerParams(vmem_limit_bytes=40 * 1024 * 1024),
        cost_estimate=pl.CostEstimate(flops=2 * tokens * width * WCOLS, bytes_accessed=width * WCOLS * 3, transcendentals=0),
        name="weight_grads",
    )(hidden, attn_b, grads)


SLOTS = 16
TILE = 128


def table_sum_kernel(low_ref, high_ref, dx_ref, row_ref, out_ref, total):
    step = pl.program_id(0)
    n_groups = HOT_CAP // SLOTS
    tiles = total.shape[0] // TILE

    def tile(index):
        return pl.ds(pl.multiple_of(index * TILE, TILE), TILE)

    @pl.when(step == 0)
    def _():
        def clear(index, carry):
            total[tile(index), :] = jnp.zeros((TILE, total.shape[1]), jnp.float32)
            return carry

        lax.fori_loop(0, tiles, clear, 0)

    @pl.when(step < n_groups)
    def _():
        dx = dx_ref[...].reshape(-1, dx_ref.shape[2])
        rows = row_ref[0]

        def add(index, carry):
            place = index * TILE + lax.broadcasted_iota(jnp.int32, (TILE, rows.shape[1]), 0)
            pick = jnp.where(place == rows, 1.0, 0.0).astype(jnp.bfloat16)
            total[tile(index), :] += jnp.dot(pick, dx, preferred_element_type=jnp.float32)
            return carry

        at = jnp.minimum(step, n_groups - 1)
        lax.fori_loop(low_ref[at], high_ref[at], add, 0)

    @pl.when(step >= n_groups)
    def _():
        out_ref[...] = total[tile(jnp.maximum(step - n_groups, 0)), :].astype(jnp.bfloat16)


def table_sum(dx_recv, rows, rows_dev):
    width = dx_recv.shape[1]
    n_groups = HOT_CAP // SLOTS
    tiles = (rows_dev + TILE - 1) // TILE
    by_group = rows.reshape(N_DEV, n_groups, SLOTS).transpose(1, 0, 2).reshape(n_groups, 1, N_DEV * SLOTS)
    valid = by_group >= 0
    low = jnp.min(jnp.where(valid, by_group, rows_dev), axis=(1, 2)) // TILE
    high = jnp.max(jnp.where(valid, by_group + TILE, 0), axis=(1, 2)) // TILE
    return pl.pallas_call(
        table_sum_kernel,
        grid_spec=pltpu.PrefetchScalarGridSpec(
            num_scalar_prefetch=2,
            grid=(n_groups + tiles,),
            in_specs=[pl.BlockSpec((N_DEV, SLOTS, width), lambda s, lo, hi: (0, jnp.minimum(s, n_groups - 1), 0)),
                      pl.BlockSpec((1, 1, N_DEV * SLOTS), lambda s, lo, hi: (jnp.minimum(s, n_groups - 1), 0, 0))],
            out_specs=pl.BlockSpec((TILE, width), lambda s, lo, hi: (jnp.maximum(s - n_groups, 0), 0)),
            scratch_shapes=[pltpu.VMEM((tiles * TILE, width), jnp.float32)]),
        out_shape=jax.ShapeDtypeStruct((rows_dev, width), jnp.bfloat16),
        compiler_params=pltpu.CompilerParams(vmem_limit_bytes=56 * 1024 * 1024),
        cost_estimate=pl.CostEstimate(flops=30_000_000_000, bytes_accessed=45_000_000, transcendentals=0),
        name="table_sum",
    )(low, high, dx_recv.reshape(N_DEV, HOT_CAP, width), by_group)


Q_GROUP = 8
KV_HEADS = 2


def turn(vector):
    return pltpu.roll(vector, HEAD_DIM // 2, 1)


def attention_kernel(q_ref, k_ref, v_ref, d_attn_ref, cos_ref, sin_ref,
                     attn_ref, dq_ref, dk_ref, dv_ref, gq_ref, gk_ref, gv_ref, k_rot, v_val, dk_sum, dv_sum):
    member = lax.rem(pl.program_id(0), Q_GROUP)
    scale = HEAD_DIM ** -0.5
    cos_t, sin_t = cos_ref[...], sin_ref[...]
    rows_t = (((1,), (1,)), ((), ()))
    cols_t = (((0,), (0,)), ((), ()))
    f32 = jnp.float32

    @pl.when(member == 0)
    def _():
        k_lin = k_ref[...]
        k_rot[...] = (k_lin * cos_t + turn(k_lin) * sin_t).astype(jnp.bfloat16)
        v_val[...] = v_ref[...].astype(jnp.bfloat16)
        dk_sum[...] = jnp.zeros_like(dk_sum)
        dv_sum[...] = jnp.zeros_like(dv_sum)

    q_lin = q_ref[...]
    q_rot = (q_lin * cos_t + turn(q_lin) * sin_t).astype(jnp.bfloat16)
    scores = lax.dot_general(q_rot, k_rot[...], rows_t, preferred_element_type=f32) * scale
    seq = scores.shape[0]
    causal = lax.broadcasted_iota(jnp.int32, (seq, seq), 0) >= lax.broadcasted_iota(jnp.int32, (seq, seq), 1)
    scores = jnp.where(causal, scores, MASK_VALUE)
    weight = jnp.exp(scores - jnp.max(scores, axis=1, keepdims=True))
    prob_f = weight / jnp.sum(weight, axis=1, keepdims=True)
    prob_b = prob_f.astype(jnp.bfloat16)
    attn_ref[...] = jnp.dot(prob_b, v_val[...], preferred_element_type=f32).astype(jnp.bfloat16)

    d_attn = d_attn_ref[...]
    d_probs = lax.dot_general(d_attn, v_val[...], rows_t, preferred_element_type=f32)
    dv_sum[...] += lax.dot_general(prob_b, d_attn, cols_t, preferred_element_type=f32)
    d_scores = prob_f * (d_probs - jnp.sum(d_probs * prob_f, axis=1, keepdims=True))
    d_scores = (d_scores * scale).astype(jnp.bfloat16)
    d_qrot = jnp.dot(d_scores, k_rot[...], preferred_element_type=f32)
    dk_sum[...] += lax.dot_general(d_scores, q_rot, cols_t, preferred_element_type=f32)
    d_query = d_qrot * cos_t - turn(d_qrot) * sin_t
    dq_ref[...] = d_query.astype(jnp.bfloat16)
    gq_ref[...] = jnp.sum(d_query, axis=0, keepdims=True)

    @pl.when(member == Q_GROUP - 1)
    def _():
        d_krot = dk_sum[...]
        d_key = d_krot * cos_t - turn(d_krot) * sin_t
        d_value = dv_sum[...]
        dk_ref[...] = d_key.astype(jnp.bfloat16)
        dv_ref[...] = d_value.astype(jnp.bfloat16)
        gk_ref[...] = jnp.sum(d_key, axis=0, keepdims=True)
        gv_ref[...] = jnp.sum(d_value, axis=0, keepdims=True)


def attention(lin, d_attn, cos_t, sin_t):
    seq = lin.shape[0]
    heads = KV_HEADS * Q_GROUP

    def cols(index):
        return pl.BlockSpec((seq, HEAD_DIM), lambda h: (0, index(h)))

    def line(index):
        return pl.BlockSpec((1, HEAD_DIM), lambda h: (0, index(h)))

    def shape(rows, width, dtype):
        return jax.ShapeDtypeStruct((rows, width), dtype)

    q_width, kv_width = heads * HEAD_DIM, KV_HEADS * HEAD_DIM
    own = lambda h: h
    group = lambda h: h // Q_GROUP
    first = lambda h: 0
    return pl.pallas_call(
        attention_kernel,
        grid=(heads,),
        in_specs=[cols(own), cols(lambda h: heads + h // Q_GROUP), cols(lambda h: heads + KV_HEADS + h // Q_GROUP),
                  cols(own), cols(first), cols(first)],
        out_specs=(cols(own), cols(own), cols(group), cols(group), line(own), line(group), line(group)),
        out_shape=(shape(seq, q_width, jnp.bfloat16), shape(seq, q_width, jnp.bfloat16),
                   shape(seq, kv_width, jnp.bfloat16), shape(seq, kv_width, jnp.bfloat16),
                   shape(1, q_width, jnp.float32), shape(1, kv_width, jnp.float32), shape(1, kv_width, jnp.float32)),
        scratch_shapes=[pltpu.VMEM((seq, HEAD_DIM), jnp.bfloat16), pltpu.VMEM((seq, HEAD_DIM), jnp.bfloat16),
                        pltpu.VMEM((seq, HEAD_DIM), jnp.float32), pltpu.VMEM((seq, HEAD_DIM), jnp.float32)],
        cost_estimate=pl.CostEstimate(flops=14 * seq * seq * q_width, bytes_accessed=10_000_000, transcendentals=heads * seq * seq),
        name="attention",
    )(lin, lin, lin, d_attn, cos_t, sin_t)


def block_fwd_bwd(x_rows, grad_out, gain_vec, w_all, b_qkv):
    seq_len = x_rows.shape[0]
    w_qkv = w_all[:, :QKV]
    w_out = w_all[:, QKV:]
    half_dim = HEAD_DIM // 2
    inv_freq = jnp.power(ROPE_THETA, -(jnp.arange(half_dim, dtype=jnp.float32) * 2.0 / HEAD_DIM))
    angles = jnp.arange(seq_len, dtype=jnp.float32)[:, None] * inv_freq[None, :]
    cos_h, sin_h = jnp.cos(angles), jnp.sin(angles)
    cos_t = jnp.concatenate([cos_h, cos_h], axis=1)
    sin_t = jnp.concatenate([-sin_h, sin_h], axis=1)
    x_full = x_rows.astype(jnp.float32)
    inv_rms = lax.rsqrt(jnp.mean(x_full * x_full, axis=-1, keepdims=True) + NORM_EPS)
    x_norm = x_full * inv_rms
    gain_f = gain_vec.astype(jnp.float32)
    hidden = (x_norm * gain_f).astype(jnp.bfloat16)
    lin = jnp.dot(hidden, w_qkv, preferred_element_type=jnp.float32) + b_qkv.astype(jnp.float32)
    d_attn = jnp.einsum("lo,io->li", grad_out, w_out, preferred_element_type=jnp.float32).astype(jnp.bfloat16)
    attn_b, dq_b, dk_b, dv_b, grad_bq, grad_bk, grad_bv = attention(lin, d_attn, cos_t, sin_t)
    proj_out = jnp.dot(attn_b, w_out, preferred_element_type=jnp.float32)
    block_out = (x_full + proj_out).astype(jnp.bfloat16)
    d_lin_b = jnp.concatenate([dq_b, dk_b, dv_b], axis=1)
    grad_w = weight_grads(hidden, attn_b, jnp.concatenate([d_lin_b, grad_out], axis=1))
    d_hidden = jnp.einsum("lo,io->li", d_lin_b, w_qkv, preferred_element_type=jnp.float32)
    grad_gain = jnp.sum(d_hidden * x_norm, axis=0)
    d_norm = d_hidden * gain_f
    d_x = grad_out.astype(jnp.float32) + inv_rms * (d_norm - x_norm * jnp.mean(d_norm * x_norm, axis=-1, keepdims=True))
    grad_b = jnp.concatenate([grad_bq[0], grad_bk[0], grad_bv[0]])
    return block_out, d_x, grad_w, grad_gain, grad_b


def solution(mesh):
    row_spec = P("fsdp", None)
    vec_spec = P("fsdp")
    act_spec = P("fsdp", None, None)
    weight_specs = (vec_spec, row_spec, vec_spec, row_spec, vec_spec, row_spec, vec_spec, row_spec)
    in_specs = (row_spec, act_spec, row_spec) + weight_specs
    out_specs = (act_spec, row_spec) + weight_specs

    def device_step(tok_ids, grad_out, table_part, gain_part, wq_part, bq_part, wk_part, bk_part, wv_part, bv_part, wo_part):
        rows_dev, model_width = table_part.shape
        seq_len = tok_ids.shape[1]
        me = lax.axis_index("fsdp")
        first_row = me * rows_dev
        w_all = lax.all_gather(jnp.concatenate([wq_part, wk_part, wv_part, wo_part], axis=1), "fsdp", axis=0, tiled=True)

        vec_part = jnp.concatenate([gain_part, bq_part, bk_part, bv_part]).astype(jnp.float32)
        block = jnp.concatenate([tok_ids.reshape(-1).astype(jnp.float32), jnp.pad(vec_part, (0, 1024 - 256 - 144))])
        gathered = small_gather(block.reshape(8, 128)).reshape(N_DEV, 1024)
        all_ids = gathered[:, :seq_len].astype(jnp.int32)
        vecs = gathered[:, seq_len:seq_len + 144].astype(jnp.bfloat16)
        gain_full = vecs[:, :64].reshape(-1)
        b_qkv = jnp.concatenate([vecs[:, 64:128].reshape(-1), vecs[:, 128:136].reshape(-1), vecs[:, 136:144].reshape(-1)])

        owner = all_ids // rows_dev
        key = all_ids * seq_len + jnp.arange(seq_len)
        counts = jnp.sum((owner[:, :, None] == jnp.arange(N_DEV)).astype(jnp.int32), axis=1)
        overflow = (jnp.max(counts[:, 0]) > HOT_CAP) | (jnp.max(counts[:, 1:]) > COLD_CAP)

        mask = owner == me
        rank = jnp.sum((mask[:, None, :] & (key[:, None, :] < key[:, :, None])).astype(jnp.int32), axis=2)
        hit = mask[:, None, :] & (rank[:, None, :] == jnp.arange(HOT_CAP)[None, :, None])
        rows = jnp.sum(jnp.where(hit, (all_ids - first_row)[:, None, :] + 1, 0), axis=2).reshape(-1) - 1
        hot_recv, cold_recv = lookup_exchange(jnp.take(table_part, jnp.maximum(rows, 0), axis=0, mode="clip"))

        my_ids = tok_ids.reshape(-1)
        my_owner = my_ids // rows_dev
        my_key = my_ids * seq_len + jnp.arange(seq_len)
        same = (my_owner[:, None] == my_owner[None, :]) & (my_key[None, :] < my_key[:, None])
        my_rank = jnp.sum(same.astype(jnp.int32), axis=1)
        hot_slot = jnp.where(my_owner == 0, my_rank, -1)
        cold_slot = jnp.where(my_owner > 0, (my_owner - 1) * COLD_CAP + my_rank, -1)
        hot_pick = (hot_slot[:, None] == jnp.arange(HOT_CAP)[None, :]).astype(jnp.bfloat16)
        cold_pick = (cold_slot[:, None] == jnp.arange((N_DEV - 1) * COLD_CAP)[None, :]).astype(jnp.bfloat16)

        def rows_fast():
            picked = jnp.dot(hot_pick, hot_recv, preferred_element_type=jnp.float32)
            picked = picked + jnp.dot(cold_pick, cold_recv, preferred_element_type=jnp.float32)
            return picked.astype(jnp.bfloat16)

        ring = [(i, (i + 1) % N_DEV) for i in range(N_DEV)]

        def owned_rows(step):
            local_idx = jnp.take(all_ids, lax.rem(me - step + N_DEV, N_DEV), axis=0) - first_row
            return local_idx, (local_idx >= 0) & (local_idx < rows_dev)

        def rows_ring():
            def body(step, acc):
                local_idx, is_owned = owned_rows(step)
                looked = jnp.take(table_part, jnp.where(is_owned, local_idx, 0), axis=0, mode="clip")
                acc = jnp.where(is_owned[:, None], looked, acc)
                return lax.ppermute(acc, "fsdp", ring)

            return lax.fori_loop(0, N_DEV, body, jnp.zeros((seq_len, model_width), jnp.bfloat16))

        x_rows = lax.cond(overflow, rows_ring, rows_fast)
        g_rows = grad_out.reshape(seq_len, model_width)
        block_out, d_x, grad_w, grad_gain, grad_b = block_fwd_bwd(x_rows, g_rows, gain_full, w_all, b_qkv)
        dx_b = d_x.astype(jnp.bfloat16)
        tdims = (((0,), (0,)), ((), ()))
        hot_back = lax.dot_general(hot_pick, dx_b, tdims, preferred_element_type=jnp.float32).astype(jnp.bfloat16)
        cold_back = lax.dot_general(cold_pick, dx_b, tdims, preferred_element_type=jnp.float32).astype(jnp.bfloat16)
        vec_grad = jnp.concatenate(
            [grad_gain.reshape(N_DEV, 64), grad_b[:2048].reshape(N_DEV, 64), grad_b[2048:2304].reshape(N_DEV, 8),
             grad_b[2304:].reshape(N_DEV, 8), jnp.zeros((N_DEV, 1024 - 144), jnp.float32)], axis=1)
        dx_recv, vec_sum, w_red = return_exchange(hot_back, cold_back, vec_grad.reshape(N_DEV, 8, 128), *grad_w)

        def table_fast():
            return table_sum(dx_recv, rows, rows_dev)

        def table_ring():
            def body(step, carry):
                total, moving = carry
                local_idx, is_owned = owned_rows(step)
                seg_idx = jnp.where(is_owned, local_idx, rows_dev)
                total = total.at[seg_idx].add(moving.astype(jnp.float32), mode="drop")
                return total, lax.ppermute(moving, "fsdp", ring)

            start = (jnp.zeros((rows_dev, model_width), jnp.float32), dx_b)
            return lax.fori_loop(0, N_DEV, body, start)[0].astype(jnp.bfloat16)

        grad_table = lax.cond(overflow, table_ring, table_fast)
        v_red = jnp.sum(vec_sum.reshape(N_DEV, 1024), axis=0)
        return (block_out[None], grad_table, v_red[:64], w_red[:, :2048], v_red[64:128], w_red[:, 2048:2304],
                v_red[128:136], w_red[:, 2304:2560], v_red[136:144], w_red[:, 2560:])

    return jax.shard_map(device_step, mesh=mesh, in_specs=in_specs, out_specs=out_specs, check_vma=False)
```

```python
import functools

import jax
import jax.numpy as jnp
from jax import lax
from jax.experimental import pallas as pl
from jax.experimental.pallas import tpu as pltpu
from jax.sharding import PartitionSpec as P

HEAD_DIM = 128
ROPE_THETA = 1.0e6
NORM_EPS = 1e-6
MASK_VALUE = -1e30
N_DEV = 32
HOT_CAP = 160
COLD_CAP = 16
QKV = 2560
WCOLS = 4608
MESH = pl.DeviceIdType.MESH


RELAYS = {2: (26, 18, 10, 6), 4: (28, 20, 12, 14), 8: (30, 22)}
N_RELAY = 4
RELAY_STEPS = (8, 11, 14, 17)


def far_blocks():
    out = []
    for k in range(N_RELAY):
        for via, ends in RELAYS.items():
            if k < len(ends):
                out.extend((ends[k] + core, via + core, k) for core in range(2))
    return out


def near_blocks():
    return [24, 25, 16, 17, 8, 9, 2, 3, 4, 5, 1]


def enter_all(me):
    barrier = pltpu.get_barrier_semaphore()

    def tell(off, carry):
        pl.semaphore_signal(barrier, inc=1, device_id=(lax.rem(me + off, N_DEV),), device_id_type=MESH)
        return carry

    lax.fori_loop(1, N_DEV, tell, 0)
    pl.semaphore_wait(barrier, N_DEV - 1)


def small_gather_kernel(src, dst, send_sem, recv_sem, own_sem):
    me = lax.axis_index("fsdp")
    enter_all(me)

    def copy(off):
        return pltpu.make_async_remote_copy(
            src_ref=src, dst_ref=dst.at[me], send_sem=send_sem.at[off], recv_sem=recv_sem.at[off],
            device_id=(lax.rem(me + off, N_DEV),), device_id_type=MESH)

    def start(off, carry):
        copy(off).start()
        return carry

    def finish(off, carry):
        copy(off).wait()
        return carry

    lax.fori_loop(1, N_DEV, start, 0)
    own = pltpu.make_async_copy(src, dst.at[me], own_sem)
    own.start()
    lax.fori_loop(1, N_DEV, finish, 0)
    own.wait()


def small_gather(block):
    return pl.pallas_call(
        small_gather_kernel,
        out_shape=jax.ShapeDtypeStruct((N_DEV,) + block.shape, block.dtype),
        in_specs=[pl.BlockSpec(memory_space=pltpu.VMEM)],
        out_specs=pl.BlockSpec(memory_space=pltpu.VMEM),
        scratch_shapes=[pltpu.SemaphoreType.DMA((N_DEV,)), pltpu.SemaphoreType.DMA((N_DEV,)), pltpu.SemaphoreType.DMA],
        compiler_params=pltpu.CompilerParams(collective_id=1, has_side_effects=True),
        name="small_gather",
    )(block)


def rows_at(ref, start, rows):
    return ref.at[pl.ds(pl.multiple_of(start, 16), rows)]


def on_relays(me, body):
    for via, ends in RELAYS.items():
        for core in range(2):
            @pl.when(me == via + core)
            def _(ends=ends, core=core):
                body([end + core for end in ends])


def lookup_kernel(send, hot_recv, cold_recv, relay, hs_sem, hr_sem, rr_sem, fs_sem, cs_sem, cr_sem, own_sem):
    me = lax.axis_index("fsdp")
    enter_all(me)

    def block(dev):
        return rows_at(send, dev * HOT_CAP, HOT_CAP)

    def near_copy(dev):
        return pltpu.make_async_remote_copy(
            src_ref=block(dev), dst_ref=hot_recv, send_sem=hs_sem.at[dev], recv_sem=hr_sem,
            device_id=(dev,), device_id_type=MESH)

    def far_copy(dev, via, k):
        return pltpu.make_async_remote_copy(
            src_ref=block(dev), dst_ref=relay.at[k], send_sem=hs_sem.at[dev], recv_sem=rr_sem.at[k],
            device_id=(via,), device_id_type=MESH)

    def cold_copy(off):
        other = lax.rem(me + off, N_DEV)
        return pltpu.make_async_remote_copy(
            src_ref=rows_at(send, other * HOT_CAP, COLD_CAP), dst_ref=rows_at(cold_recv, (me - 1) * COLD_CAP, COLD_CAP),
            send_sem=cs_sem.at[off], recv_sem=cr_sem.at[off], device_id=(other,), device_id_type=MESH)

    def cold_from(off):
        src = lax.rem(me - off + N_DEV, N_DEV)
        return src, pltpu.make_async_copy(
            rows_at(send, 0, COLD_CAP), rows_at(cold_recv, jnp.maximum(src - 1, 0) * COLD_CAP, COLD_CAP), cr_sem.at[off])

    own_hot = pltpu.make_async_copy(block(0), hot_recv, own_sem.at[0])
    own_cold = pltpu.make_async_copy(
        rows_at(send, me * HOT_CAP, COLD_CAP), rows_at(cold_recv, jnp.maximum(me - 1, 0) * COLD_CAP, COLD_CAP), own_sem.at[1])

    @pl.when(me == 0)
    def _():
        far, near = far_blocks(), near_blocks()
        for dev, via, k in far[:6]:
            far_copy(dev, via, k).start()
        for dev in near[:4]:
            near_copy(dev).start()
        for dev, via, k in far[6:]:
            far_copy(dev, via, k).start()
        for dev in near[4:]:
            near_copy(dev).start()
        own_hot.start()

    @pl.when(me != 0)
    def _():
        def start(off, carry):
            cold_copy(off).start()
            return carry

        lax.fori_loop(1, N_DEV, start, 0)
        own_cold.start()

    def pass_on(ends):
        def onward(k):
            return pltpu.make_async_remote_copy(
                src_ref=relay.at[k], dst_ref=hot_recv, send_sem=fs_sem.at[k], recv_sem=hr_sem,
                device_id=(ends[k],), device_id_type=MESH)

        for k in range(len(ends)):
            pltpu.make_async_copy(relay.at[k], relay.at[k], rr_sem.at[k]).wait()
            onward(k).start()
        for k in range(len(ends)):
            onward(k).wait_send()

    on_relays(me, pass_on)

    def arrived(off, carry):
        src, copy = cold_from(off)

        @pl.when(src != 0)
        def _():
            copy.wait()

        return carry

    lax.fori_loop(1, N_DEV, arrived, 0)

    @pl.when(me == 0)
    def _():
        own_hot.wait()
        for dev, via, k in far_blocks():
            far_copy(dev, via, k).wait_send()
        for dev in near_blocks():
            near_copy(dev).wait_send()

    @pl.when(me != 0)
    def _():
        pltpu.make_async_copy(hot_recv, hot_recv, hr_sem).wait()

        def sent(off, carry):
            cold_copy(off).wait_send()
            return carry

        lax.fori_loop(1, N_DEV, sent, 0)
        own_cold.wait()


def lookup_exchange(send):
    width = send.shape[1]
    dma = pltpu.SemaphoreType.DMA
    return pl.pallas_call(
        lookup_kernel,
        out_shape=(jax.ShapeDtypeStruct((HOT_CAP, width), jnp.bfloat16),
                   jax.ShapeDtypeStruct(((N_DEV - 1) * COLD_CAP, width), jnp.bfloat16)),
        in_specs=[pl.BlockSpec(memory_space=pl.ANY)],
        out_specs=(pl.BlockSpec(memory_space=pl.ANY),) * 2,
        scratch_shapes=[pltpu.VMEM((N_RELAY, HOT_CAP, width), jnp.bfloat16),
                        dma((N_DEV,)), dma, dma((N_RELAY,)), dma((N_RELAY,)), dma((N_DEV,)), dma((N_DEV,)), dma((2,))],
        compiler_params=pltpu.CompilerParams(collective_id=2, has_side_effects=True),
        cost_estimate=pl.CostEstimate(flops=60_000_000_000, bytes_accessed=30_000_000, transcendentals=0),
        name="lookup_exchange",
    )(send)


GROUP = 256
LAG = 4
KEPT = LAG + 1


def chunk_spot(dev):
    z, y, x, core = dev // 8, dev // 4 % 2, dev // 2 % 2, dev % 2
    return ((x * 2 + y) if core == 0 else (y * 2 + x)) * 4 + z


def return_kernel(hot_send, cold_send, vec_send, hidden, attn, grads, recv, vec_recv, out, relay,
                  held, oth, got0, send1, keep1, got1, send2, keep2, got2, send3, keep3, got3,
                  s0_sem, r0_sem, s1_sem, r1_sem, s2_sem, r2_sem, s3_sem, r3_sem, hs_sem, hr_sem, rr_sem, fs_sem, cs_sem, cr_sem, vs_sem, vr_sem, own_sem):
    me = lax.axis_index("fsdp")
    enter_all(me)

    def block(dev):
        return rows_at(recv, dev * HOT_CAP, HOT_CAP)

    def near_copy(dev):
        return pltpu.make_async_remote_copy(
            src_ref=hot_send, dst_ref=block(dev), send_sem=hs_sem, recv_sem=hr_sem.at[dev],
            device_id=(0,), device_id_type=MESH)

    def far_copy(via, k):
        return pltpu.make_async_remote_copy(
            src_ref=hot_send, dst_ref=relay.at[k], send_sem=hs_sem, recv_sem=rr_sem.at[k],
            device_id=(via,), device_id_type=MESH)

    def vec_copy(off):
        other = lax.rem(me + off, N_DEV)
        return pltpu.make_async_remote_copy(
            src_ref=vec_send.at[other], dst_ref=vec_recv.at[me], send_sem=vs_sem.at[off], recv_sem=vr_sem.at[off],
            device_id=(other,), device_id_type=MESH)

    def cold_copy(off):
        other = lax.rem(me + off, N_DEV)
        return other, pltpu.make_async_remote_copy(
            src_ref=rows_at(cold_send, jnp.maximum(other - 1, 0) * COLD_CAP, COLD_CAP),
            dst_ref=rows_at(recv, me * HOT_CAP, COLD_CAP),
            send_sem=cs_sem.at[off], recv_sem=cr_sem.at[off], device_id=(other,), device_id_type=MESH)

    def cold_from(off):
        src = lax.rem(me - off + N_DEV, N_DEV)
        return pltpu.make_async_copy(
            rows_at(cold_send, 0, COLD_CAP), rows_at(recv, src * HOT_CAP, COLD_CAP), cr_sem.at[off])

    own_hot = pltpu.make_async_copy(hot_send, block(0), own_sem.at[0])
    own_cold = pltpu.make_async_copy(
        rows_at(cold_send, jnp.maximum(me - 1, 0) * COLD_CAP, COLD_CAP), rows_at(recv, me * HOT_CAP, COLD_CAP), own_sem.at[1])
    own_vec = pltpu.make_async_copy(vec_send.at[me], vec_recv.at[me], own_sem.at[2])

    for dev in near_blocks():
        @pl.when(me == dev)
        def _(dev=dev):
            near_copy(dev).start()

    for dev, via, k in far_blocks():
        @pl.when(me == dev)
        def _(via=via, k=k):
            far_copy(via, k).start()

    def start(off, carry):
        other, copy = cold_copy(off)

        @pl.when(other != 0)
        def _():
            copy.start()

        vec_copy(off).start()
        return carry

    lax.fori_loop(1, N_DEV, start, 0)
    own_vec.start()

    @pl.when(me == 0)
    def _():
        own_hot.start()

    @pl.when(me != 0)
    def _():
        own_cold.start()

    groups, half, width = got0.shape
    chunk = half // 16
    core, x, y, z = lax.rem(me, 2), lax.rem(me // 2, 2), lax.rem(me // 4, 2), me // 8
    first = jnp.where(core == 0, x, y)
    second = jnp.where(core == 0, y, x)
    span = jnp.where(core == 0, 2, 4)
    near1 = me + span * (1 - 2 * first)
    near2 = me + (6 - span) * (1 - 2 * second)
    f32, bf16 = jnp.float32, jnp.bfloat16

    def part(size, index):
        return pl.ds(pl.multiple_of(index * size, size), size)

    def to(src, dst, send_sem, recv_sem, dev):
        return pltpu.make_async_remote_copy(src_ref=src, dst_ref=dst, send_sem=send_sem, recv_sem=recv_sem,
                                            device_id=(dev,), device_id_type=MESH)

    def copy0(g):
        return to(oth.at[g], got0.at[g], s0_sem, r0_sem.at[g], me + 1 - 2 * core)

    def copy1(g):
        return to(send1.at[g], got1.at[g], s1_sem, r1_sem.at[g], near1)

    def copy2(g):
        return to(send2.at[g], got2.at[g], s2_sem, r2_sem.at[g], near2)

    def copy3(g, dz):
        peer = lax.rem(z + dz, 4)
        return to(send3.at[g, dz - 1], got3.at[g, dz - 1], s3_sem, r3_sem.at[g, dz - 1], me + 8 * (peer - z))

    def stage(lag, step, body):
        g = step - lag

        @pl.when((g >= 0) & (g < groups))
        def _():
            body(g, lax.rem(g, KEPT))

    def make(g, slot):
        def place(lhs):
            cols = pl.ds(pl.multiple_of(g * width, width), width)
            res = lax.dot_general(lhs[...], grads[:, cols], (((0,), (0,)), ((), ())), preferred_element_type=f32)
            for mine in range(2):
                @pl.when(core == mine)
                def _(mine=mine):
                    for dev in range(N_DEV):
                        spot = chunk_spot(dev) * chunk
                        piece = res[dev * chunk:(dev + 1) * chunk]
                        if dev % 2 == mine:
                            held[slot, spot:spot + chunk, :] = piece
                        else:
                            oth[g, spot:spot + chunk, :] = piece.astype(bf16)

        @pl.when(g < groups * QKV // WCOLS)
        def _():
            place(hidden)

        @pl.when(g >= groups * QKV // WCOLS)
        def _():
            place(attn)

        copy0(g).start()

    def across_core(g, slot):
        copy0(g).wait_recv()
        for sent in range(2):
            rows = part(half // 2, 1 - first if sent else first)
            total = held[slot, rows, :] + got0[g, rows, :].astype(f32)
            if sent:
                send1[g] = total.astype(bf16)
            else:
                keep1[slot] = total
        copy1(g).start()

    def across_first(g, slot):
        copy1(g).wait_recv()
        for sent in range(2):
            rows = part(half // 4, 1 - second if sent else second)
            total = keep1[slot, rows, :] + got1[g, rows, :].astype(f32)
            if sent:
                send2[g] = total.astype(bf16)
            else:
                keep2[slot] = total
        copy2(g).start()

    def across_second(g, slot):
        copy2(g).wait_recv()
        for dz in range(1, 4):
            rows = part(half // 16, lax.rem(z + dz, 4))
            send3[g, dz - 1] = (keep2[slot, rows, :] + got2[g, rows, :].astype(f32)).astype(bf16)
        rows = part(half // 16, z)
        keep3[slot] = keep2[slot, rows, :] + got2[g, rows, :].astype(f32)
        for dz in range(1, 4):
            copy3(g, dz).start()

    def across_z(g, slot):
        total = keep3[slot]
        for dz in range(1, 4):
            copy3(g, dz).wait_recv()
            total = total + got3[g, dz - 1].astype(f32)
        out[:, pl.ds(pl.multiple_of(g * width, width), width)] = total

    def onward(ends, k):
        return to(relay.at[k], block(ends[k]), fs_sem.at[k], hr_sem.at[ends[k]], 0)

    def run(step, carry):
        stage(0, step, make)
        stage(2, step, across_core)
        stage(2 + LAG, step, across_first)
        stage(2 + 2 * LAG, step, across_second)
        stage(2 + 3 * LAG, step, across_z)

        def pass_on(ends):
            for k in reversed(range(len(ends))):
                @pl.when(step == RELAY_STEPS[N_RELAY - 1 - k])
                def _(k=k):
                    pltpu.make_async_copy(relay.at[k], relay.at[k], rr_sem.at[k]).wait()
                    onward(ends, k).start()

        on_relays(me, pass_on)
        return carry

    lax.fori_loop(0, groups + 2 + 3 * LAG, run, 0)

    def passed(ends):
        for k in range(len(ends)):
            onward(ends, k).wait_send()

    on_relays(me, passed)

    for buf, sem in ((got0, s0_sem), (send1, s1_sem), (send2, s2_sem), (send3, s3_sem)):
        pltpu.make_async_copy(buf, buf, sem).wait()

    def finish(off, carry):
        other, copy = cold_copy(off)

        @pl.when(other != 0)
        def _():
            copy.wait_send()

        vec_copy(off).wait()
        return carry

    lax.fori_loop(1, N_DEV, finish, 0)
    own_vec.wait()

    @pl.when(me != 0)
    def _():
        def arrived(off, carry):
            cold_from(off).wait()
            return carry

        lax.fori_loop(1, N_DEV, arrived, 0)
        own_cold.wait()
        far_copy(2, 0).wait_send()

    @pl.when(me == 0)
    def _():
        own_hot.wait()

        def arrived(dev, carry):
            pltpu.make_async_copy(block(dev), block(dev), hr_sem.at[dev]).wait()
            return carry

        lax.fori_loop(1, N_DEV, arrived, 0)


def return_exchange(hot_send, cold_send, vec_send, hidden, attn, grads):
    width = hot_send.shape[1]
    tokens, rows = hidden.shape
    cols, half, groups = GROUP, rows // 2, grads.shape[1] // GROUP
    dma = pltpu.SemaphoreType.DMA
    f32, bf16 = jnp.float32, jnp.bfloat16
    anywhere = pl.BlockSpec(memory_space=pl.ANY)
    in_vmem = pl.BlockSpec(memory_space=pltpu.VMEM)
    return pl.pallas_call(
        return_kernel,
        out_shape=(jax.ShapeDtypeStruct((N_DEV * HOT_CAP, width), bf16),
                   jax.ShapeDtypeStruct(vec_send.shape, f32),
                   jax.ShapeDtypeStruct((half // 16, groups * cols), f32)),
        in_specs=[anywhere] * 3 + [in_vmem] * 3,
        out_specs=(anywhere, anywhere, in_vmem),
        scratch_shapes=[pltpu.VMEM((N_RELAY, HOT_CAP, width), bf16),
                        pltpu.VMEM((KEPT, half, cols), f32), pltpu.VMEM((groups, half, cols), bf16),
                        pltpu.VMEM((groups, half, cols), bf16),
                        pltpu.VMEM((groups, half // 2, cols), bf16), pltpu.VMEM((KEPT, half // 2, cols), f32),
                        pltpu.VMEM((groups, half // 2, cols), bf16),
                        pltpu.VMEM((groups, half // 4, cols), bf16), pltpu.VMEM((KEPT, half // 4, cols), f32),
                        pltpu.VMEM((groups, half // 4, cols), bf16),
                        pltpu.VMEM((groups, 3, half // 16, cols), bf16), pltpu.VMEM((KEPT, half // 16, cols), f32),
                        pltpu.VMEM((groups, 3, half // 16, cols), bf16),
                        dma, dma((groups,)), dma, dma((groups,)), dma, dma((groups,)), dma, dma((groups, 3)),
                        dma, dma((N_DEV,)), dma((N_RELAY,)), dma((N_RELAY,)), dma((N_DEV,)), dma((N_DEV,)),
                        dma((N_DEV,)), dma((N_DEV,)), dma((3,))],
        compiler_params=pltpu.CompilerParams(collective_id=3, has_side_effects=True, vmem_limit_bytes=60 * 1024 * 1024),
        cost_estimate=pl.CostEstimate(flops=60_000_000_000, bytes_accessed=60_000_000, transcendentals=0),
        name="return_exchange",
    )(hot_send, cold_send, vec_send, hidden, attn, grads)


SLOTS = 16
TILE = 256


def table_sum_kernel(low_ref, high_ref, dx_ref, row_ref, out_ref, total):
    step = pl.program_id(0)
    n_groups = HOT_CAP // SLOTS
    tiles = total.shape[0] // TILE

    def tile(index):
        return pl.ds(pl.multiple_of(index * TILE, TILE), TILE)

    @pl.when(step == 0)
    def _():
        def clear(index, carry):
            total[tile(index), :] = jnp.zeros((TILE, total.shape[1]), jnp.float32)
            return carry

        lax.fori_loop(0, tiles, clear, 0)

    @pl.when(step < n_groups)
    def _():
        dx = dx_ref[...].reshape(-1, dx_ref.shape[2])
        rows = row_ref[0]

        def add(index, carry):
            place = index * TILE + lax.broadcasted_iota(jnp.int32, (TILE, rows.shape[1]), 0)
            pick = jnp.where(place == rows, 1.0, 0.0).astype(jnp.bfloat16)
            total[tile(index), :] += jnp.dot(pick, dx, preferred_element_type=jnp.float32)
            return carry

        at = jnp.minimum(step, n_groups - 1)
        lax.fori_loop(low_ref[at], high_ref[at], add, 0)

    @pl.when(step >= n_groups)
    def _():
        out_ref[...] = total[tile(jnp.maximum(step - n_groups, 0)), :].astype(jnp.bfloat16)


def table_sum(dx_recv, rows, rows_dev):
    width = dx_recv.shape[1]
    n_groups = HOT_CAP // SLOTS
    tiles = (rows_dev + TILE - 1) // TILE
    by_group = rows.reshape(N_DEV, n_groups, SLOTS).transpose(1, 0, 2).reshape(n_groups, 1, N_DEV * SLOTS)
    valid = by_group >= 0
    low = jnp.min(jnp.where(valid, by_group, rows_dev), axis=(1, 2)) // TILE
    high = jnp.max(jnp.where(valid, by_group + TILE, 0), axis=(1, 2)) // TILE
    return pl.pallas_call(
        table_sum_kernel,
        grid_spec=pltpu.PrefetchScalarGridSpec(
            num_scalar_prefetch=2,
            grid=(n_groups + tiles,),
            in_specs=[pl.BlockSpec((N_DEV, SLOTS, width), lambda s, lo, hi: (0, jnp.minimum(s, n_groups - 1), 0)),
                      pl.BlockSpec((1, 1, N_DEV * SLOTS), lambda s, lo, hi: (jnp.minimum(s, n_groups - 1), 0, 0))],
            out_specs=pl.BlockSpec((TILE, width), lambda s, lo, hi: (jnp.maximum(s - n_groups, 0), 0)),
            scratch_shapes=[pltpu.VMEM((tiles * TILE, width), jnp.float32)]),
        out_shape=jax.ShapeDtypeStruct((rows_dev, width), jnp.bfloat16),
        compiler_params=pltpu.CompilerParams(vmem_limit_bytes=56 * 1024 * 1024),
        cost_estimate=pl.CostEstimate(flops=30_000_000_000, bytes_accessed=45_000_000, transcendentals=0),
        name="table_sum",
    )(low, high, dx_recv.reshape(N_DEV, HOT_CAP, width), by_group)


Q_GROUP = 8
KV_HEADS = 2


def turn(vector):
    return pltpu.roll(vector, HEAD_DIM // 2, 1)


def attention_kernel(q_ref, k_ref, v_ref, d_attn_ref, cos_ref, sin_ref,
                     attn_ref, dq_ref, dk_ref, dv_ref, gq_ref, gk_ref, gv_ref, k_rot, v_val, dk_sum, dv_sum):
    member = lax.rem(pl.program_id(0), Q_GROUP)
    scale = HEAD_DIM ** -0.5
    cos_t, sin_t = cos_ref[...], sin_ref[...]
    rows_t = (((1,), (1,)), ((), ()))
    cols_t = (((0,), (0,)), ((), ()))
    f32 = jnp.float32

    @pl.when(member == 0)
    def _():
        k_lin = k_ref[...]
        k_rot[...] = (k_lin * cos_t + turn(k_lin) * sin_t).astype(jnp.bfloat16)
        v_val[...] = v_ref[...].astype(jnp.bfloat16)
        dk_sum[...] = jnp.zeros_like(dk_sum)
        dv_sum[...] = jnp.zeros_like(dv_sum)

    q_lin = q_ref[...]
    q_rot = (q_lin * cos_t + turn(q_lin) * sin_t).astype(jnp.bfloat16)
    scores = lax.dot_general(q_rot, k_rot[...], rows_t, preferred_element_type=f32) * scale
    seq = scores.shape[0]
    causal = lax.broadcasted_iota(jnp.int32, (seq, seq), 0) >= lax.broadcasted_iota(jnp.int32, (seq, seq), 1)
    scores = jnp.where(causal, scores, MASK_VALUE)
    weight = jnp.exp(scores - jnp.max(scores, axis=1, keepdims=True))
    prob_f = weight / jnp.sum(weight, axis=1, keepdims=True)
    prob_b = prob_f.astype(jnp.bfloat16)
    attn_ref[...] = jnp.dot(prob_b, v_val[...], preferred_element_type=f32).astype(jnp.bfloat16)

    d_attn = d_attn_ref[...]
    d_probs = lax.dot_general(d_attn, v_val[...], rows_t, preferred_element_type=f32)
    dv_sum[...] += lax.dot_general(prob_b, d_attn, cols_t, preferred_element_type=f32)
    d_scores = prob_f * (d_probs - jnp.sum(d_probs * prob_f, axis=1, keepdims=True))
    d_scores = (d_scores * scale).astype(jnp.bfloat16)
    d_qrot = jnp.dot(d_scores, k_rot[...], preferred_element_type=f32)
    dk_sum[...] += lax.dot_general(d_scores, q_rot, cols_t, preferred_element_type=f32)
    d_query = d_qrot * cos_t - turn(d_qrot) * sin_t
    dq_ref[...] = d_query.astype(jnp.bfloat16)
    gq_ref[...] = jnp.sum(d_query, axis=0, keepdims=True)

    @pl.when(member == Q_GROUP - 1)
    def _():
        d_krot = dk_sum[...]
        d_key = d_krot * cos_t - turn(d_krot) * sin_t
        d_value = dv_sum[...]
        dk_ref[...] = d_key.astype(jnp.bfloat16)
        dv_ref[...] = d_value.astype(jnp.bfloat16)
        gk_ref[...] = jnp.sum(d_key, axis=0, keepdims=True)
        gv_ref[...] = jnp.sum(d_value, axis=0, keepdims=True)


def attention(lin, d_attn, cos_t, sin_t):
    seq = lin.shape[0]
    heads = KV_HEADS * Q_GROUP

    def cols(index):
        return pl.BlockSpec((seq, HEAD_DIM), lambda h: (0, index(h)))

    def line(index):
        return pl.BlockSpec((1, HEAD_DIM), lambda h: (0, index(h)))

    def shape(rows, width, dtype):
        return jax.ShapeDtypeStruct((rows, width), dtype)

    q_width, kv_width = heads * HEAD_DIM, KV_HEADS * HEAD_DIM
    own = lambda h: h
    group = lambda h: h // Q_GROUP
    first = lambda h: 0
    return pl.pallas_call(
        attention_kernel,
        grid=(heads,),
        in_specs=[cols(own), cols(lambda h: heads + h // Q_GROUP), cols(lambda h: heads + KV_HEADS + h // Q_GROUP),
                  cols(own), cols(first), cols(first)],
        out_specs=(cols(own), cols(own), cols(group), cols(group), line(own), line(group), line(group)),
        out_shape=(shape(seq, q_width, jnp.bfloat16), shape(seq, q_width, jnp.bfloat16),
                   shape(seq, kv_width, jnp.bfloat16), shape(seq, kv_width, jnp.bfloat16),
                   shape(1, q_width, jnp.float32), shape(1, kv_width, jnp.float32), shape(1, kv_width, jnp.float32)),
        scratch_shapes=[pltpu.VMEM((seq, HEAD_DIM), jnp.bfloat16), pltpu.VMEM((seq, HEAD_DIM), jnp.bfloat16),
                        pltpu.VMEM((seq, HEAD_DIM), jnp.float32), pltpu.VMEM((seq, HEAD_DIM), jnp.float32)],
        cost_estimate=pl.CostEstimate(flops=14 * seq * seq * q_width, bytes_accessed=10_000_000, transcendentals=heads * seq * seq),
        name="attention",
    )(lin, lin, lin, d_attn, cos_t, sin_t)


def block_fwd_bwd(x_rows, grad_out, gain_vec, w_all, b_qkv):
    seq_len = x_rows.shape[0]
    w_qkv = w_all[:, :QKV]
    w_out = w_all[:, QKV:]
    half_dim = HEAD_DIM // 2
    inv_freq = jnp.power(ROPE_THETA, -(jnp.arange(half_dim, dtype=jnp.float32) * 2.0 / HEAD_DIM))
    angles = jnp.arange(seq_len, dtype=jnp.float32)[:, None] * inv_freq[None, :]
    cos_h, sin_h = jnp.cos(angles), jnp.sin(angles)
    cos_t = jnp.concatenate([cos_h, cos_h], axis=1)
    sin_t = jnp.concatenate([-sin_h, sin_h], axis=1)
    x_full = x_rows.astype(jnp.float32)
    inv_rms = lax.rsqrt(jnp.mean(x_full * x_full, axis=-1, keepdims=True) + NORM_EPS)
    x_norm = x_full * inv_rms
    gain_f = gain_vec.astype(jnp.float32)
    hidden = (x_norm * gain_f).astype(jnp.bfloat16)
    lin = jnp.dot(hidden, w_qkv, preferred_element_type=jnp.float32) + b_qkv.astype(jnp.float32)
    d_attn = jnp.einsum("lo,io->li", grad_out, w_out, preferred_element_type=jnp.float32).astype(jnp.bfloat16)
    attn_b, dq_b, dk_b, dv_b, grad_bq, grad_bk, grad_bv = attention(lin, d_attn, cos_t, sin_t)
    proj_out = jnp.dot(attn_b, w_out, preferred_element_type=jnp.float32)
    block_out = (x_full + proj_out).astype(jnp.bfloat16)
    d_lin_b = jnp.concatenate([dq_b, dk_b, dv_b], axis=1)
    grad_w = (hidden, attn_b, jnp.concatenate([d_lin_b, grad_out], axis=1))
    d_hidden = jnp.einsum("lo,io->li", d_lin_b, w_qkv, preferred_element_type=jnp.float32)
    grad_gain = jnp.sum(d_hidden * x_norm, axis=0)
    d_norm = d_hidden * gain_f
    d_x = grad_out.astype(jnp.float32) + inv_rms * (d_norm - x_norm * jnp.mean(d_norm * x_norm, axis=-1, keepdims=True))
    grad_b = jnp.concatenate([grad_bq[0], grad_bk[0], grad_bv[0]])
    return block_out, d_x, grad_w, grad_gain, grad_b


def solution(mesh):
    row_spec = P("fsdp", None)
    vec_spec = P("fsdp")
    act_spec = P("fsdp", None, None)
    weight_specs = (vec_spec, row_spec, vec_spec, row_spec, vec_spec, row_spec, vec_spec, row_spec)
    in_specs = (row_spec, act_spec, row_spec) + weight_specs
    out_specs = (act_spec, row_spec) + weight_specs

    def device_step(tok_ids, grad_out, table_part, gain_part, wq_part, bq_part, wk_part, bk_part, wv_part, bv_part, wo_part):
        rows_dev, model_width = table_part.shape
        seq_len = tok_ids.shape[1]
        me = lax.axis_index("fsdp")
        first_row = me * rows_dev
        w_all = lax.all_gather(jnp.concatenate([wq_part, wk_part, wv_part, wo_part], axis=1), "fsdp", axis=0, tiled=True)

        vec_part = jnp.concatenate([gain_part, bq_part, bk_part, bv_part]).astype(jnp.float32)
        block = jnp.concatenate([tok_ids.reshape(-1).astype(jnp.float32), jnp.pad(vec_part, (0, 1024 - 256 - 144))])
        gathered = small_gather(block.reshape(8, 128)).reshape(N_DEV, 1024)
        all_ids = gathered[:, :seq_len].astype(jnp.int32)
        vecs = gathered[:, seq_len:seq_len + 144].astype(jnp.bfloat16)
        gain_full = vecs[:, :64].reshape(-1)
        b_qkv = jnp.concatenate([vecs[:, 64:128].reshape(-1), vecs[:, 128:136].reshape(-1), vecs[:, 136:144].reshape(-1)])

        owner = all_ids // rows_dev
        key = all_ids * seq_len + jnp.arange(seq_len)
        counts = jnp.sum((owner[:, :, None] == jnp.arange(N_DEV)).astype(jnp.int32), axis=1)
        overflow = (jnp.max(counts[:, 0]) > HOT_CAP) | (jnp.max(counts[:, 1:]) > COLD_CAP)

        mask = owner == me
        rank = jnp.sum((mask[:, None, :] & (key[:, None, :] < key[:, :, None])).astype(jnp.int32), axis=2)
        hit = mask[:, None, :] & (rank[:, None, :] == jnp.arange(HOT_CAP)[None, :, None])
        rows = jnp.sum(jnp.where(hit, (all_ids - first_row)[:, None, :] + 1, 0), axis=2).reshape(-1) - 1
        hot_recv, cold_recv = lookup_exchange(jnp.take(table_part, jnp.maximum(rows, 0), axis=0, mode="clip"))

        my_ids = tok_ids.reshape(-1)
        my_owner = my_ids // rows_dev
        my_key = my_ids * seq_len + jnp.arange(seq_len)
        same = (my_owner[:, None] == my_owner[None, :]) & (my_key[None, :] < my_key[:, None])
        my_rank = jnp.sum(same.astype(jnp.int32), axis=1)
        hot_slot = jnp.where(my_owner == 0, my_rank, -1)
        cold_slot = jnp.where(my_owner > 0, (my_owner - 1) * COLD_CAP + my_rank, -1)
        hot_pick = (hot_slot[:, None] == jnp.arange(HOT_CAP)[None, :]).astype(jnp.bfloat16)
        cold_pick = (cold_slot[:, None] == jnp.arange((N_DEV - 1) * COLD_CAP)[None, :]).astype(jnp.bfloat16)

        def rows_fast():
            picked = jnp.dot(hot_pick, hot_recv, preferred_element_type=jnp.float32)
            picked = picked + jnp.dot(cold_pick, cold_recv, preferred_element_type=jnp.float32)
            return picked.astype(jnp.bfloat16)

        ring = [(i, (i + 1) % N_DEV) for i in range(N_DEV)]

        def owned_rows(step):
            local_idx = jnp.take(all_ids, lax.rem(me - step + N_DEV, N_DEV), axis=0) - first_row
            return local_idx, (local_idx >= 0) & (local_idx < rows_dev)

        def rows_ring():
            def body(step, acc):
                local_idx, is_owned = owned_rows(step)
                looked = jnp.take(table_part, jnp.where(is_owned, local_idx, 0), axis=0, mode="clip")
                acc = jnp.where(is_owned[:, None], looked, acc)
                return lax.ppermute(acc, "fsdp", ring)

            return lax.fori_loop(0, N_DEV, body, jnp.zeros((seq_len, model_width), jnp.bfloat16))

        x_rows = lax.cond(overflow, rows_ring, rows_fast)
        g_rows = grad_out.reshape(seq_len, model_width)
        block_out, d_x, grad_w, grad_gain, grad_b = block_fwd_bwd(x_rows, g_rows, gain_full, w_all, b_qkv)
        dx_b = d_x.astype(jnp.bfloat16)
        tdims = (((0,), (0,)), ((), ()))
        hot_back = lax.dot_general(hot_pick, dx_b, tdims, preferred_element_type=jnp.float32).astype(jnp.bfloat16)
        cold_back = lax.dot_general(cold_pick, dx_b, tdims, preferred_element_type=jnp.float32).astype(jnp.bfloat16)
        vec_grad = jnp.concatenate(
            [grad_gain.reshape(N_DEV, 64), grad_b[:2048].reshape(N_DEV, 64), grad_b[2048:2304].reshape(N_DEV, 8),
             grad_b[2304:].reshape(N_DEV, 8), jnp.zeros((N_DEV, 1024 - 144), jnp.float32)], axis=1)
        dx_recv, vec_sum, w_red = return_exchange(hot_back, cold_back, vec_grad.reshape(N_DEV, 8, 128), *grad_w)

        def table_fast():
            return table_sum(dx_recv, rows, rows_dev)

        def table_ring():
            def body(step, carry):
                total, moving = carry
                local_idx, is_owned = owned_rows(step)
                seg_idx = jnp.where(is_owned, local_idx, rows_dev)
                total = total.at[seg_idx].add(moving.astype(jnp.float32), mode="drop")
                return total, lax.ppermute(moving, "fsdp", ring)

            start = (jnp.zeros((rows_dev, model_width), jnp.float32), dx_b)
            return lax.fori_loop(0, N_DEV, body, start)[0].astype(jnp.bfloat16)

        grad_table = lax.cond(overflow, table_ring, table_fast)
        v_red = jnp.sum(vec_sum.reshape(N_DEV, 1024), axis=0)
        return (block_out[None], grad_table, v_red[:64], w_red[:, :2048], v_red[64:128], w_red[:, 2048:2304],
                v_red[128:136], w_red[:, 2304:2560], v_red[136:144], w_red[:, 2560:])

    return jax.shard_map(device_step, mesh=mesh, in_specs=in_specs, out_specs=out_specs, check_vma=False)
```

```python
import functools

import jax
import jax.numpy as jnp
from jax import lax
from jax.experimental import pallas as pl
from jax.experimental.pallas import tpu as pltpu
from jax.sharding import PartitionSpec as P

HEAD_DIM = 128
ROPE_THETA = 1.0e6
NORM_EPS = 1e-6
MASK_VALUE = -1e30
N_DEV = 32
HOT_CAP = 160
COLD_CAP = 16
QKV = 2560
WCOLS = 4608
MESH = pl.DeviceIdType.MESH


RELAYS = {2: (26, 18, 10, 6), 3: (27, 19, 11), 4: (28, 20, 12), 5: (29, 21, 13, 7), 8: (30, 22, 14), 9: (31, 23, 15)}
N_RELAY = 4
RELAY_STEPS = (6, 9, 12, 15)


def far_blocks():
    return [(ends[k], via, k) for k in range(N_RELAY) for via, ends in RELAYS.items() if k < len(ends)]


def near_blocks():
    return [24, 25, 16, 17, 8, 9, 2, 3, 4, 5, 1]


def enter_all(me):
    barrier = pltpu.get_barrier_semaphore()

    def tell(off, carry):
        pl.semaphore_signal(barrier, inc=1, device_id=(lax.rem(me + off, N_DEV),), device_id_type=MESH)
        return carry

    lax.fori_loop(1, N_DEV, tell, 0)
    pl.semaphore_wait(barrier, N_DEV - 1)


def small_gather_kernel(src, dst, send_sem, recv_sem, own_sem):
    me = lax.axis_index("fsdp")
    enter_all(me)

    def copy(off):
        return pltpu.make_async_remote_copy(
            src_ref=src, dst_ref=dst.at[me], send_sem=send_sem.at[off], recv_sem=recv_sem.at[off],
            device_id=(lax.rem(me + off, N_DEV),), device_id_type=MESH)

    def start(off, carry):
        copy(off).start()
        return carry

    def finish(off, carry):
        copy(off).wait()
        return carry

    lax.fori_loop(1, N_DEV, start, 0)
    own = pltpu.make_async_copy(src, dst.at[me], own_sem)
    own.start()
    lax.fori_loop(1, N_DEV, finish, 0)
    own.wait()


def small_gather(block):
    return pl.pallas_call(
        small_gather_kernel,
        out_shape=jax.ShapeDtypeStruct((N_DEV,) + block.shape, block.dtype),
        in_specs=[pl.BlockSpec(memory_space=pltpu.VMEM)],
        out_specs=pl.BlockSpec(memory_space=pltpu.VMEM),
        scratch_shapes=[pltpu.SemaphoreType.DMA((N_DEV,)), pltpu.SemaphoreType.DMA((N_DEV,)), pltpu.SemaphoreType.DMA],
        compiler_params=pltpu.CompilerParams(collective_id=1, has_side_effects=True),
        name="small_gather",
    )(block)


def rows_at(ref, start, rows):
    return ref.at[pl.ds(pl.multiple_of(start, 16), rows)]


def on_relays(me, body):
    for via, ends in RELAYS.items():
        @pl.when(me == via)
        def _(ends=ends):
            body(ends)


def lookup_kernel(send, hot_recv, cold_recv, relay, hs_sem, hr_sem, rr_sem, fs_sem, cs_sem, cr_sem, own_sem):
    me = lax.axis_index("fsdp")
    enter_all(me)

    def block(dev):
        return rows_at(send, dev * HOT_CAP, HOT_CAP)

    def near_copy(dev):
        return pltpu.make_async_remote_copy(
            src_ref=block(dev), dst_ref=hot_recv, send_sem=hs_sem.at[dev], recv_sem=hr_sem,
            device_id=(dev,), device_id_type=MESH)

    def far_copy(dev, via, k):
        return pltpu.make_async_remote_copy(
            src_ref=block(dev), dst_ref=relay.at[k], send_sem=hs_sem.at[dev], recv_sem=rr_sem.at[k],
            device_id=(via,), device_id_type=MESH)

    def cold_copy(off):
        other = lax.rem(me + off, N_DEV)
        return pltpu.make_async_remote_copy(
            src_ref=rows_at(send, other * HOT_CAP, COLD_CAP), dst_ref=rows_at(cold_recv, (me - 1) * COLD_CAP, COLD_CAP),
            send_sem=cs_sem.at[off], recv_sem=cr_sem.at[off], device_id=(other,), device_id_type=MESH)

    def cold_from(off):
        src = lax.rem(me - off + N_DEV, N_DEV)
        return src, pltpu.make_async_copy(
            rows_at(send, 0, COLD_CAP), rows_at(cold_recv, jnp.maximum(src - 1, 0) * COLD_CAP, COLD_CAP), cr_sem.at[off])

    own_hot = pltpu.make_async_copy(block(0), hot_recv, own_sem.at[0])
    own_cold = pltpu.make_async_copy(
        rows_at(send, me * HOT_CAP, COLD_CAP), rows_at(cold_recv, jnp.maximum(me - 1, 0) * COLD_CAP, COLD_CAP), own_sem.at[1])

    @pl.when(me == 0)
    def _():
        far, near = far_blocks(), near_blocks()
        for dev, via, k in far[:6]:
            far_copy(dev, via, k).start()
        for dev in near[:4]:
            near_copy(dev).start()
        for dev, via, k in far[6:]:
            far_copy(dev, via, k).start()
        for dev in near[4:]:
            near_copy(dev).start()
        own_hot.start()

    @pl.when(me != 0)
    def _():
        def start(off, carry):
            cold_copy(off).start()
            return carry

        lax.fori_loop(1, N_DEV, start, 0)
        own_cold.start()

    def pass_on(ends):
        def onward(k):
            return pltpu.make_async_remote_copy(
                src_ref=relay.at[k], dst_ref=hot_recv, send_sem=fs_sem.at[k], recv_sem=hr_sem,
                device_id=(ends[k],), device_id_type=MESH)

        for k in range(len(ends)):
            pltpu.make_async_copy(relay.at[k], relay.at[k], rr_sem.at[k]).wait()
            onward(k).start()
        for k in range(len(ends)):
            onward(k).wait_send()

    on_relays(me, pass_on)

    def arrived(off, carry):
        src, copy = cold_from(off)

        @pl.when(src != 0)
        def _():
            copy.wait()

        return carry

    lax.fori_loop(1, N_DEV, arrived, 0)

    @pl.when(me == 0)
    def _():
        own_hot.wait()
        for dev, via, k in far_blocks():
            far_copy(dev, via, k).wait_send()
        for dev in near_blocks():
            near_copy(dev).wait_send()

    @pl.when(me != 0)
    def _():
        pltpu.make_async_copy(hot_recv, hot_recv, hr_sem).wait()

        def sent(off, carry):
            cold_copy(off).wait_send()
            return carry

        lax.fori_loop(1, N_DEV, sent, 0)
        own_cold.wait()


def lookup_exchange(send):
    width = send.shape[1]
    dma = pltpu.SemaphoreType.DMA
    return pl.pallas_call(
        lookup_kernel,
        out_shape=(jax.ShapeDtypeStruct((HOT_CAP, width), jnp.bfloat16),
                   jax.ShapeDtypeStruct(((N_DEV - 1) * COLD_CAP, width), jnp.bfloat16)),
        in_specs=[pl.BlockSpec(memory_space=pl.ANY)],
        out_specs=(pl.BlockSpec(memory_space=pl.ANY),) * 2,
        scratch_shapes=[pltpu.VMEM((N_RELAY, HOT_CAP, width), jnp.bfloat16),
                        dma((N_DEV,)), dma, dma((N_RELAY,)), dma((N_RELAY,)), dma((N_DEV,)), dma((N_DEV,)), dma((2,))],
        compiler_params=pltpu.CompilerParams(collective_id=2, has_side_effects=True),
        cost_estimate=pl.CostEstimate(flops=60_000_000_000, bytes_accessed=30_000_000, transcendentals=0),
        name="lookup_exchange",
    )(send)


GROUP = 256
LAG = 4
KEPT = LAG + 1


def chunk_spot(dev):
    z, y, x, core = dev // 8, dev // 4 % 2, dev // 2 % 2, dev % 2
    return ((x * 2 + y) if core == 0 else (y * 2 + x)) * 4 + z


def return_kernel(hot_send, cold_send, vec_send, w_all, hidden, attn, grads, x_rows, recv, vec_recv, out, block_out, relay,
                  w_tile, w_sem, held, oth, got0, send1, keep1, got1, send2, keep2, got2, send3, keep3, got3,
                  s0_sem, r0_sem, s1_sem, r1_sem, s2_sem, r2_sem, s3_sem, r3_sem, hs_sem, hr_sem, rr_sem, fs_sem, cs_sem, cr_sem, vs_sem, vr_sem, own_sem):
    me = lax.axis_index("fsdp")
    enter_all(me)

    def block(dev):
        return rows_at(recv, dev * HOT_CAP, HOT_CAP)

    def near_copy(dev):
        return pltpu.make_async_remote_copy(
            src_ref=hot_send, dst_ref=block(dev), send_sem=hs_sem, recv_sem=hr_sem.at[dev],
            device_id=(0,), device_id_type=MESH)

    def far_copy(via, k):
        return pltpu.make_async_remote_copy(
            src_ref=hot_send, dst_ref=relay.at[k], send_sem=hs_sem, recv_sem=rr_sem.at[k],
            device_id=(via,), device_id_type=MESH)

    def vec_copy(off):
        other = lax.rem(me + off, N_DEV)
        return pltpu.make_async_remote_copy(
            src_ref=vec_send.at[other], dst_ref=vec_recv.at[me], send_sem=vs_sem.at[off], recv_sem=vr_sem.at[off],
            device_id=(other,), device_id_type=MESH)

    def cold_copy(off):
        other = lax.rem(me + off, N_DEV)
        return other, pltpu.make_async_remote_copy(
            src_ref=rows_at(cold_send, jnp.maximum(other - 1, 0) * COLD_CAP, COLD_CAP),
            dst_ref=rows_at(recv, me * HOT_CAP, COLD_CAP),
            send_sem=cs_sem.at[off], recv_sem=cr_sem.at[off], device_id=(other,), device_id_type=MESH)

    def cold_from(off):
        src = lax.rem(me - off + N_DEV, N_DEV)
        return pltpu.make_async_copy(
            rows_at(cold_send, 0, COLD_CAP), rows_at(recv, src * HOT_CAP, COLD_CAP), cr_sem.at[off])

    own_hot = pltpu.make_async_copy(hot_send, block(0), own_sem.at[0])
    own_cold = pltpu.make_async_copy(
        rows_at(cold_send, jnp.maximum(me - 1, 0) * COLD_CAP, COLD_CAP), rows_at(recv, me * HOT_CAP, COLD_CAP), own_sem.at[1])
    own_vec = pltpu.make_async_copy(vec_send.at[me], vec_recv.at[me], own_sem.at[2])

    for dev in near_blocks():
        @pl.when(me == dev)
        def _(dev=dev):
            near_copy(dev).start()

    for dev, via, k in far_blocks():
        @pl.when(me == dev)
        def _(via=via, k=k):
            far_copy(via, k).start()

    def start(off, carry):
        other, copy = cold_copy(off)

        @pl.when(other != 0)
        def _():
            copy.start()

        vec_copy(off).start()
        return carry

    lax.fori_loop(1, N_DEV, start, 0)
    own_vec.start()

    @pl.when(me == 0)
    def _():
        own_hot.start()

    @pl.when(me != 0)
    def _():
        own_cold.start()

    groups, half, width = got0.shape
    chunk = half // 16
    core, x, y, z = lax.rem(me, 2), lax.rem(me // 2, 2), lax.rem(me // 4, 2), me // 8
    first = jnp.where(core == 0, x, y)
    second = jnp.where(core == 0, y, x)
    span = jnp.where(core == 0, 2, 4)
    near1 = me + span * (1 - 2 * first)
    near2 = me + (6 - span) * (1 - 2 * second)
    f32, bf16 = jnp.float32, jnp.bfloat16

    def part(size, index):
        return pl.ds(pl.multiple_of(index * size, size), size)

    def to(src, dst, send_sem, recv_sem, dev):
        return pltpu.make_async_remote_copy(src_ref=src, dst_ref=dst, send_sem=send_sem, recv_sem=recv_sem,
                                            device_id=(dev,), device_id_type=MESH)

    def copy0(g):
        return to(oth.at[g], got0.at[g], s0_sem, r0_sem.at[g], me + 1 - 2 * core)

    def copy1(g):
        return to(send1.at[g], got1.at[g], s1_sem, r1_sem.at[g], near1)

    def copy2(g):
        return to(send2.at[g], got2.at[g], s2_sem, r2_sem.at[g], near2)

    def copy3(g, dz):
        peer = lax.rem(z + dz, 4)
        return to(send3.at[g, dz - 1], got3.at[g, dz - 1], s3_sem, r3_sem.at[g, dz - 1], me + 8 * (peer - z))

    def stage(lag, step, body):
        g = step - lag

        @pl.when((g >= 0) & (g < groups))
        def _():
            body(g, lax.rem(g, KEPT))

    def make(g, slot):
        def place(lhs):
            cols = pl.ds(pl.multiple_of(g * width, width), width)
            res = lax.dot_general(lhs[...], grads[:, cols], (((0,), (0,)), ((), ())), preferred_element_type=f32)
            for mine in range(2):
                @pl.when(core == mine)
                def _(mine=mine):
                    for dev in range(N_DEV):
                        spot = chunk_spot(dev) * chunk
                        piece = res[dev * chunk:(dev + 1) * chunk]
                        if dev % 2 == mine:
                            held[slot, spot:spot + chunk, :] = piece
                        else:
                            oth[g, spot:spot + chunk, :] = piece.astype(bf16)

        @pl.when(g < groups * QKV // WCOLS)
        def _():
            place(hidden)

        @pl.when(g >= groups * QKV // WCOLS)
        def _():
            place(attn)

        copy0(g).start()

    def across_core(g, slot):
        copy0(g).wait_recv()
        for sent in range(2):
            rows = part(half // 2, 1 - first if sent else first)
            total = held[slot, rows, :] + got0[g, rows, :].astype(f32)
            if sent:
                send1[g] = total.astype(bf16)
            else:
                keep1[slot] = total
        copy1(g).start()

    def across_first(g, slot):
        copy1(g).wait_recv()
        for sent in range(2):
            rows = part(half // 4, 1 - second if sent else second)
            total = keep1[slot, rows, :] + got1[g, rows, :].astype(f32)
            if sent:
                send2[g] = total.astype(bf16)
            else:
                keep2[slot] = total
        copy2(g).start()

    def across_second(g, slot):
        copy2(g).wait_recv()
        for dz in range(1, 4):
            rows = part(half // 16, lax.rem(z + dz, 4))
            send3[g, dz - 1] = (keep2[slot, rows, :] + got2[g, rows, :].astype(f32)).astype(bf16)
        rows = part(half // 16, z)
        keep3[slot] = keep2[slot, rows, :] + got2[g, rows, :].astype(f32)
        for dz in range(1, 4):
            copy3(g, dz).start()

    def across_z(g, slot):
        total = keep3[slot]
        for dz in range(1, 4):
            copy3(g, dz).wait_recv()
            total = total + got3[g, dz - 1].astype(f32)
        out[:, pl.ds(pl.multiple_of(g * width, width), width)] = total

    out_tiles = block_out.shape[1] // width

    def fetch(j):
        cols = pl.ds(pl.multiple_of(QKV + j * width, width), width)
        return pltpu.make_async_copy(w_all.at[:, cols], w_tile.at[lax.rem(j, 2)], w_sem.at[lax.rem(j, 2)])

    def project(j, slot):
        fetch(j).wait()
        cols = pl.ds(pl.multiple_of(j * width, width), width)
        proj = jnp.dot(attn[...], w_tile[lax.rem(j, 2)], preferred_element_type=f32)
        block_out[:, cols] = (x_rows[:, cols].astype(f32) + proj).astype(bf16)

        @pl.when(j + 2 < out_tiles)
        def _():
            fetch(j + 2).start()

    fetch(0).start()
    fetch(1).start()

    def onward(ends, k):
        return to(relay.at[k], block(ends[k]), fs_sem.at[k], hr_sem.at[ends[k]], 0)

    def run(step, carry):
        stage(0, step, make)
        stage(2, step, across_core)
        stage(2 + LAG, step, across_first)
        stage(2 + 2 * LAG, step, across_second)
        stage(2 + 3 * LAG, step, across_z)

        @pl.when((step >= 4) & (step < 4 + out_tiles))
        def _():
            project(step - 4, 0)

        def pass_on(ends):
            for k in reversed(range(len(ends))):
                @pl.when(step == RELAY_STEPS[N_RELAY - 1 - k])
                def _(k=k):
                    pltpu.make_async_copy(relay.at[k], relay.at[k], rr_sem.at[k]).wait()
                    onward(ends, k).start()

        on_relays(me, pass_on)
        return carry

    lax.fori_loop(0, groups + 2 + 3 * LAG, run, 0)

    def passed(ends):
        for k in range(len(ends)):
            onward(ends, k).wait_send()

    on_relays(me, passed)

    for buf, sem in ((got0, s0_sem), (send1, s1_sem), (send2, s2_sem), (send3, s3_sem)):
        pltpu.make_async_copy(buf, buf, sem).wait()

    def finish(off, carry):
        other, copy = cold_copy(off)

        @pl.when(other != 0)
        def _():
            copy.wait_send()

        vec_copy(off).wait()
        return carry

    lax.fori_loop(1, N_DEV, finish, 0)
    own_vec.wait()

    @pl.when(me != 0)
    def _():
        def arrived(off, carry):
            cold_from(off).wait()
            return carry

        lax.fori_loop(1, N_DEV, arrived, 0)
        own_cold.wait()
        far_copy(2, 0).wait_send()

    @pl.when(me == 0)
    def _():
        own_hot.wait()

        def arrived(dev, carry):
            pltpu.make_async_copy(block(dev), block(dev), hr_sem.at[dev]).wait()
            return carry

        lax.fori_loop(1, N_DEV, arrived, 0)


def return_exchange(hot_send, cold_send, vec_send, w_all, hidden, attn, grads, x_rows):
    width = hot_send.shape[1]
    tokens, rows = hidden.shape
    cols, half, groups = GROUP, rows // 2, grads.shape[1] // GROUP
    dma = pltpu.SemaphoreType.DMA
    f32, bf16 = jnp.float32, jnp.bfloat16
    anywhere = pl.BlockSpec(memory_space=pl.ANY)
    in_vmem = pl.BlockSpec(memory_space=pltpu.VMEM)
    return pl.pallas_call(
        return_kernel,
        out_shape=(jax.ShapeDtypeStruct((N_DEV * HOT_CAP, width), bf16),
                   jax.ShapeDtypeStruct(vec_send.shape, f32),
                   jax.ShapeDtypeStruct((half // 16, groups * cols), f32),
                   jax.ShapeDtypeStruct(x_rows.shape, bf16)),
        in_specs=[anywhere] * 4 + [in_vmem] * 4,
        out_specs=(anywhere, anywhere, in_vmem, in_vmem),
        scratch_shapes=[pltpu.VMEM((N_RELAY, HOT_CAP, width), bf16),
                        pltpu.VMEM((2, rows, cols), bf16), dma((2,)),
                        pltpu.VMEM((KEPT, half, cols), f32), pltpu.VMEM((groups, half, cols), bf16),
                        pltpu.VMEM((groups, half, cols), bf16),
                        pltpu.VMEM((groups, half // 2, cols), bf16), pltpu.VMEM((KEPT, half // 2, cols), f32),
                        pltpu.VMEM((groups, half // 2, cols), bf16),
                        pltpu.VMEM((groups, half // 4, cols), bf16), pltpu.VMEM((KEPT, half // 4, cols), f32),
                        pltpu.VMEM((groups, half // 4, cols), bf16),
                        pltpu.VMEM((groups, 3, half // 16, cols), bf16), pltpu.VMEM((KEPT, half // 16, cols), f32),
                        pltpu.VMEM((groups, 3, half // 16, cols), bf16),
                        dma, dma((groups,)), dma, dma((groups,)), dma, dma((groups,)), dma, dma((groups, 3)),
                        dma, dma((N_DEV,)), dma((N_RELAY,)), dma((N_RELAY,)), dma((N_DEV,)), dma((N_DEV,)),
                        dma((N_DEV,)), dma((N_DEV,)), dma((3,))],
        compiler_params=pltpu.CompilerParams(collective_id=3, has_side_effects=True, vmem_limit_bytes=60 * 1024 * 1024),
        cost_estimate=pl.CostEstimate(flops=60_000_000_000, bytes_accessed=60_000_000, transcendentals=0),
        name="return_exchange",
    )(hot_send, cold_send, vec_send, w_all, hidden, attn, grads, x_rows)


SLOTS = 16
TILE = 256


def table_sum_kernel(low_ref, high_ref, dx_ref, row_ref, out_ref, total):
    step = pl.program_id(0)
    n_groups = HOT_CAP // SLOTS
    tiles = total.shape[0] // TILE

    def tile(index):
        return pl.ds(pl.multiple_of(index * TILE, TILE), TILE)

    @pl.when(step == 0)
    def _():
        def clear(index, carry):
            total[tile(index), :] = jnp.zeros((TILE, total.shape[1]), jnp.float32)
            return carry

        lax.fori_loop(0, tiles, clear, 0)

    @pl.when(step < n_groups)
    def _():
        dx = dx_ref[...].reshape(-1, dx_ref.shape[2])
        rows = row_ref[0]

        def add(index, carry):
            place = index * TILE + lax.broadcasted_iota(jnp.int32, (TILE, rows.shape[1]), 0)
            pick = jnp.where(place == rows, 1.0, 0.0).astype(jnp.bfloat16)
            total[tile(index), :] += jnp.dot(pick, dx, preferred_element_type=jnp.float32)
            return carry

        at = jnp.minimum(step, n_groups - 1)
        lax.fori_loop(low_ref[at], high_ref[at], add, 0)

    @pl.when(step >= n_groups)
    def _():
        out_ref[...] = total[tile(jnp.maximum(step - n_groups, 0)), :].astype(jnp.bfloat16)


def table_sum(dx_recv, rows, rows_dev):
    width = dx_recv.shape[1]
    n_groups = HOT_CAP // SLOTS
    tiles = (rows_dev + TILE - 1) // TILE
    by_group = rows.reshape(N_DEV, n_groups, SLOTS).transpose(1, 0, 2).reshape(n_groups, 1, N_DEV * SLOTS)
    valid = by_group >= 0
    low = jnp.min(jnp.where(valid, by_group, rows_dev), axis=(1, 2)) // TILE
    high = jnp.max(jnp.where(valid, by_group + TILE, 0), axis=(1, 2)) // TILE
    return pl.pallas_call(
        table_sum_kernel,
        grid_spec=pltpu.PrefetchScalarGridSpec(
            num_scalar_prefetch=2,
            grid=(n_groups + tiles,),
            in_specs=[pl.BlockSpec((N_DEV, SLOTS, width), lambda s, lo, hi: (0, jnp.minimum(s, n_groups - 1), 0)),
                      pl.BlockSpec((1, 1, N_DEV * SLOTS), lambda s, lo, hi: (jnp.minimum(s, n_groups - 1), 0, 0))],
            out_specs=pl.BlockSpec((TILE, width), lambda s, lo, hi: (jnp.maximum(s - n_groups, 0), 0)),
            scratch_shapes=[pltpu.VMEM((tiles * TILE, width), jnp.float32)]),
        out_shape=jax.ShapeDtypeStruct((rows_dev, width), jnp.bfloat16),
        compiler_params=pltpu.CompilerParams(vmem_limit_bytes=56 * 1024 * 1024),
        cost_estimate=pl.CostEstimate(flops=30_000_000_000, bytes_accessed=45_000_000, transcendentals=0),
        name="table_sum",
    )(low, high, dx_recv.reshape(N_DEV, HOT_CAP, width), by_group)


Q_GROUP = 8
KV_HEADS = 2


def turn(vector):
    return pltpu.roll(vector, HEAD_DIM // 2, 1)


def attention_kernel(q_ref, k_ref, v_ref, d_attn_ref, cos_ref, sin_ref,
                     attn_ref, dq_ref, dk_ref, dv_ref, gq_ref, gk_ref, gv_ref, k_rot, v_val, dk_sum, dv_sum):
    member = lax.rem(pl.program_id(0), Q_GROUP)
    scale = HEAD_DIM ** -0.5
    cos_t, sin_t = cos_ref[...], sin_ref[...]
    rows_t = (((1,), (1,)), ((), ()))
    cols_t = (((0,), (0,)), ((), ()))
    f32 = jnp.float32

    @pl.when(member == 0)
    def _():
        k_lin = k_ref[...]
        k_rot[...] = (k_lin * cos_t + turn(k_lin) * sin_t).astype(jnp.bfloat16)
        v_val[...] = v_ref[...].astype(jnp.bfloat16)
        dk_sum[...] = jnp.zeros_like(dk_sum)
        dv_sum[...] = jnp.zeros_like(dv_sum)

    q_lin = q_ref[...]
    q_rot = (q_lin * cos_t + turn(q_lin) * sin_t).astype(jnp.bfloat16)
    seq = q_lin.shape[0]
    part = seq // 2
    d_qrot = []
    for low in (0, part):
        seen = low + part
        at, keys = slice(low, seen), slice(0, seen)
        scores = lax.dot_general(q_rot[at], k_rot[keys], rows_t, preferred_element_type=f32) * scale
        causal = low + lax.broadcasted_iota(jnp.int32, (part, seen), 0) >= lax.broadcasted_iota(jnp.int32, (part, seen), 1)
        scores = jnp.where(causal, scores, MASK_VALUE)
        weight = jnp.exp(scores - jnp.max(scores, axis=1, keepdims=True))
        prob_f = weight * (1.0 / jnp.sum(weight, axis=1, keepdims=True))
        prob_b = prob_f.astype(jnp.bfloat16)
        attn_ref[at] = jnp.dot(prob_b, v_val[keys], preferred_element_type=f32).astype(jnp.bfloat16)

        d_attn = d_attn_ref[at]
        d_probs = lax.dot_general(d_attn, v_val[keys], rows_t, preferred_element_type=f32)
        dv_sum[keys] += lax.dot_general(prob_b, d_attn, cols_t, preferred_element_type=f32)
        d_scores = prob_f * (d_probs - jnp.sum(d_probs * prob_f, axis=1, keepdims=True))
        d_scores = (d_scores * scale).astype(jnp.bfloat16)
        d_qrot.append(jnp.dot(d_scores, k_rot[keys], preferred_element_type=f32))
        dk_sum[keys] += lax.dot_general(d_scores, q_rot[at], cols_t, preferred_element_type=f32)
    d_qrot = jnp.concatenate(d_qrot, axis=0)
    d_query = d_qrot * cos_t - turn(d_qrot) * sin_t
    dq_ref[...] = d_query.astype(jnp.bfloat16)
    gq_ref[...] = jnp.sum(d_query, axis=0, keepdims=True)

    @pl.when(member == Q_GROUP - 1)
    def _():
        d_krot = dk_sum[...]
        d_key = d_krot * cos_t - turn(d_krot) * sin_t
        d_value = dv_sum[...]
        dk_ref[...] = d_key.astype(jnp.bfloat16)
        dv_ref[...] = d_value.astype(jnp.bfloat16)
        gk_ref[...] = jnp.sum(d_key, axis=0, keepdims=True)
        gv_ref[...] = jnp.sum(d_value, axis=0, keepdims=True)


def attention(lin, d_attn, cos_t, sin_t):
    seq = lin.shape[0]
    heads = KV_HEADS * Q_GROUP

    def cols(index):
        return pl.BlockSpec((seq, HEAD_DIM), lambda h: (0, index(h)))

    def line(index):
        return pl.BlockSpec((1, HEAD_DIM), lambda h: (0, index(h)))

    def shape(rows, width, dtype):
        return jax.ShapeDtypeStruct((rows, width), dtype)

    q_width, kv_width = heads * HEAD_DIM, KV_HEADS * HEAD_DIM
    own = lambda h: h
    group = lambda h: h // Q_GROUP
    first = lambda h: 0
    return pl.pallas_call(
        attention_kernel,
        grid=(heads,),
        in_specs=[cols(own), cols(lambda h: heads + h // Q_GROUP), cols(lambda h: heads + KV_HEADS + h // Q_GROUP),
                  cols(own), cols(first), cols(first)],
        out_specs=(cols(own), cols(own), cols(group), cols(group), line(own), line(group), line(group)),
        out_shape=(shape(seq, q_width, jnp.bfloat16), shape(seq, q_width, jnp.bfloat16),
                   shape(seq, kv_width, jnp.bfloat16), shape(seq, kv_width, jnp.bfloat16),
                   shape(1, q_width, jnp.float32), shape(1, kv_width, jnp.float32), shape(1, kv_width, jnp.float32)),
        scratch_shapes=[pltpu.VMEM((seq, HEAD_DIM), jnp.bfloat16), pltpu.VMEM((seq, HEAD_DIM), jnp.bfloat16),
                        pltpu.VMEM((seq, HEAD_DIM), jnp.float32), pltpu.VMEM((seq, HEAD_DIM), jnp.float32)],
        cost_estimate=pl.CostEstimate(flops=14 * seq * seq * q_width, bytes_accessed=10_000_000, transcendentals=heads * seq * seq),
        name="attention",
    )(lin, lin, lin, d_attn, cos_t, sin_t)


def block_fwd_bwd(x_rows, grad_out, gain_vec, w_all, b_qkv):
    seq_len = x_rows.shape[0]
    w_qkv = w_all[:, :QKV]
    w_out = w_all[:, QKV:]
    half_dim = HEAD_DIM // 2
    inv_freq = jnp.power(ROPE_THETA, -(jnp.arange(half_dim, dtype=jnp.float32) * 2.0 / HEAD_DIM))
    angles = jnp.arange(seq_len, dtype=jnp.float32)[:, None] * inv_freq[None, :]
    cos_h, sin_h = jnp.cos(angles), jnp.sin(angles)
    cos_t = jnp.concatenate([cos_h, cos_h], axis=1)
    sin_t = jnp.concatenate([-sin_h, sin_h], axis=1)
    x_full = x_rows.astype(jnp.float32)
    inv_rms = lax.rsqrt(jnp.mean(x_full * x_full, axis=-1, keepdims=True) + NORM_EPS)
    x_norm = x_full * inv_rms
    gain_f = gain_vec.astype(jnp.float32)
    hidden = (x_norm * gain_f).astype(jnp.bfloat16)
    lin = jnp.dot(hidden, w_qkv, preferred_element_type=jnp.float32) + b_qkv.astype(jnp.float32)
    d_attn = jnp.einsum("lo,io->li", grad_out, w_out, preferred_element_type=jnp.float32).astype(jnp.bfloat16)
    attn_b, dq_b, dk_b, dv_b, grad_bq, grad_bk, grad_bv = attention(lin, d_attn, cos_t, sin_t)
    d_lin_b = jnp.concatenate([dq_b, dk_b, dv_b], axis=1)
    grad_in = (hidden, attn_b, jnp.concatenate([d_lin_b, grad_out], axis=1))
    d_hidden = jnp.einsum("lo,io->li", d_lin_b, w_qkv, preferred_element_type=jnp.float32)
    grad_gain = jnp.sum(d_hidden * x_norm, axis=0)
    d_norm = d_hidden * gain_f
    d_x = grad_out.astype(jnp.float32) + inv_rms * (d_norm - x_norm * jnp.mean(d_norm * x_norm, axis=-1, keepdims=True))
    grad_b = jnp.concatenate([grad_bq[0], grad_bk[0], grad_bv[0]])
    return d_x, grad_in, grad_gain, grad_b


def solution(mesh):
    row_spec = P("fsdp", None)
    vec_spec = P("fsdp")
    act_spec = P("fsdp", None, None)
    weight_specs = (vec_spec, row_spec, vec_spec, row_spec, vec_spec, row_spec, vec_spec, row_spec)
    in_specs = (row_spec, act_spec, row_spec) + weight_specs
    out_specs = (act_spec, row_spec) + weight_specs

    def device_step(tok_ids, grad_out, table_part, gain_part, wq_part, bq_part, wk_part, bk_part, wv_part, bv_part, wo_part):
        rows_dev, model_width = table_part.shape
        seq_len = tok_ids.shape[1]
        me = lax.axis_index("fsdp")
        first_row = me * rows_dev
        w_all = lax.all_gather(jnp.concatenate([wq_part, wk_part, wv_part, wo_part], axis=1), "fsdp", axis=0, tiled=True)

        vec_part = jnp.concatenate([gain_part, bq_part, bk_part, bv_part]).astype(jnp.float32)
        block = jnp.concatenate([tok_ids.reshape(-1).astype(jnp.float32), jnp.pad(vec_part, (0, 1024 - 256 - 144))])
        gathered = small_gather(block.reshape(8, 128)).reshape(N_DEV, 1024)
        all_ids = gathered[:, :seq_len].astype(jnp.int32)
        vecs = gathered[:, seq_len:seq_len + 144].astype(jnp.bfloat16)
        gain_full = vecs[:, :64].reshape(-1)
        b_qkv = jnp.concatenate([vecs[:, 64:128].reshape(-1), vecs[:, 128:136].reshape(-1), vecs[:, 136:144].reshape(-1)])

        owner = all_ids // rows_dev
        key = all_ids * seq_len + jnp.arange(seq_len)
        counts = jnp.sum((owner[:, :, None] == jnp.arange(N_DEV)).astype(jnp.int32), axis=1)
        overflow = (jnp.max(counts[:, 0]) > HOT_CAP) | (jnp.max(counts[:, 1:]) > COLD_CAP)

        mask = owner == me
        rank = jnp.sum((mask[:, None, :] & (key[:, None, :] < key[:, :, None])).astype(jnp.int32), axis=2)
        hit = mask[:, None, :] & (rank[:, None, :] == jnp.arange(HOT_CAP)[None, :, None])
        rows = jnp.sum(jnp.where(hit, (all_ids - first_row)[:, None, :] + 1, 0), axis=2).reshape(-1) - 1
        hot_recv, cold_recv = lookup_exchange(jnp.take(table_part, jnp.maximum(rows, 0), axis=0, mode="clip"))

        my_ids = tok_ids.reshape(-1)
        my_owner = my_ids // rows_dev
        my_key = my_ids * seq_len + jnp.arange(seq_len)
        same = (my_owner[:, None] == my_owner[None, :]) & (my_key[None, :] < my_key[:, None])
        my_rank = jnp.sum(same.astype(jnp.int32), axis=1)
        hot_slot = jnp.where(my_owner == 0, my_rank, -1)
        cold_slot = jnp.where(my_owner > 0, (my_owner - 1) * COLD_CAP + my_rank, -1)
        hot_pick = (hot_slot[:, None] == jnp.arange(HOT_CAP)[None, :]).astype(jnp.bfloat16)
        cold_pick = (cold_slot[:, None] == jnp.arange((N_DEV - 1) * COLD_CAP)[None, :]).astype(jnp.bfloat16)

        def rows_fast():
            picked = jnp.dot(hot_pick, hot_recv, preferred_element_type=jnp.float32)
            picked = picked + jnp.dot(cold_pick, cold_recv, preferred_element_type=jnp.float32)
            return picked.astype(jnp.bfloat16)

        ring = [(i, (i + 1) % N_DEV) for i in range(N_DEV)]

        def owned_rows(step):
            local_idx = jnp.take(all_ids, lax.rem(me - step + N_DEV, N_DEV), axis=0) - first_row
            return local_idx, (local_idx >= 0) & (local_idx < rows_dev)

        def rows_ring():
            def body(step, acc):
                local_idx, is_owned = owned_rows(step)
                looked = jnp.take(table_part, jnp.where(is_owned, local_idx, 0), axis=0, mode="clip")
                acc = jnp.where(is_owned[:, None], looked, acc)
                return lax.ppermute(acc, "fsdp", ring)

            return lax.fori_loop(0, N_DEV, body, jnp.zeros((seq_len, model_width), jnp.bfloat16))

        x_rows = lax.cond(overflow, rows_ring, rows_fast)
        g_rows = grad_out.reshape(seq_len, model_width)
        d_x, grad_in, grad_gain, grad_b = block_fwd_bwd(x_rows, g_rows, gain_full, w_all, b_qkv)
        dx_b = d_x.astype(jnp.bfloat16)
        tdims = (((0,), (0,)), ((), ()))
        hot_back = lax.dot_general(hot_pick, dx_b, tdims, preferred_element_type=jnp.float32).astype(jnp.bfloat16)
        cold_back = lax.dot_general(cold_pick, dx_b, tdims, preferred_element_type=jnp.float32).astype(jnp.bfloat16)
        vec_grad = jnp.concatenate(
            [grad_gain.reshape(N_DEV, 64), grad_b[:2048].reshape(N_DEV, 64), grad_b[2048:2304].reshape(N_DEV, 8),
             grad_b[2304:].reshape(N_DEV, 8), jnp.zeros((N_DEV, 1024 - 144), jnp.float32)], axis=1)
        dx_recv, vec_sum, w_red, block_out = return_exchange(
            hot_back, cold_back, vec_grad.reshape(N_DEV, 8, 128), w_all, *grad_in, x_rows)

        def table_fast():
            return table_sum(dx_recv, rows, rows_dev)

        def table_ring():
            def body(step, carry):
                total, moving = carry
                local_idx, is_owned = owned_rows(step)
                seg_idx = jnp.where(is_owned, local_idx, rows_dev)
                total = total.at[seg_idx].add(moving.astype(jnp.float32), mode="drop")
                return total, lax.ppermute(moving, "fsdp", ring)

            start = (jnp.zeros((rows_dev, model_width), jnp.float32), dx_b)
            return lax.fori_loop(0, N_DEV, body, start)[0].astype(jnp.bfloat16)

        grad_table = lax.cond(overflow, table_ring, table_fast)
        v_red = jnp.sum(vec_sum.reshape(N_DEV, 1024), axis=0)
        return (block_out[None], grad_table, v_red[:64], w_red[:, :2048], v_red[64:128], w_red[:, 2048:2304],
                v_red[128:136], w_red[:, 2304:2560], v_red[136:144], w_red[:, 2560:])

    return jax.shard_map(device_step, mesh=mesh, in_specs=in_specs, out_specs=out_specs, check_vma=False)
```

```python
import functools

import jax
import jax.numpy as jnp
from jax import lax
from jax.experimental import pallas as pl
from jax.experimental.pallas import tpu as pltpu
from jax.sharding import PartitionSpec as P

HEAD_DIM = 128
ROPE_THETA = 1.0e6
NORM_EPS = 1e-6
MASK_VALUE = -1e30
N_DEV = 32
HOT_CAP = 160
COLD_CAP = 16
QKV = 2560
WCOLS = 4608
MESH = pl.DeviceIdType.MESH


LOOKUP_RELAYS = {2: (26, 18, 10, 6), 3: (27, 19, 11, 7), 4: (28, 20, 12, 14), 5: (29, 21, 13, 15), 8: (30, 22), 9: (31, 23)}
RETURN_RELAYS = {2: (26, 18, 10, 6), 3: (27, 19, 11), 4: (28, 20, 12), 5: (29, 21, 13, 7), 8: (30, 22, 14), 9: (31, 23, 15)}
N_RELAY = 4
RELAY_STEPS = (6, 9, 12, 15)


def far_blocks(relays):
    return [(ends[k], via, k) for k in range(N_RELAY) for via, ends in relays.items() if k < len(ends)]


def near_blocks():
    return [24, 25, 16, 17, 8, 9, 2, 3, 4, 5, 1]


def enter_all(me):
    barrier = pltpu.get_barrier_semaphore()

    def tell(off, carry):
        pl.semaphore_signal(barrier, inc=1, device_id=(lax.rem(me + off, N_DEV),), device_id_type=MESH)
        return carry

    lax.fori_loop(1, N_DEV, tell, 0)
    pl.semaphore_wait(barrier, N_DEV - 1)


def small_gather_kernel(src, dst, send_sem, recv_sem, own_sem):
    me = lax.axis_index("fsdp")
    enter_all(me)

    def copy(off):
        return pltpu.make_async_remote_copy(
            src_ref=src, dst_ref=dst.at[me], send_sem=send_sem.at[off], recv_sem=recv_sem.at[off],
            device_id=(lax.rem(me + off, N_DEV),), device_id_type=MESH)

    def start(off, carry):
        copy(off).start()
        return carry

    def finish(off, carry):
        copy(off).wait()
        return carry

    lax.fori_loop(1, N_DEV, start, 0)
    own = pltpu.make_async_copy(src, dst.at[me], own_sem)
    own.start()
    lax.fori_loop(1, N_DEV, finish, 0)
    own.wait()


def small_gather(block):
    return pl.pallas_call(
        small_gather_kernel,
        out_shape=jax.ShapeDtypeStruct((N_DEV,) + block.shape, block.dtype),
        in_specs=[pl.BlockSpec(memory_space=pltpu.VMEM)],
        out_specs=pl.BlockSpec(memory_space=pltpu.VMEM),
        scratch_shapes=[pltpu.SemaphoreType.DMA((N_DEV,)), pltpu.SemaphoreType.DMA((N_DEV,)), pltpu.SemaphoreType.DMA],
        compiler_params=pltpu.CompilerParams(collective_id=1, has_side_effects=True),
        name="small_gather",
    )(block)


def rows_at(ref, start, rows):
    return ref.at[pl.ds(pl.multiple_of(start, 16), rows)]


def on_relays(me, relays, body):
    for via, ends in relays.items():
        @pl.when(me == via)
        def _(ends=ends):
            body(ends)


def lookup_kernel(send, hot_recv, cold_recv, relay, hs_sem, hr_sem, rr_sem, fs_sem, cs_sem, cr_sem, own_sem):
    me = lax.axis_index("fsdp")
    enter_all(me)

    def block(dev):
        return rows_at(send, dev * HOT_CAP, HOT_CAP)

    def near_copy(dev):
        return pltpu.make_async_remote_copy(
            src_ref=block(dev), dst_ref=hot_recv, send_sem=hs_sem.at[dev], recv_sem=hr_sem,
            device_id=(dev,), device_id_type=MESH)

    def far_copy(dev, via, k):
        return pltpu.make_async_remote_copy(
            src_ref=block(dev), dst_ref=relay.at[k], send_sem=hs_sem.at[dev], recv_sem=rr_sem.at[k],
            device_id=(via,), device_id_type=MESH)

    def cold_copy(off):
        other = lax.rem(me + off, N_DEV)
        return pltpu.make_async_remote_copy(
            src_ref=rows_at(send, other * HOT_CAP, COLD_CAP), dst_ref=rows_at(cold_recv, (me - 1) * COLD_CAP, COLD_CAP),
            send_sem=cs_sem.at[off], recv_sem=cr_sem.at[off], device_id=(other,), device_id_type=MESH)

    def cold_from(off):
        src = lax.rem(me - off + N_DEV, N_DEV)
        return src, pltpu.make_async_copy(
            rows_at(send, 0, COLD_CAP), rows_at(cold_recv, jnp.maximum(src - 1, 0) * COLD_CAP, COLD_CAP), cr_sem.at[off])

    own_hot = pltpu.make_async_copy(block(0), hot_recv, own_sem.at[0])
    own_cold = pltpu.make_async_copy(
        rows_at(send, me * HOT_CAP, COLD_CAP), rows_at(cold_recv, jnp.maximum(me - 1, 0) * COLD_CAP, COLD_CAP), own_sem.at[1])

    @pl.when(me == 0)
    def _():
        far, near = far_blocks(LOOKUP_RELAYS), near_blocks()
        for dev, via, k in far[:6]:
            far_copy(dev, via, k).start()
        for dev in near[:4]:
            near_copy(dev).start()
        for dev, via, k in far[6:]:
            far_copy(dev, via, k).start()
        for dev in near[4:]:
            near_copy(dev).start()
        own_hot.start()

    @pl.when(me != 0)
    def _():
        def start(off, carry):
            cold_copy(off).start()
            return carry

        lax.fori_loop(1, N_DEV, start, 0)
        own_cold.start()

    def pass_on(ends):
        def onward(k):
            return pltpu.make_async_remote_copy(
                src_ref=relay.at[k], dst_ref=hot_recv, send_sem=fs_sem.at[k], recv_sem=hr_sem,
                device_id=(ends[k],), device_id_type=MESH)

        for k in range(len(ends)):
            pltpu.make_async_copy(relay.at[k], relay.at[k], rr_sem.at[k]).wait()
            onward(k).start()
        for k in range(len(ends)):
            onward(k).wait_send()

    on_relays(me, LOOKUP_RELAYS, pass_on)

    def arrived(off, carry):
        src, copy = cold_from(off)

        @pl.when(src != 0)
        def _():
            copy.wait()

        return carry

    lax.fori_loop(1, N_DEV, arrived, 0)

    @pl.when(me == 0)
    def _():
        own_hot.wait()
        for dev, via, k in far_blocks(LOOKUP_RELAYS):
            far_copy(dev, via, k).wait_send()
        for dev in near_blocks():
            near_copy(dev).wait_send()

    @pl.when(me != 0)
    def _():
        pltpu.make_async_copy(hot_recv, hot_recv, hr_sem).wait()

        def sent(off, carry):
            cold_copy(off).wait_send()
            return carry

        lax.fori_loop(1, N_DEV, sent, 0)
        own_cold.wait()


def lookup_exchange(send):
    width = send.shape[1]
    dma = pltpu.SemaphoreType.DMA
    return pl.pallas_call(
        lookup_kernel,
        out_shape=(jax.ShapeDtypeStruct((HOT_CAP, width), jnp.bfloat16),
                   jax.ShapeDtypeStruct(((N_DEV - 1) * COLD_CAP, width), jnp.bfloat16)),
        in_specs=[pl.BlockSpec(memory_space=pl.ANY)],
        out_specs=(pl.BlockSpec(memory_space=pl.ANY),) * 2,
        scratch_shapes=[pltpu.VMEM((N_RELAY, HOT_CAP, width), jnp.bfloat16),
                        dma((N_DEV,)), dma, dma((N_RELAY,)), dma((N_RELAY,)), dma((N_DEV,)), dma((N_DEV,)), dma((2,))],
        compiler_params=pltpu.CompilerParams(collective_id=2, has_side_effects=True),
        cost_estimate=pl.CostEstimate(flops=60_000_000_000, bytes_accessed=30_000_000, transcendentals=0),
        name="lookup_exchange",
    )(send)


GROUP = 256
LAG = 4
KEPT = LAG + 1


def chunk_spot(dev):
    z, y, x, core = dev // 8, dev // 4 % 2, dev // 2 % 2, dev % 2
    return ((x * 2 + y) if core == 0 else (y * 2 + x)) * 4 + z


def return_kernel(hot_send, cold_send, vec_send, w_all, hidden, attn, grads, x_rows, recv, vec_recv, out, block_out, relay,
                  w_tile, w_sem, held, oth, got0, send1, keep1, got1, send2, keep2, got2, send3, keep3, got3,
                  s0_sem, r0_sem, s1_sem, r1_sem, s2_sem, r2_sem, s3_sem, r3_sem, hs_sem, hr_sem, rr_sem, fs_sem, cs_sem, cr_sem, vs_sem, vr_sem, own_sem):
    me = lax.axis_index("fsdp")
    enter_all(me)

    def block(dev):
        return rows_at(recv, dev * HOT_CAP, HOT_CAP)

    def near_copy(dev):
        return pltpu.make_async_remote_copy(
            src_ref=hot_send, dst_ref=block(dev), send_sem=hs_sem, recv_sem=hr_sem.at[dev],
            device_id=(0,), device_id_type=MESH)

    def far_copy(via, k):
        return pltpu.make_async_remote_copy(
            src_ref=hot_send, dst_ref=relay.at[k], send_sem=hs_sem, recv_sem=rr_sem.at[k],
            device_id=(via,), device_id_type=MESH)

    def vec_copy(off):
        other = lax.rem(me + off, N_DEV)
        return pltpu.make_async_remote_copy(
            src_ref=vec_send.at[other], dst_ref=vec_recv.at[me], send_sem=vs_sem.at[off], recv_sem=vr_sem.at[off],
            device_id=(other,), device_id_type=MESH)

    def cold_copy(off):
        other = lax.rem(me + off, N_DEV)
        return other, pltpu.make_async_remote_copy(
            src_ref=rows_at(cold_send, jnp.maximum(other - 1, 0) * COLD_CAP, COLD_CAP),
            dst_ref=rows_at(recv, me * HOT_CAP, COLD_CAP),
            send_sem=cs_sem.at[off], recv_sem=cr_sem.at[off], device_id=(other,), device_id_type=MESH)

    def cold_from(off):
        src = lax.rem(me - off + N_DEV, N_DEV)
        return pltpu.make_async_copy(
            rows_at(cold_send, 0, COLD_CAP), rows_at(recv, src * HOT_CAP, COLD_CAP), cr_sem.at[off])

    own_hot = pltpu.make_async_copy(hot_send, block(0), own_sem.at[0])
    own_cold = pltpu.make_async_copy(
        rows_at(cold_send, jnp.maximum(me - 1, 0) * COLD_CAP, COLD_CAP), rows_at(recv, me * HOT_CAP, COLD_CAP), own_sem.at[1])
    own_vec = pltpu.make_async_copy(vec_send.at[me], vec_recv.at[me], own_sem.at[2])

    for dev in near_blocks():
        @pl.when(me == dev)
        def _(dev=dev):
            near_copy(dev).start()

    for dev, via, k in far_blocks(RETURN_RELAYS):
        @pl.when(me == dev)
        def _(via=via, k=k):
            far_copy(via, k).start()

    def start(off, carry):
        other, copy = cold_copy(off)

        @pl.when(other != 0)
        def _():
            copy.start()

        vec_copy(off).start()
        return carry

    lax.fori_loop(1, N_DEV, start, 0)
    own_vec.start()

    @pl.when(me == 0)
    def _():
        own_hot.start()

    @pl.when(me != 0)
    def _():
        own_cold.start()

    groups, half, width = got0.shape
    chunk = half // 16
    core, x, y, z = lax.rem(me, 2), lax.rem(me // 2, 2), lax.rem(me // 4, 2), me // 8
    first = jnp.where(core == 0, x, y)
    second = jnp.where(core == 0, y, x)
    span = jnp.where(core == 0, 2, 4)
    near1 = me + span * (1 - 2 * first)
    near2 = me + (6 - span) * (1 - 2 * second)
    f32, bf16 = jnp.float32, jnp.bfloat16

    def part(size, index):
        return pl.ds(pl.multiple_of(index * size, size), size)

    def to(src, dst, send_sem, recv_sem, dev):
        return pltpu.make_async_remote_copy(src_ref=src, dst_ref=dst, send_sem=send_sem, recv_sem=recv_sem,
                                            device_id=(dev,), device_id_type=MESH)

    def copy0(g):
        return to(oth.at[g], got0.at[g], s0_sem, r0_sem.at[g], me + 1 - 2 * core)

    def copy1(g):
        return to(send1.at[g], got1.at[g], s1_sem, r1_sem.at[g], near1)

    def copy2(g):
        return to(send2.at[g], got2.at[g], s2_sem, r2_sem.at[g], near2)

    def copy3(g, dz):
        peer = lax.rem(z + dz, 4)
        return to(send3.at[g, dz - 1], got3.at[g, dz - 1], s3_sem, r3_sem.at[g, dz - 1], me + 8 * (peer - z))

    def stage(lag, step, body):
        g = step - lag

        @pl.when((g >= 0) & (g < groups))
        def _():
            body(g, lax.rem(g, KEPT))

    def make(g, slot):
        def place(lhs):
            cols = pl.ds(pl.multiple_of(g * width, width), width)
            res = lax.dot_general(lhs[...], grads[:, cols], (((0,), (0,)), ((), ())), preferred_element_type=f32)
            for mine in range(2):
                @pl.when(core == mine)
                def _(mine=mine):
                    for dev in range(N_DEV):
                        spot = chunk_spot(dev) * chunk
                        piece = res[dev * chunk:(dev + 1) * chunk]
                        if dev % 2 == mine:
                            held[slot, spot:spot + chunk, :] = piece
                        else:
                            oth[g, spot:spot + chunk, :] = piece.astype(bf16)

        @pl.when(g < groups * QKV // WCOLS)
        def _():
            place(hidden)

        @pl.when(g >= groups * QKV // WCOLS)
        def _():
            place(attn)

        copy0(g).start()

    def across_core(g, slot):
        copy0(g).wait_recv()
        for sent in range(2):
            rows = part(half // 2, 1 - first if sent else first)
            total = held[slot, rows, :] + got0[g, rows, :].astype(f32)
            if sent:
                send1[g] = total.astype(bf16)
            else:
                keep1[slot] = total
        copy1(g).start()

    def across_first(g, slot):
        copy1(g).wait_recv()
        for sent in range(2):
            rows = part(half // 4, 1 - second if sent else second)
            total = keep1[slot, rows, :] + got1[g, rows, :].astype(f32)
            if sent:
                send2[g] = total.astype(bf16)
            else:
                keep2[slot] = total
        copy2(g).start()

    def across_second(g, slot):
        copy2(g).wait_recv()
        for dz in range(1, 4):
            rows = part(half // 16, lax.rem(z + dz, 4))
            send3[g, dz - 1] = (keep2[slot, rows, :] + got2[g, rows, :].astype(f32)).astype(bf16)
        rows = part(half // 16, z)
        keep3[slot] = keep2[slot, rows, :] + got2[g, rows, :].astype(f32)
        for dz in range(1, 4):
            copy3(g, dz).start()

    def across_z(g, slot):
        total = keep3[slot]
        for dz in range(1, 4):
            copy3(g, dz).wait_recv()
            total = total + got3[g, dz - 1].astype(f32)
        out[:, pl.ds(pl.multiple_of(g * width, width), width)] = total

    out_tiles = block_out.shape[1] // width

    def fetch(j):
        cols = pl.ds(pl.multiple_of(QKV + j * width, width), width)
        return pltpu.make_async_copy(w_all.at[:, cols], w_tile.at[lax.rem(j, 2)], w_sem.at[lax.rem(j, 2)])

    def project(j, slot):
        fetch(j).wait()
        cols = pl.ds(pl.multiple_of(j * width, width), width)
        proj = jnp.dot(attn[...], w_tile[lax.rem(j, 2)], preferred_element_type=f32)
        block_out[:, cols] = (x_rows[:, cols].astype(f32) + proj).astype(bf16)

        @pl.when(j + 2 < out_tiles)
        def _():
            fetch(j + 2).start()

    fetch(0).start()
    fetch(1).start()

    def onward(ends, k):
        return to(relay.at[k], block(ends[k]), fs_sem.at[k], hr_sem.at[ends[k]], 0)

    def run(step, carry):
        stage(0, step, make)
        stage(2, step, across_core)
        stage(2 + LAG, step, across_first)
        stage(2 + 2 * LAG, step, across_second)
        stage(2 + 3 * LAG, step, across_z)

        @pl.when((step >= 4) & (step < 4 + out_tiles))
        def _():
            project(step - 4, 0)

        def pass_on(ends):
            for k in reversed(range(len(ends))):
                @pl.when(step == RELAY_STEPS[N_RELAY - 1 - k])
                def _(k=k):
                    pltpu.make_async_copy(relay.at[k], relay.at[k], rr_sem.at[k]).wait()
                    onward(ends, k).start()

        on_relays(me, RETURN_RELAYS, pass_on)
        return carry

    lax.fori_loop(0, groups + 2 + 3 * LAG, run, 0)

    def passed(ends):
        for k in range(len(ends)):
            onward(ends, k).wait_send()

    on_relays(me, RETURN_RELAYS, passed)

    for buf, sem in ((got0, s0_sem), (send1, s1_sem), (send2, s2_sem), (send3, s3_sem)):
        pltpu.make_async_copy(buf, buf, sem).wait()

    def finish(off, carry):
        other, copy = cold_copy(off)

        @pl.when(other != 0)
        def _():
            copy.wait_send()

        vec_copy(off).wait()
        return carry

    lax.fori_loop(1, N_DEV, finish, 0)
    own_vec.wait()

    @pl.when(me != 0)
    def _():
        def arrived(off, carry):
            cold_from(off).wait()
            return carry

        lax.fori_loop(1, N_DEV, arrived, 0)
        own_cold.wait()
        far_copy(2, 0).wait_send()

    @pl.when(me == 0)
    def _():
        own_hot.wait()

        def arrived(dev, carry):
            pltpu.make_async_copy(block(dev), block(dev), hr_sem.at[dev]).wait()
            return carry

        lax.fori_loop(1, N_DEV, arrived, 0)


def return_exchange(hot_send, cold_send, vec_send, w_all, hidden, attn, grads, x_rows):
    width = hot_send.shape[1]
    tokens, rows = hidden.shape
    cols, half, groups = GROUP, rows // 2, grads.shape[1] // GROUP
    dma = pltpu.SemaphoreType.DMA
    f32, bf16 = jnp.float32, jnp.bfloat16
    anywhere = pl.BlockSpec(memory_space=pl.ANY)
    in_vmem = pl.BlockSpec(memory_space=pltpu.VMEM)
    return pl.pallas_call(
        return_kernel,
        out_shape=(jax.ShapeDtypeStruct((N_DEV * HOT_CAP, width), bf16),
                   jax.ShapeDtypeStruct(vec_send.shape, f32),
                   jax.ShapeDtypeStruct((half // 16, groups * cols), f32),
                   jax.ShapeDtypeStruct(x_rows.shape, bf16)),
        in_specs=[anywhere] * 4 + [in_vmem] * 4,
        out_specs=(anywhere, anywhere, in_vmem, in_vmem),
        scratch_shapes=[pltpu.VMEM((N_RELAY, HOT_CAP, width), bf16),
                        pltpu.VMEM((2, rows, cols), bf16), dma((2,)),
                        pltpu.VMEM((KEPT, half, cols), f32), pltpu.VMEM((groups, half, cols), bf16),
                        pltpu.VMEM((groups, half, cols), bf16),
                        pltpu.VMEM((groups, half // 2, cols), bf16), pltpu.VMEM((KEPT, half // 2, cols), f32),
                        pltpu.VMEM((groups, half // 2, cols), bf16),
                        pltpu.VMEM((groups, half // 4, cols), bf16), pltpu.VMEM((KEPT, half // 4, cols), f32),
                        pltpu.VMEM((groups, half // 4, cols), bf16),
                        pltpu.VMEM((groups, 3, half // 16, cols), bf16), pltpu.VMEM((KEPT, half // 16, cols), f32),
                        pltpu.VMEM((groups, 3, half // 16, cols), bf16),
                        dma, dma((groups,)), dma, dma((groups,)), dma, dma((groups,)), dma, dma((groups, 3)),
                        dma, dma((N_DEV,)), dma((N_RELAY,)), dma((N_RELAY,)), dma((N_DEV,)), dma((N_DEV,)),
                        dma((N_DEV,)), dma((N_DEV,)), dma((3,))],
        compiler_params=pltpu.CompilerParams(collective_id=3, has_side_effects=True, vmem_limit_bytes=60 * 1024 * 1024),
        cost_estimate=pl.CostEstimate(flops=60_000_000_000, bytes_accessed=60_000_000, transcendentals=0),
        name="return_exchange",
    )(hot_send, cold_send, vec_send, w_all, hidden, attn, grads, x_rows)


SLOTS = 16
TILE = 256


def table_sum_kernel(low_ref, high_ref, dx_ref, row_ref, out_ref, total):
    step = pl.program_id(0)
    n_groups = HOT_CAP // SLOTS
    tiles = total.shape[0] // TILE

    def tile(index):
        return pl.ds(pl.multiple_of(index * TILE, TILE), TILE)

    @pl.when(step == 0)
    def _():
        def clear(index, carry):
            total[tile(index), :] = jnp.zeros((TILE, total.shape[1]), jnp.float32)
            return carry

        lax.fori_loop(0, tiles, clear, 0)

    @pl.when(step < n_groups)
    def _():
        dx = dx_ref[...].reshape(-1, dx_ref.shape[2])
        rows = row_ref[0]

        def add(index, carry):
            place = index * TILE + lax.broadcasted_iota(jnp.int32, (TILE, rows.shape[1]), 0)
            pick = jnp.where(place == rows, 1.0, 0.0).astype(jnp.bfloat16)
            total[tile(index), :] += jnp.dot(pick, dx, preferred_element_type=jnp.float32)
            return carry

        at = jnp.minimum(step, n_groups - 1)
        lax.fori_loop(low_ref[at], high_ref[at], add, 0)

    @pl.when(step >= n_groups)
    def _():
        out_ref[...] = total[tile(jnp.maximum(step - n_groups, 0)), :].astype(jnp.bfloat16)


def table_sum(dx_recv, rows, rows_dev):
    width = dx_recv.shape[1]
    n_groups = HOT_CAP // SLOTS
    tiles = (rows_dev + TILE - 1) // TILE
    by_group = rows.reshape(N_DEV, n_groups, SLOTS).transpose(1, 0, 2).reshape(n_groups, 1, N_DEV * SLOTS)
    valid = by_group >= 0
    low = jnp.min(jnp.where(valid, by_group, rows_dev), axis=(1, 2)) // TILE
    high = jnp.max(jnp.where(valid, by_group + TILE, 0), axis=(1, 2)) // TILE
    return pl.pallas_call(
        table_sum_kernel,
        grid_spec=pltpu.PrefetchScalarGridSpec(
            num_scalar_prefetch=2,
            grid=(n_groups + tiles,),
            in_specs=[pl.BlockSpec((N_DEV, SLOTS, width), lambda s, lo, hi: (0, jnp.minimum(s, n_groups - 1), 0)),
                      pl.BlockSpec((1, 1, N_DEV * SLOTS), lambda s, lo, hi: (jnp.minimum(s, n_groups - 1), 0, 0))],
            out_specs=pl.BlockSpec((TILE, width), lambda s, lo, hi: (jnp.maximum(s - n_groups, 0), 0)),
            scratch_shapes=[pltpu.VMEM((tiles * TILE, width), jnp.float32)]),
        out_shape=jax.ShapeDtypeStruct((rows_dev, width), jnp.bfloat16),
        compiler_params=pltpu.CompilerParams(vmem_limit_bytes=56 * 1024 * 1024),
        cost_estimate=pl.CostEstimate(flops=30_000_000_000, bytes_accessed=45_000_000, transcendentals=0),
        name="table_sum",
    )(low, high, dx_recv.reshape(N_DEV, HOT_CAP, width), by_group)


Q_GROUP = 8
KV_HEADS = 2


def turn(vector):
    return pltpu.roll(vector, HEAD_DIM // 2, 1)


def attention_kernel(q_ref, k_ref, v_ref, d_attn_ref, cos_ref, sin_ref,
                     attn_ref, dq_ref, dk_ref, dv_ref, gq_ref, gk_ref, gv_ref, k_rot, v_val, dk_sum, dv_sum):
    member = lax.rem(pl.program_id(0), Q_GROUP)
    scale = HEAD_DIM ** -0.5
    cos_t, sin_t = cos_ref[...], sin_ref[...]
    rows_t = (((1,), (1,)), ((), ()))
    cols_t = (((0,), (0,)), ((), ()))
    f32 = jnp.float32

    @pl.when(member == 0)
    def _():
        k_lin = k_ref[...]
        k_rot[...] = (k_lin * cos_t + turn(k_lin) * sin_t).astype(jnp.bfloat16)
        v_val[...] = v_ref[...].astype(jnp.bfloat16)
        dk_sum[...] = jnp.zeros_like(dk_sum)
        dv_sum[...] = jnp.zeros_like(dv_sum)

    q_lin = q_ref[...]
    q_rot = (q_lin * cos_t + turn(q_lin) * sin_t).astype(jnp.bfloat16)
    scores = lax.dot_general(q_rot, k_rot[...], rows_t, preferred_element_type=f32) * scale
    seq = scores.shape[0]
    causal = lax.broadcasted_iota(jnp.int32, (seq, seq), 0) >= lax.broadcasted_iota(jnp.int32, (seq, seq), 1)
    scores = jnp.where(causal, scores, MASK_VALUE)
    weight = jnp.exp(scores - jnp.max(scores, axis=1, keepdims=True))
    prob_f = weight * (1.0 / jnp.sum(weight, axis=1, keepdims=True))
    prob_b = prob_f.astype(jnp.bfloat16)
    attn_ref[...] = jnp.dot(prob_b, v_val[...], preferred_element_type=f32).astype(jnp.bfloat16)

    d_attn = d_attn_ref[...]
    d_probs = lax.dot_general(d_attn, v_val[...], rows_t, preferred_element_type=f32)
    dv_sum[...] += lax.dot_general(prob_b, d_attn, cols_t, preferred_element_type=f32)
    d_scores = prob_f * (d_probs - jnp.sum(d_probs * prob_f, axis=1, keepdims=True))
    d_scores = (d_scores * scale).astype(jnp.bfloat16)
    d_qrot = jnp.dot(d_scores, k_rot[...], preferred_element_type=f32)
    dk_sum[...] += lax.dot_general(d_scores, q_rot, cols_t, preferred_element_type=f32)
    d_query = d_qrot * cos_t - turn(d_qrot) * sin_t
    dq_ref[...] = d_query.astype(jnp.bfloat16)
    gq_ref[...] = jnp.sum(d_query, axis=0, keepdims=True)

    @pl.when(member == Q_GROUP - 1)
    def _():
        d_krot = dk_sum[...]
        d_key = d_krot * cos_t - turn(d_krot) * sin_t
        d_value = dv_sum[...]
        dk_ref[...] = d_key.astype(jnp.bfloat16)
        dv_ref[...] = d_value.astype(jnp.bfloat16)
        gk_ref[...] = jnp.sum(d_key, axis=0, keepdims=True)
        gv_ref[...] = jnp.sum(d_value, axis=0, keepdims=True)


def attention(lin, d_attn, cos_t, sin_t):
    seq = lin.shape[0]
    heads = KV_HEADS * Q_GROUP

    def cols(index):
        return pl.BlockSpec((seq, HEAD_DIM), lambda h: (0, index(h)))

    def line(index):
        return pl.BlockSpec((1, HEAD_DIM), lambda h: (0, index(h)))

    def shape(rows, width, dtype):
        return jax.ShapeDtypeStruct((rows, width), dtype)

    q_width, kv_width = heads * HEAD_DIM, KV_HEADS * HEAD_DIM
    own = lambda h: h
    group = lambda h: h // Q_GROUP
    first = lambda h: 0
    return pl.pallas_call(
        attention_kernel,
        grid=(heads,),
        in_specs=[cols(own), cols(lambda h: heads + h // Q_GROUP), cols(lambda h: heads + KV_HEADS + h // Q_GROUP),
                  cols(own), cols(first), cols(first)],
        out_specs=(cols(own), cols(own), cols(group), cols(group), line(own), line(group), line(group)),
        out_shape=(shape(seq, q_width, jnp.bfloat16), shape(seq, q_width, jnp.bfloat16),
                   shape(seq, kv_width, jnp.bfloat16), shape(seq, kv_width, jnp.bfloat16),
                   shape(1, q_width, jnp.float32), shape(1, kv_width, jnp.float32), shape(1, kv_width, jnp.float32)),
        scratch_shapes=[pltpu.VMEM((seq, HEAD_DIM), jnp.bfloat16), pltpu.VMEM((seq, HEAD_DIM), jnp.bfloat16),
                        pltpu.VMEM((seq, HEAD_DIM), jnp.float32), pltpu.VMEM((seq, HEAD_DIM), jnp.float32)],
        cost_estimate=pl.CostEstimate(flops=14 * seq * seq * q_width, bytes_accessed=10_000_000, transcendentals=heads * seq * seq),
        name="attention",
    )(lin, lin, lin, d_attn, cos_t, sin_t)


def block_fwd_bwd(x_rows, grad_out, gain_vec, w_all, b_qkv):
    seq_len = x_rows.shape[0]
    w_qkv = w_all[:, :QKV]
    w_out = w_all[:, QKV:]
    half_dim = HEAD_DIM // 2
    inv_freq = jnp.power(ROPE_THETA, -(jnp.arange(half_dim, dtype=jnp.float32) * 2.0 / HEAD_DIM))
    angles = jnp.arange(seq_len, dtype=jnp.float32)[:, None] * inv_freq[None, :]
    cos_h, sin_h = jnp.cos(angles), jnp.sin(angles)
    cos_t = jnp.concatenate([cos_h, cos_h], axis=1)
    sin_t = jnp.concatenate([-sin_h, sin_h], axis=1)
    x_full = x_rows.astype(jnp.float32)
    inv_rms = lax.rsqrt(jnp.mean(x_full * x_full, axis=-1, keepdims=True) + NORM_EPS)
    x_norm = x_full * inv_rms
    gain_f = gain_vec.astype(jnp.float32)
    hidden = (x_norm * gain_f).astype(jnp.bfloat16)
    lin = jnp.dot(hidden, w_qkv, preferred_element_type=jnp.float32) + b_qkv.astype(jnp.float32)
    d_attn = jnp.einsum("lo,io->li", grad_out, w_out, preferred_element_type=jnp.float32).astype(jnp.bfloat16)
    attn_b, dq_b, dk_b, dv_b, grad_bq, grad_bk, grad_bv = attention(lin, d_attn, cos_t, sin_t)
    d_lin_b = jnp.concatenate([dq_b, dk_b, dv_b], axis=1)
    grad_in = (hidden, attn_b, jnp.concatenate([d_lin_b, grad_out], axis=1))
    d_hidden = jnp.einsum("lo,io->li", d_lin_b, w_qkv, preferred_element_type=jnp.float32)
    grad_gain = jnp.sum(d_hidden * x_norm, axis=0)
    d_norm = d_hidden * gain_f
    d_x = grad_out.astype(jnp.float32) + inv_rms * (d_norm - x_norm * jnp.mean(d_norm * x_norm, axis=-1, keepdims=True))
    grad_b = jnp.concatenate([grad_bq[0], grad_bk[0], grad_bv[0]])
    return d_x, grad_in, grad_gain, grad_b


def solution(mesh):
    row_spec = P("fsdp", None)
    vec_spec = P("fsdp")
    act_spec = P("fsdp", None, None)
    weight_specs = (vec_spec, row_spec, vec_spec, row_spec, vec_spec, row_spec, vec_spec, row_spec)
    in_specs = (row_spec, act_spec, row_spec) + weight_specs
    out_specs = (act_spec, row_spec) + weight_specs

    def device_step(tok_ids, grad_out, table_part, gain_part, wq_part, bq_part, wk_part, bk_part, wv_part, bv_part, wo_part):
        rows_dev, model_width = table_part.shape
        seq_len = tok_ids.shape[1]
        me = lax.axis_index("fsdp")
        first_row = me * rows_dev
        w_all = lax.all_gather(jnp.concatenate([wq_part, wk_part, wv_part, wo_part], axis=1), "fsdp", axis=0, tiled=True)

        vec_part = jnp.concatenate([gain_part, bq_part, bk_part, bv_part]).astype(jnp.float32)
        block = jnp.concatenate([tok_ids.reshape(-1).astype(jnp.float32), jnp.pad(vec_part, (0, 1024 - 256 - 144))])
        gathered = small_gather(block.reshape(8, 128)).reshape(N_DEV, 1024)
        all_ids = gathered[:, :seq_len].astype(jnp.int32)
        vecs = gathered[:, seq_len:seq_len + 144].astype(jnp.bfloat16)
        gain_full = vecs[:, :64].reshape(-1)
        b_qkv = jnp.concatenate([vecs[:, 64:128].reshape(-1), vecs[:, 128:136].reshape(-1), vecs[:, 136:144].reshape(-1)])

        owner = all_ids // rows_dev
        key = all_ids * seq_len + jnp.arange(seq_len)
        counts = jnp.sum((owner[:, :, None] == jnp.arange(N_DEV)).astype(jnp.int32), axis=1)
        overflow = (jnp.max(counts[:, 0]) > HOT_CAP) | (jnp.max(counts[:, 1:]) > COLD_CAP)

        mask = owner == me
        rank = jnp.sum((mask[:, None, :] & (key[:, None, :] < key[:, :, None])).astype(jnp.int32), axis=2)
        hit = mask[:, None, :] & (rank[:, None, :] == jnp.arange(HOT_CAP)[None, :, None])
        rows = jnp.sum(jnp.where(hit, (all_ids - first_row)[:, None, :] + 1, 0), axis=2).reshape(-1) - 1
        hot_recv, cold_recv = lookup_exchange(jnp.take(table_part, jnp.maximum(rows, 0), axis=0, mode="clip"))

        my_ids = tok_ids.reshape(-1)
        my_owner = my_ids // rows_dev
        my_key = my_ids * seq_len + jnp.arange(seq_len)
        same = (my_owner[:, None] == my_owner[None, :]) & (my_key[None, :] < my_key[:, None])
        my_rank = jnp.sum(same.astype(jnp.int32), axis=1)
        hot_slot = jnp.where(my_owner == 0, my_rank, -1)
        cold_slot = jnp.where(my_owner > 0, (my_owner - 1) * COLD_CAP + my_rank, -1)
        hot_pick = (hot_slot[:, None] == jnp.arange(HOT_CAP)[None, :]).astype(jnp.bfloat16)
        cold_pick = (cold_slot[:, None] == jnp.arange((N_DEV - 1) * COLD_CAP)[None, :]).astype(jnp.bfloat16)

        def rows_fast():
            picked = jnp.dot(hot_pick, hot_recv, preferred_element_type=jnp.float32)
            picked = picked + jnp.dot(cold_pick, cold_recv, preferred_element_type=jnp.float32)
            return picked.astype(jnp.bfloat16)

        ring = [(i, (i + 1) % N_DEV) for i in range(N_DEV)]

        def owned_rows(step):
            local_idx = jnp.take(all_ids, lax.rem(me - step + N_DEV, N_DEV), axis=0) - first_row
            return local_idx, (local_idx >= 0) & (local_idx < rows_dev)

        def rows_ring():
            def body(step, acc):
                local_idx, is_owned = owned_rows(step)
                looked = jnp.take(table_part, jnp.where(is_owned, local_idx, 0), axis=0, mode="clip")
                acc = jnp.where(is_owned[:, None], looked, acc)
                return lax.ppermute(acc, "fsdp", ring)

            return lax.fori_loop(0, N_DEV, body, jnp.zeros((seq_len, model_width), jnp.bfloat16))

        x_rows = lax.cond(overflow, rows_ring, rows_fast)
        g_rows = grad_out.reshape(seq_len, model_width)
        d_x, grad_in, grad_gain, grad_b = block_fwd_bwd(x_rows, g_rows, gain_full, w_all, b_qkv)
        dx_b = d_x.astype(jnp.bfloat16)
        tdims = (((0,), (0,)), ((), ()))
        hot_back = lax.dot_general(hot_pick, dx_b, tdims, preferred_element_type=jnp.float32).astype(jnp.bfloat16)
        cold_back = lax.dot_general(cold_pick, dx_b, tdims, preferred_element_type=jnp.float32).astype(jnp.bfloat16)
        vec_grad = jnp.concatenate(
            [grad_gain.reshape(N_DEV, 64), grad_b[:2048].reshape(N_DEV, 64), grad_b[2048:2304].reshape(N_DEV, 8),
             grad_b[2304:].reshape(N_DEV, 8), jnp.zeros((N_DEV, 1024 - 144), jnp.float32)], axis=1)
        dx_recv, vec_sum, w_red, block_out = return_exchange(
            hot_back, cold_back, vec_grad.reshape(N_DEV, 8, 128), w_all, *grad_in, x_rows)

        def table_fast():
            return table_sum(dx_recv, rows, rows_dev)

        def table_ring():
            def body(step, carry):
                total, moving = carry
                local_idx, is_owned = owned_rows(step)
                seg_idx = jnp.where(is_owned, local_idx, rows_dev)
                total = total.at[seg_idx].add(moving.astype(jnp.float32), mode="drop")
                return total, lax.ppermute(moving, "fsdp", ring)

            start = (jnp.zeros((rows_dev, model_width), jnp.float32), dx_b)
            return lax.fori_loop(0, N_DEV, body, start)[0].astype(jnp.bfloat16)

        grad_table = lax.cond(overflow, table_ring, table_fast)
        v_red = jnp.sum(vec_sum.reshape(N_DEV, 1024), axis=0)
        return (block_out[None], grad_table, v_red[:64], w_red[:, :2048], v_red[64:128], w_red[:, 2048:2304],
                v_red[128:136], w_red[:, 2304:2560], v_red[136:144], w_red[:, 2560:])

    return jax.shard_map(device_step, mesh=mesh, in_specs=in_specs, out_specs=out_specs, check_vma=False)
```
